32 devices in a mesh: dp: 2 (over y), row: 4 (over z), col: 4 (over x, core).
Axes of the slice: x: 2, y: 2, z: 4, core: 2. Of those that a mesh axis runs over, the one named last changes fastest.
Arguments:
- tokens: bfloat16 [8192, 768], P(('dp', 'row'), 'col'), may hold values from -6 to 6
- prev_logits: float32 [8192, 12], P(('dp', 'row')), may hold values from -3 to 3
- routes: int32 [8192, 2], P('dp'), may hold values from 0 to 11, all different within a row; in each aligned block of 4096 rows (0 to 4095, 4096 to 8191, ...) at most 1280 rows name the same one
- prefix_len: int32 [8], P('dp'), may hold values from 0 to 1024
- norm1_gain: float32 [768], P('col'), may hold values from 0.5 to 1.5
- qkv_weight: bfloat16 [3, 768, 768], P(None, 'col', 'row'), may hold values from -0.21875 to 0.21875
- out_weight: bfloat16 [768, 768], P('row', 'col'), may hold values from -0.875 to 0.875
- norm2_gain: float32 [768], P('col'), may hold values from 0.5 to 1.5
- router_weight: bfloat16 [768, 12], P('col'), may hold values from -0.15625 to 0.15625
- const_weight: bfloat16 [768, 4], P('col'), may hold values from -0.21875 to 0.21875
- const_values: float32 [2, 768], P(None, 'col'), may hold values from -6 to 6
- gate_weight: bfloat16 [8, 768, 2048], P(None, 'col', 'row'), may hold values from -0.21875 to 0.21875
- up_weight: bfloat16 [8, 768, 2048], P(None, 'col', 'row'), may hold values from -0.21875 to 0.21875
- down_weight: bfloat16 [8, 2048, 768], P(None, 'row', 'col'), may hold values from -0.25 to 0.25
- cotangent: bfloat16 [8192, 768], P(('dp', 'row'), 'col'), may hold values from -6 to 6
Outputs:
- layer_out: float32 [8192, 768], P(('dp', 'row'), 'col')
- tokens_grad: float32 [8192, 768], P(('dp', 'row'), 'col')
- prev_grad: float32 [8192, 12], P(('dp', 'row'))
- norm1_gain_grad: float32 [768], P('col')
- qkv_grad: float32 [3, 768, 768], P(None, 'col', 'row')
- out_weight_grad: float32 [768, 768], P('row', 'col')
- norm2_gain_grad: float32 [768], P('col')
- router_grad: float32 [768, 12], P('col')
- const_weight_grad: float32 [768, 4], P('col')
- const_values_grad: float32 [2, 768], P(None, 'col')
- gate_grad: float32 [8, 768, 2048], P(None, 'col', 'row')
- up_grad: float32 [8, 768, 2048], P(None, 'col', 'row')
- down_grad: float32 [8, 2048, 768], P(None, 'row', 'col')
The draws below stay inside these ranges and needn't reach their ends.
Inputs may be any that keep to these rules, and one draw needn't show every extreme that they name: `routes`: each token names two different experts: 0 to 7 are feed-forward experts, 8 the zero expert, 9 the copy expert, 10 and 11 the constant experts. Within each dp group's 4096 tokens no expert is named more than 1280 times, a bound that some block reaches. The first prefix_len tokens of a sequence see one another in both directions; later tokens see the prefix and the tokens before them.
All inputs are finite; a program needn't handle non-finite values.
Results may differ from the reference program's by a relative error of at most 0.015.
Values may be sent and summed in bfloat16 or wider, within the bound.
No kernel may reach another device: no remote copies, remote signals or barrier semaphores. Data moves between devices by JAX's collectives and lax.ppermute only.
A program may use at most 256 MiB of HBM per device.

```python
import math
import jax
import jax.numpy as jnp
import numpy as np
from jax import lax

D = 768
HEADS = 12
HD = 64
FF = 2048
EXPERTS = 8
LEN = 1024
TOK_GRP = 4096
CAP = 1280
KINDS = 12
SEQS = 8
TOKENS = 8192


def set_ends(entries, key, smallest, top_value):
    extent = entries.shape
    spot = [jax.random.randint(jax.random.fold_in(key, axis), (), 0, extent[axis]) for axis in range(len(extent))]
    entries = entries.at[tuple(spot)].set(smallest)
    longest = extent.index(max(extent))
    spot[longest] = (spot[longest] + 1) % extent[longest]
    return entries.at[tuple(spot)].set(top_value)


def block_scale(key, dims, shards, smallest, top_value):
    factor_of = 1.0
    for dim, shards_of in shards:
        heights = jax.random.uniform(jax.random.fold_in(jax.random.fold_in(key, 6), dim), (shards_of,), jnp.float32, smallest / len(shards), top_value / len(shards))
        factor_of = factor_of * jnp.repeat(jnp.exp(heights), dims[dim] // shards_of).reshape((-1,) + (1,) * (len(dims) - 1 - dim))
    return factor_of


def assign_block(rng, own, number, rows, amount, top, bound, slope):
    ranking = jax.random.permutation(rng, amount)
    packed, usual = portions_of(amount, rows * top, bound, slope, True), portions_of(amount, rows * top, bound, slope, False)
    places = jnp.arange(amount)

    def named(sizes, turn):
        used = int((sizes > 0).sum())
        fixed = max(1, used // 4)
        shifted = fixed + (places - fixed + turn * (used - fixed)) % max(1, amount - fixed)
        return jnp.zeros((amount,), jnp.int32).at[ranking[jnp.where(places < fixed, places, shifted)]].set(jnp.asarray(sizes, jnp.int32))

    sizes = jnp.where(number % 4 == 0, named(packed, number // 4), named(usual, number - number // 4 - 1))
    mixed = jax.random.permutation(jax.random.fold_in(own, 3), amount)
    source_of, receiver = mixed[0:amount // 2 * 2:2], mixed[1:amount // 2 * 2:2]
    room = jnp.minimum(sizes[source_of] - 1, bound - sizes[receiver]) // 2
    room = jnp.where((source_of == ranking[0]) | (receiver == ranking[0]) | (sizes[receiver] == 0), 0, jnp.maximum(room, 0))
    shifted = jax.random.randint(jax.random.fold_in(own, 4), (amount // 2,), 0, 1 << 20) % (room + 1)
    sizes = sizes.at[source_of].add(-shifted).at[receiver].add(shifted)
    labels = jnp.searchsorted(jnp.cumsum(sizes), jnp.arange(rows * top), side="right").astype(jnp.int32)
    listing = labels.reshape(top, rows).T
    listing = listing[jax.random.permutation(jax.random.fold_in(own, 1), rows)]
    turn = jax.random.randint(jax.random.fold_in(own, 2), (rows, 1), 0, top)
    return jnp.take_along_axis(listing, (jnp.arange(top)[None, :] + turn) % top, axis=1)


def portions_of(number_of, total, most, slope, full):
    loads = [(1 << 20) // math.isqrt(rank ** slope) + 1 for rank in range(1, number_of + 1)]
    largest = most if full else min(most, max(-(-total // number_of), total * loads[0] // sum(loads)))
    least = 1 if total - largest >= number_of - 1 else 0
    counts, surplus = [largest] + [least] * (number_of - 1), total - largest - least * (number_of - 1)
    while surplus > 0:
        movable = [i for i in range(1, number_of) if counts[i] < largest] or [i for i in range(1, number_of) if counts[i] < most]
        mass, remaining = sum([loads[i] for i in movable]), surplus
        for i in movable:
            extra = min(most - counts[i], max(1, remaining * loads[i] // mass), surplus)
            counts[i] = counts[i] + extra
            surplus = surplus - extra
    return np.array(counts)


def noise(rng, extent, deviation, reach, cuts=(), held_as=jnp.bfloat16):
    factor_of = block_scale(rng, extent, cuts, -0.22, 0.18) if cuts else 1.0
    entries = jax.random.normal(rng, extent, jnp.float32) * deviation * factor_of
    return jnp.minimum(jnp.maximum(entries, -reach), reach).astype(held_as)


def setup_inputs(seed: int = 0) -> dict:
    seeds = jax.random.split(jax.random.key(seed), 16)
    tokens = noise(seeds[0], (TOKENS, D), 1.0, 6.0, ((0, 8), (1, 4)))
    prev_logits = noise(seeds[1], (TOKENS, KINDS), 0.5, 3.0, ((0, 8),), jnp.float32)
    routes_keys = jax.random.split(jax.random.fold_in(seeds[2], 1), TOKENS // TOK_GRP)
    routes_turns = jax.random.permutation(jax.random.fold_in(seeds[2], 3), TOKENS // TOK_GRP)
    routes = jax.vmap(lambda own, number: assign_block(jax.random.fold_in(seeds[2], 2), own, number, TOK_GRP, KINDS, 2, CAP, 1))(routes_keys, routes_turns).reshape((TOKENS, 2))
    prefix_len = set_ends(jax.random.randint(seeds[3], (SEQS,), 0, LEN + 1), jax.random.fold_in(seeds[3], 1), 0, LEN).astype(jnp.int32)
    norm1_gain = jnp.clip(1.0 + 0.1 * jax.random.normal(seeds[4], (D,), jnp.float32), 0.5, 1.5)
    qkv_weight = noise(seeds[5], (3, D, HEADS * HD), D ** -0.5, 0.21875, ((1, 4), (2, 4)))
    out_weight = noise(seeds[6], (HEADS * HD, D), (HEADS * HD // 16) ** -0.5, 0.875, ((0, 4), (1, 4)))
    norm2_gain = jnp.clip(1.0 + 0.1 * jax.random.normal(seeds[7], (D,), jnp.float32), 0.5, 1.5)
    router_weight = noise(seeds[8], (D, KINDS), (2 * D) ** -0.5, 0.15625, ((0, 4),))
    const_weight = noise(seeds[9], (D, 4), D ** -0.5, 0.21875, ((0, 4),))
    const_values = noise(seeds[10], (2, D), 1.0, 6.0, ((1, 4),), jnp.float32)
    gate_weight = noise(seeds[11], (EXPERTS, D, FF), D ** -0.5, 0.21875, ((1, 4), (2, 4)))
    up_weight = noise(seeds[12], (EXPERTS, D, FF), D ** -0.5, 0.21875, ((1, 4), (2, 4)))
    down_weight = noise(seeds[13], (EXPERTS, FF, D), (FF // 4) ** -0.5, 0.25, ((1, 4), (2, 4)))
    cotangent = noise(seeds[14], (TOKENS, D), 1.0, 6.0, ((0, 8), (1, 4)))
    return {"tokens": tokens, "prev_logits": prev_logits, "routes": routes, "prefix_len": prefix_len, "norm1_gain": norm1_gain, "qkv_weight": qkv_weight, "out_weight": out_weight, "norm2_gain": norm2_gain, "router_weight": router_weight, "const_weight": const_weight, "const_values": const_values, "gate_weight": gate_weight, "up_weight": up_weight, "down_weight": down_weight, "cotangent": cotangent}


EPS = 1e-06
HIGH = lax.Precision.HIGHEST

@jax.custom_vjp
def low(v):
    return lax.optimization_barrier(v.astype(jnp.bfloat16)).astype(jnp.float32)

@jax.custom_vjp
def low_back(v):
    return v

def low_keep(v):
    return (low(v), None)

def low_pass(kept, grad):
    return (grad,)

def back_keep(v):
    return (v, None)

def back_low(kept, grad):
    return (low(grad),)
low.defvjp(low_keep, low_pass)
low_back.defvjp(back_keep, back_low)

def matmul(left, right):
    return jnp.dot(left, right, precision=HIGH, preferred_element_type=jnp.float32)

def rms_norm(values, gain):
    inverse = lax.rsqrt(lax.optimization_barrier(jnp.mean(values * values, axis=-1, keepdims=True)) + EPS)
    return values * inverse * gain[None, :]

def rotate(vec, positions, sign):
    half = vec.shape[-1] // 2
    freq = 10000.0 ** (-jnp.arange(half, dtype=jnp.float32) / half)
    angle = positions[:, None].astype(jnp.float32) * freq[None, :]
    cosine = jnp.cos(angle)[:, None, :]
    sine = sign * jnp.sin(angle)[:, None, :]
    first = vec[..., :half]
    second = vec[..., half:]
    return jnp.concatenate([first * cosine - second * sine, second * cosine + first * sine], axis=-1)

def visible(prefix, length):
    places = jnp.arange(length, dtype=jnp.int32)
    return (places[None, :] <= places[:, None]) | (places[None, :] < prefix)

def slot_tables(routes, experts, kinds, capacity):
    flat = routes.reshape(-1)
    pairs = flat.shape[0]
    onehot = (flat[:, None] == jnp.arange(kinds, dtype=jnp.int32)[None, :]).astype(jnp.int32)
    before = jnp.cumsum(onehot, axis=0) - onehot
    place = lax.optimization_barrier(jnp.sum(before * onehot, axis=1))
    usable = flat < experts
    target = jnp.where(usable, flat * capacity + place, experts * capacity)
    table = jnp.full((experts * capacity,), -1, dtype=jnp.int32)
    table = table.at[target].set(jnp.arange(pairs, dtype=jnp.int32), mode='drop')
    slot_of = jnp.where(usable, target, 0)
    return (table.reshape(experts, capacity), slot_of.reshape(-1, 2), usable.reshape(-1, 2))

def attend(pieces):
    query, keys, values, prefix = pieces
    length = query.shape[0]
    scores = low_back(jnp.einsum('qhd,khd->hqk', query, keys, precision=HIGH) * HD ** (-0.5))
    scores = jnp.where(visible(prefix, length)[None], scores, -1e+30)
    probs = jax.nn.softmax(scores, axis=-1)
    mixed = jnp.einsum('hqk,khd->qhd', low(probs), values, precision=HIGH)
    return mixed.reshape(length, -1)

def group_forward(params, pieces):
    gain1, qkv_w, out_w, gain2, router_w, const_w, const_v, gate_w, up_w, down_w = params
    hidden, previous, routes, prefix = pieces
    count = hidden.shape[0]
    experts = gate_w.shape[0]
    kinds = router_w.shape[1]
    normed1 = rms_norm(hidden, gain1)
    act = low(normed1)
    qkv = low_back(jnp.einsum('td,jde->tje', act, qkv_w, precision=HIGH))
    positions = jnp.arange(count, dtype=jnp.int32) % LEN
    spread = (count, HEADS, HD)
    query = low(rotate(qkv[:, 0].reshape(spread), positions, 1.0))
    keys = low(rotate(qkv[:, 1].reshape(spread), positions, 1.0))
    values = low(qkv[:, 2].reshape(spread))
    split = (count // LEN, LEN, HEADS, HD)
    mixed = lax.map(jax.checkpoint(attend), (query.reshape(split), keys.reshape(split), values.reshape(split), prefix))
    attn = low(low_back(mixed.reshape(count, HEADS * HD)))
    mid = hidden + low_back(matmul(attn, out_w))
    normed2 = rms_norm(mid, gain2)
    moe_in = low(normed2)
    logits = matmul(normed2, router_w) + previous
    chosen = jnp.take_along_axis(logits, routes, axis=1)
    gates = jax.nn.softmax(chosen, axis=-1)
    table, slot_of, usable = slot_tables(routes, experts, kinds, CAP)
    source = jnp.maximum(table, 0) // 2
    picked = moe_in[source]
    gate = low_back(jnp.einsum('ecd,edf->ecf', picked, gate_w, precision=HIGH))
    up = low_back(jnp.einsum('ecd,edf->ecf', picked, up_w, precision=HIGH))
    hidden_units = low(jax.nn.silu(gate) * up)
    expert_out = low_back(jnp.einsum('ecf,efd->ecd', hidden_units, down_w, precision=HIGH))
    expert_out = expert_out.reshape(experts * CAP, -1)
    ffn = expert_out[slot_of.reshape(-1)].reshape(count, 2, -1) * usable[..., None].astype(jnp.float32)
    alpha = jax.nn.softmax(matmul(normed2, const_w).reshape(count, 2, 2), axis=-1)
    constant = alpha[:, :, 0:1] * normed2[:, None, :] + alpha[:, :, 1:2] * const_v[None, :, :]
    is_copy = (routes == experts + 1).astype(jnp.float32)[..., None]
    first_const = (routes == experts + 2).astype(jnp.float32)[..., None]
    second_const = (routes == experts + 3).astype(jnp.float32)[..., None]
    branch = ffn + is_copy * normed2[:, None, :] + first_const * constant[:, 0:1, :] + second_const * constant[:, 1:2, :]
    return mid + lax.optimization_barrier(jnp.sum(gates[..., None] * branch, axis=1))

def reference(tokens, prev_logits, routes, prefix_len, norm1_gain, qkv_weight, out_weight, norm2_gain, router_weight, const_weight, const_values, gate_weight, up_weight, down_weight, cotangent):
    groups = tokens.shape[0] // TOK_GRP

    def forward(hidden, previous, gain1, qkv_w, out_w, gain2, router_w, const_w, const_v, gate_w, up_w, down_w):
        params = (gain1, qkv_w, out_w, gain2, router_w, const_w, const_v, gate_w, up_w, down_w)
        pieces = (hidden.reshape(groups, TOK_GRP, -1), previous.reshape(groups, TOK_GRP, -1), routes.reshape(groups, TOK_GRP, 2), prefix_len.reshape(groups, -1))

        def one_group(piece):
            return group_forward(params, piece)
        return lax.map(jax.checkpoint(one_group), pieces).reshape(hidden.shape[0], -1)
    result, pullback = jax.vjp(forward, tokens.astype(jnp.float32), prev_logits.astype(jnp.float32), norm1_gain.astype(jnp.float32), qkv_weight.astype(jnp.float32), out_weight.astype(jnp.float32), norm2_gain.astype(jnp.float32), router_weight.astype(jnp.float32), const_weight.astype(jnp.float32), const_values.astype(jnp.float32), gate_weight.astype(jnp.float32), up_weight.astype(jnp.float32), down_weight.astype(jnp.float32))
    grads = pullback(cotangent.astype(jnp.float32))
    return (result, grads[0], grads[1], grads[2], grads[3], grads[4], grads[5], grads[6], grads[7], grads[8], grads[9], grads[10], grads[11])
```

```python
import jax
import jax.numpy as jnp
from jax import lax
from jax.experimental import pallas as pl
from jax.experimental.pallas import tpu as pltpu
from jax.sharding import PartitionSpec as P

HD = 64
LEN = 1024
EPS = 1e-06
HIGH = lax.Precision.HIGHEST
NEGATIVE = -1e30
TILE = 256
VMEM_LIMIT = 60 * 1024 * 1024
F32 = jnp.float32
BF16 = jnp.bfloat16
GAIN1, GAIN2, VALUE0, VALUE1 = 16, 17, 18, 19


def mm(left, right, over_left, over_right, precision=None):
    return lax.dot_general(
        left,
        right,
        (((over_left,), (over_right,)), ((), ())),
        preferred_element_type=F32,
        precision=precision,
    )


def after(value, *others):
    return lax.optimization_barrier((value,) + others)[0]


def col_swap(value, bits):
    count = lax.axis_size("col")
    return lax.ppermute(value, "col", [(i, i ^ bits) for i in range(count)])


def row_swap(value, bits):
    count = lax.axis_size("row")
    return lax.ppermute(value, "row", [(i, i ^ bits) for i in range(count)])


def row_shift(value, steps):
    count = lax.axis_size("row")
    return lax.ppermute(value, "row", [(i, (i + steps) % count) for i in range(count)])


def col_gather(value):
    count = lax.axis_size("col")
    found = {0: value}
    bit = count // 2
    while bit:
        found.update({k | bit: col_swap(v, bit) for k, v in found.items()})
        bit //= 2
    return [found[k] for k in range(count)]


def row_gather(value):
    count = lax.axis_size("row")
    return [value] + [row_shift(value, s) for s in range(1, count)]


def dp_total(value):
    count = lax.axis_size("dp")
    if count == 2:
        other = lax.ppermute(value, "dp", [(0, 1), (1, 0)])
        return value.astype(F32) + other.astype(F32)
    return lax.psum(value.astype(F32), "dp")


def row_total(value):
    bit = 1
    while bit < lax.axis_size("row"):
        value = value + row_swap(value, bit)
        bit *= 2
    return value


def rotate_halves(block, cosine, sine):
    half = HD // 2
    out = []
    for head in range(block.shape[0] // HD):
        first = block[head * HD : head * HD + half]
        second = block[head * HD + half : (head + 1) * HD]
        out.append(first * cosine - second * sine)
        out.append(second * cosine + first * sine)
    return jnp.concatenate(out, axis=0)


def attend_kernel(
    place, t0, t1, t2, t3, p0, p1, p2, p3, weight, cosine, sine,
    query_out, key_out, value_out, attn_out, logsum_out, act, w_all,
):
    block = pl.program_id(0)
    row = place[0]
    prefix = place[2]
    size = t0.shape[0]
    heads = query_out.shape[1] // HD
    width = heads * HD
    count = query_out.shape[0]
    span = query_out.shape[2]

    @pl.when(block == 0)
    def _():
        square = jnp.zeros((1, t0.shape[1]), F32)
        for ref in (t0, t1, t2, t3):
            hidden = ref[...].astype(F32)
            square = square + jnp.sum(hidden * hidden, axis=0, keepdims=True)
        inverse = lax.rsqrt(square / (size * 4) + EPS)
        for k, (ref, params) in enumerate(((t0, p0), (t1, p1), (t2, p2), (t3, p3))):
            gain = params[:, GAIN1 : GAIN1 + 1]
            act[k * size : (k + 1) * size] = (ref[...].astype(F32) * inverse * gain).astype(BF16)
            w_all[k * size : (k + 1) * size] = weight[row ^ k]
        qkv = mm(w_all[...], act[...], 0, 0)
        query = rotate_halves(qkv[:width], cosine[...], sine[...]).astype(BF16)
        keys = rotate_halves(qkv[width : 2 * width], cosine[...], sine[...]).astype(BF16)
        for i in range(count):
            query_out[i] = query[:, i * span : (i + 1) * span]
        key_out[...] = keys
        value_out[...] = qkv[2 * width :].astype(BF16)

    length = key_out.shape[1]
    places = lax.broadcasted_iota(jnp.int32, (length, span), 0)
    mine = lax.broadcasted_iota(jnp.int32, (1, span), 1) + block * span
    seen = places <= jnp.maximum(mine, prefix - 1)
    rows = []
    for head in range(heads):
        cut = slice(head * HD, (head + 1) * HD)
        query = (query_out[block, cut].astype(F32) * HD ** (-0.5)).astype(BF16)
        scores = jnp.where(seen, mm(key_out[cut], query, 0, 0), NEGATIVE)
        top = jnp.max(scores, axis=0, keepdims=True)
        weights = jnp.exp(scores - top)
        total = jnp.sum(weights, axis=0, keepdims=True)
        mixed = mm(value_out[cut], weights.astype(BF16), 1, 0)
        attn_out[0, cut] = (mixed / total).astype(BF16)
        rows.append(top + jnp.log(total))
    rows.append(jnp.zeros((8 - heads, span), F32))
    logsum_out[...] = jnp.concatenate(rows, axis=0)


def attend(place, toks, params, weight, cosine, sine):
    size, length = toks[0].shape
    count = lax.axis_size("col")
    span = length // count
    width = weight.shape[2] // 3

    def whole(array):
        zeros = (0,) * array.ndim
        return pl.BlockSpec(array.shape, lambda q, s: zeros)

    args = (*toks, *params, weight, cosine, sine)
    return pl.pallas_call(
        attend_kernel,
        name="attend",
        grid_spec=pltpu.PrefetchScalarGridSpec(
            num_scalar_prefetch=1,
            grid=(count,),
            in_specs=[whole(a) for a in args],
            out_specs=[
                pl.BlockSpec((count, width, span), lambda q, s: (0, 0, 0)),
                pl.BlockSpec((width, length), lambda q, s: (0, 0)),
                pl.BlockSpec((width, length), lambda q, s: (0, 0)),
                pl.BlockSpec((1, width, span), lambda q, s: (q ^ s[1], 0, 0)),
                pl.BlockSpec((8, span), lambda q, s: (0, q)),
            ],
            scratch_shapes=[
                pltpu.VMEM((size * count, length), BF16),
                pltpu.VMEM((size * count, 3 * width), BF16),
            ],
        ),
        out_shape=[
            jax.ShapeDtypeStruct((count, width, span), BF16),
            jax.ShapeDtypeStruct((width, length), BF16),
            jax.ShapeDtypeStruct((width, length), BF16),
            jax.ShapeDtypeStruct((count, width, span), BF16),
            jax.ShapeDtypeStruct((8, length), F32),
        ],
        compiler_params=pltpu.CompilerParams(vmem_limit_bytes=VMEM_LIMIT),
    )(place, *args)


def attend_back_kernel(
    place, t0, t1, t2, t3, p0, p1, p2, p3, weight, proj, cosine, sine,
    query, keys, values, attn, logsum, d0, d1, d2, d3, grad_mid,
    tokens_out, qkv_out, proj_out, gain_out,
    dmid, proj_all, proj_acc, key_acc, value_acc, grad_all,
):
    block = pl.program_id(0)
    row = place[0]
    col = place[1]
    prefix = place[2]
    size, length = t0.shape
    count, width, span = query.shape
    heads = width // HD
    last = count - 1

    @pl.when(block == 0)
    def _():
        for k in range(count):
            proj_all[k * size : (k + 1) * size] = proj[row ^ k]
        proj_acc[...] = jnp.zeros_like(proj_acc)
        key_acc[...] = jnp.zeros_like(key_acc)
        value_acc[...] = jnp.zeros_like(value_acc)

    for k, ref in enumerate((d0, d1, d2, d3)):

        @pl.when((block ^ col) == k)
        def _():
            for j in range(count):
                dmid[j * size : (j + 1) * size] = ref[(k ^ j) * size : ((k ^ j) + 1) * size]

    low = dmid[...]
    grad_attn = mm(proj_all[...], low, 0, 0).astype(BF16)
    proj_acc[...] += mm(low, attn[0], 1, 1)
    places = lax.broadcasted_iota(jnp.int32, (length, span), 0)
    mine = lax.broadcasted_iota(jnp.int32, (1, span), 1) + block * span
    seen = places <= jnp.maximum(mine, prefix - 1)
    scale = HD ** (-0.5)
    parts = []
    for head in range(heads):
        cut = slice(head * HD, (head + 1) * HD)
        plain = query[block, cut]
        scaled = (plain.astype(F32) * scale).astype(BF16)
        scores = mm(keys[cut], scaled, 0, 0)
        probs = jnp.where(seen, jnp.exp(scores - logsum[head : head + 1]), 0.0)
        above = grad_attn[cut]
        grad_probs = mm(values[cut], above, 0, 0)
        inner = jnp.sum(probs * grad_probs, axis=0, keepdims=True)
        grad_scores = (probs * (grad_probs - inner)).astype(BF16)
        parts.append(mm(keys[cut], grad_scores, 1, 0) * scale)
        key_acc[cut] += mm(plain, grad_scores, 1, 1)
        value_acc[cut] += mm(above, probs.astype(BF16), 1, 1)
    for i in range(count):

        @pl.when(block == i)
        def _():
            here = slice(i * span, (i + 1) * span)
            turned = rotate_halves(
                jnp.concatenate(parts, axis=0), cosine[:, here], -sine[:, here]
            )
            grad_all[:width, here] = turned.astype(BF16)

    @pl.when(block == last)
    def _():
        turned = rotate_halves(key_acc[...] * scale, cosine[...], -sine[...])
        grad_all[width : 2 * width] = turned.astype(BF16)
        grad_all[2 * width :] = value_acc[...].astype(BF16)
        refs = (t0, t1, t2, t3)
        gains = [params[:, GAIN1 : GAIN1 + 1] for params in (p0, p1, p2, p3)]
        square = jnp.zeros((1, length), F32)
        for ref in refs:
            hidden = ref[...].astype(F32)
            square = square + jnp.sum(hidden * hidden, axis=0, keepdims=True)
        inverse = lax.rsqrt(square / (size * count) + EPS)
        backs = []
        inner = jnp.zeros((1, length), F32)
        for k in range(count):
            hidden = refs[k][...].astype(F32)
            act = (hidden * inverse * gains[k]).astype(BF16)
            qkv_out[row ^ col ^ k] = mm(act, grad_all[...], 1, 1).astype(BF16)
            proj_out[row ^ col ^ k] = proj_acc[k * size : (k + 1) * size].astype(BF16)
            back = mm(weight[row ^ k], grad_all[...], 1, 0)
            inner = inner + jnp.sum(hidden * gains[k] * back, axis=0, keepdims=True)
            summed = jnp.sum(hidden * inverse * back, axis=1, keepdims=True)
            gain_out[k] = jnp.transpose(jnp.broadcast_to(summed, (size, 128)))[:8]
            backs.append(back)
        inner = inner * (inverse * inverse * inverse) / (size * count)
        for k in range(count):
            hidden = refs[k][...].astype(F32)
            grad = inverse * gains[k] * backs[k] - hidden * inner
            for i in range(count):
                here = slice(i * span, (i + 1) * span)
                extra = jnp.where(col == i, grad_mid[k * size : (k + 1) * size], 0.0)
                tokens_out[k, :, here] = (grad[:, here] + extra).astype(BF16)


def attend_back(
    place, toks, params, weight, proj, cosine, sine, query, keys, values, attn, logsum, lows, grad_mid
):
    size, length = toks[0].shape
    count, width, span = query.shape

    def whole(array):
        zeros = (0,) * array.ndim
        return pl.BlockSpec(array.shape, lambda q, s: zeros)

    args = (
        *toks, *params, weight, proj, cosine, sine, query, keys, values, attn, logsum, *lows, grad_mid,
    )
    specs = [whole(a) for a in args]
    at = len(toks) + len(params) + 4 + 3
    specs[at] = pl.BlockSpec((1, width, span), lambda q, s: (q ^ s[1], 0, 0))
    specs[at + 1] = pl.BlockSpec((8, span), lambda q, s: (0, q))
    return pl.pallas_call(
        attend_back_kernel,
        name="attend_back",
        grid_spec=pltpu.PrefetchScalarGridSpec(
            num_scalar_prefetch=1,
            grid=(count,),
            in_specs=specs,
            out_specs=[
                pl.BlockSpec((count, size, length), lambda q, s: (0, 0, 0)),
                pl.BlockSpec((count, size, 3 * width), lambda q, s: (0, 0, 0)),
                pl.BlockSpec((count, size, width), lambda q, s: (0, 0, 0)),
                pl.BlockSpec((count, 8, size), lambda q, s: (0, 0, 0)),
            ],
            scratch_shapes=[
                pltpu.VMEM((size * count, span), BF16),
                pltpu.VMEM((size * count, width), BF16),
                pltpu.VMEM((size * count, width), F32),
                pltpu.VMEM((width, length), F32),
                pltpu.VMEM((width, length), F32),
                pltpu.VMEM((3 * width, length), BF16),
            ],
        ),
        out_shape=[
            jax.ShapeDtypeStruct((count, size, length), BF16),
            jax.ShapeDtypeStruct((count, size, 3 * width), BF16),
            jax.ShapeDtypeStruct((count, size, width), BF16),
            jax.ShapeDtypeStruct((count, 8, size), F32),
        ],
        compiler_params=pltpu.CompilerParams(vmem_limit_bytes=VMEM_LIMIT),
    )(place, *args)


def route_rows(routes, logits):
    places = lax.broadcasted_iota(jnp.int32, logits.shape, 0)
    hots = [places == routes[k : k + 1] for k in range(2)]
    return hots, [jnp.sum(jnp.where(hot, logits, 0.0), axis=0, keepdims=True) for hot in hots]


def pair_softmax(first, second):
    top = jnp.maximum(first, second)
    first = jnp.exp(first - top)
    second = jnp.exp(second - top)
    total = first + second
    return first / total, second / total


def middle_kernel(
    place, t0, t1, t2, t3, p0, p1, p2, p3, a0, a1, a2, a3, o0, o1, o2, o3, previous, routes,
    mid_out, rows_out, stats_out,
):
    row = place[0]
    size, span = t0.shape
    params = (p0, p1, p2, p3)
    kinds = previous.shape[0]
    square = jnp.zeros((1, span), F32)
    for j, ref in enumerate((t0, t1, t2, t3)):
        mid = ref[...].astype(F32)
        for k, (part, proj) in enumerate(((a0, o0), (a1, o1), (a2, o2), (a3, o3))):
            mid = mid + mm(proj[row ^ k ^ j], part[...], 1, 0)
        square = square + jnp.sum(mid * mid, axis=0, keepdims=True)
        mid_out[j * size : (j + 1) * size] = mid
    inverse = lax.rsqrt(square / (size * 4) + EPS)
    summed = jnp.zeros((128, span), F32)
    normed = []
    for j in range(4):
        norm = mid_out[j * size : (j + 1) * size] * inverse * params[j][:, GAIN2 : GAIN2 + 1]
        summed = summed + mm(params[j][...], norm, 0, 0, HIGH)
        normed.append(norm)
    rows_out[...] = jnp.transpose(jnp.concatenate(normed, axis=0)).astype(BF16)
    logits = summed[:kinds] + previous[...]
    _, chosen = route_rows(routes[...], logits)
    gates = pair_softmax(*chosen)
    alpha = [
        *pair_softmax(summed[12:13], summed[13:14]),
        *pair_softmax(summed[14:15], summed[15:16]),
    ]
    stats_out[...] = jnp.concatenate([*gates, inverse, *alpha, jnp.zeros((1, span), F32)], axis=0)


def middle(place, toks, params, parts, projs, previous, routes):
    size, length = toks[0].shape
    span = parts[0].shape[1]
    count = lax.axis_size("col")

    def whole(array):
        zeros = (0,) * array.ndim
        return pl.BlockSpec(array.shape, lambda i, s: zeros)

    args = (*toks, *params, *parts, *projs, previous, routes)
    specs = [pl.BlockSpec((size, span), lambda i, s: (0, s[1])) for _ in toks]
    specs += [whole(a) for a in (*params, *parts, *projs)]
    specs += [
        pl.BlockSpec((previous.shape[0], span), lambda i, s: (0, s[1])),
        pl.BlockSpec((2, span), lambda i, s: (0, s[0] * count + s[1])),
    ]
    full = size * count
    return pl.pallas_call(
        middle_kernel,
        name="middle",
        grid_spec=pltpu.PrefetchScalarGridSpec(
            num_scalar_prefetch=1,
            grid=(1,),
            in_specs=specs,
            out_specs=[
                pl.BlockSpec((full, span), lambda i, s: (0, 0)),
                pl.BlockSpec((span, full), lambda i, s: (0, 0)),
                pl.BlockSpec((8, span), lambda i, s: (0, 0)),
            ],
        ),
        out_shape=[
            jax.ShapeDtypeStruct((full, span), F32),
            jax.ShapeDtypeStruct((span, full), BF16),
            jax.ShapeDtypeStruct((8, span), F32),
        ],
        compiler_params=pltpu.CompilerParams(vmem_limit_bytes=VMEM_LIMIT),
    )(place, *args)


def middle_back_kernel(
    place, p0, p1, p2, p3, mid, grad, stats, routes, x0, x1, x2, x3, g0, g1, g2, g3,
    low_out, mid_out, logits_out, small_out,
):
    params = (p0, p1, p2, p3)
    full, span = mid.shape
    size = p0.shape[0]
    kinds = logits_out.shape[0]
    gates = [stats[0:1], stats[1:2]]
    inverse = stats[2:3]
    alpha = [stats[3:4], stats[4:5], stats[5:6], stats[6:7]]
    names = [routes[0:1], routes[1:2]]
    moe = x0[...].astype(F32) + x1[...].astype(F32) + x2[...].astype(F32) + x3[...].astype(F32)
    moe = jnp.transpose(moe)
    ffn = g0[...] + g1[...] + g2[...] + g3[...]
    flow = grad[...].astype(F32)
    normed = []
    dot_norm = jnp.zeros((1, span), F32)
    dot_value = [jnp.zeros((1, span), F32), jnp.zeros((1, span), F32)]
    for j in range(4):
        here = slice(j * size, (j + 1) * size)
        norm = mid[here] * inverse * params[j][:, GAIN2 : GAIN2 + 1]
        dot_norm = dot_norm + jnp.sum(flow[here] * norm, axis=0, keepdims=True)
        for c, column in enumerate((VALUE0, VALUE1)):
            value = params[j][:, column : column + 1]
            dot_value[c] = dot_value[c] + jnp.sum(flow[here] * value, axis=0, keepdims=True)
        normed.append(norm)
    experts = kinds - 4
    is_copy = [(name == experts + 1).astype(F32) for name in names]
    is_const = [[(name == experts + 2 + c).astype(F32) for name in names] for c in range(2)]
    grad_gate = []
    for k in range(2):
        value = ffn[k : k + 1] + is_copy[k] * dot_norm
        for c in range(2):
            value = value + is_const[c][k] * (
                alpha[2 * c] * dot_norm + alpha[2 * c + 1] * dot_value[c]
            )
        grad_gate.append(value)
    shared = gates[0] * grad_gate[0] + gates[1] * grad_gate[1]
    chosen = [gates[k] * (grad_gate[k] - shared) for k in range(2)]
    places = lax.broadcasted_iota(jnp.int32, (kinds, span), 0)
    logits = jnp.where(places == names[0], chosen[0], 0.0) + jnp.where(
        places == names[1], chosen[1], 0.0
    )
    logits_out[...] = logits
    direct = gates[0] * is_copy[0] + gates[1] * is_copy[1]
    rows = [logits]
    portions = []
    for c in range(2):
        portion = gates[0] * is_const[c][0] + gates[1] * is_const[c][1]
        first, second = alpha[2 * c], alpha[2 * c + 1]
        along = [portion * dot_norm, portion * dot_value[c]]
        mean = first * along[0] + second * along[1]
        rows += [first * (along[0] - mean), second * (along[1] - mean)]
        direct = direct + first * portion
        portions.append(second * portion)
    rows.append(jnp.zeros((128 - kinds - 4, span), F32))
    routed = jnp.concatenate(rows, axis=0)
    lanes = lax.broadcasted_iota(jnp.int32, (size, 128), 1)
    backs = []
    inner = jnp.zeros((1, span), F32)
    for j in range(4):
        here = slice(j * size, (j + 1) * size)
        back = moe[here] + direct * flow[here] + mm(params[j][...], routed, 1, 0, HIGH)
        small = mm(normed[j], routed, 1, 1, HIGH)
        columns = (
            (GAIN2, mid[here] * inverse * back),
            (VALUE0, portions[0] * flow[here]),
            (VALUE1, portions[1] * flow[here]),
        )
        for column, terms in columns:
            total = jnp.sum(terms, axis=1, keepdims=True)
            small = jnp.where(lanes == column, total, small)
        small_out[j] = jnp.transpose(small)[:32]
        gain = params[j][:, GAIN2 : GAIN2 + 1]
        inner = inner + jnp.sum(mid[here] * gain * back, axis=0, keepdims=True)
        backs.append(back)
    inner = inner * (inverse * inverse * inverse) / full
    for j in range(4):
        here = slice(j * size, (j + 1) * size)
        gain = params[j][:, GAIN2 : GAIN2 + 1]
        value = flow[here] + inverse * gain * backs[j] - mid[here] * inner
        mid_out[here] = value
        low_out[here] = value.astype(BF16)


def middle_back(place, params, mid, grad, stats, routes, pieces, gate_pieces, kinds):
    full, span = mid.shape
    count = lax.axis_size("col")
    size = full // count

    def whole(array):
        zeros = (0,) * array.ndim
        return pl.BlockSpec(array.shape, lambda i, s: zeros)

    args = (*params, mid, grad, stats, routes, *pieces, *gate_pieces)
    specs = [whole(a) for a in args]
    specs[len(params) + 3] = pl.BlockSpec((2, span), lambda i, s: (0, s[0] * count + s[1]))
    return pl.pallas_call(
        middle_back_kernel,
        name="middle_back",
        grid_spec=pltpu.PrefetchScalarGridSpec(
            num_scalar_prefetch=1,
            grid=(1,),
            in_specs=specs,
            out_specs=[
                pl.BlockSpec((full, span), lambda i, s: (0, 0)),
                pl.BlockSpec((full, span), lambda i, s: (0, 0)),
                pl.BlockSpec((kinds, span), lambda i, s: (0, 0)),
                pl.BlockSpec((count, 32, size), lambda i, s: (0, 0, 0)),
            ],
        ),
        out_shape=[
            jax.ShapeDtypeStruct((full, span), BF16),
            jax.ShapeDtypeStruct((full, span), F32),
            jax.ShapeDtypeStruct((kinds, span), F32),
            jax.ShapeDtypeStruct((count, 32, size), F32),
        ],
        compiler_params=pltpu.CompilerParams(vmem_limit_bytes=VMEM_LIMIT),
    )(place, *args)


def result_kernel(place, p0, p1, p2, p3, mid, stats, routes, y0, y1, y2, y3, out):
    params = (p0, p1, p2, p3)
    size = p0.shape[0]
    experts = place[3]
    inverse = stats[2:3]
    names = [routes[0:1], routes[1:2]]
    gates = [stats[0:1], stats[1:2]]

    def portion(kind):
        return jnp.where(names[0] == kind, gates[0], 0.0) + jnp.where(
            names[1] == kind, gates[1], 0.0
        )

    first, second = portion(experts + 2), portion(experts + 3)
    direct = portion(experts + 1) + first * stats[3:4] + second * stats[5:6]
    moe = y0[...].astype(F32) + y1[...].astype(F32) + y2[...].astype(F32) + y3[...].astype(F32)
    moe = jnp.transpose(moe)
    for j in range(4):
        here = slice(j * size, (j + 1) * size)
        norm = mid[here] * inverse * params[j][:, GAIN2 : GAIN2 + 1]
        out[j] = (
            mid[here]
            + moe[here]
            + direct * norm
            + first * stats[4:5] * params[j][:, VALUE0 : VALUE0 + 1]
            + second * stats[6:7] * params[j][:, VALUE1 : VALUE1 + 1]
        )


def result(place, params, mid, stats, routes, pieces):
    full, span = mid.shape
    count = lax.axis_size("col")

    def whole(array):
        zeros = (0,) * array.ndim
        return pl.BlockSpec(array.shape, lambda i, s: zeros)

    args = (*params, mid, stats, routes, *pieces)
    specs = [whole(a) for a in args]
    specs[len(params) + 2] = pl.BlockSpec((2, span), lambda i, s: (0, s[0] * count + s[1]))
    return pl.pallas_call(
        result_kernel,
        name="result",
        grid_spec=pltpu.PrefetchScalarGridSpec(
            num_scalar_prefetch=1,
            grid=(1,),
            in_specs=specs,
            out_specs=pl.BlockSpec((count, full // count, span), lambda i, s: (0, 0, 0)),
        ),
        out_shape=jax.ShapeDtypeStruct((count, full // count, span), F32),
        compiler_params=pltpu.CompilerParams(vmem_limit_bytes=VMEM_LIMIT),
    )(place, *args)


def experts_kernel(
    order, x0, x1, x2, x3, g0, g1, g2, g3, s0, s1, s2, s3, ranks, routes,
    w0, w1, near2, far2, near3, far3,
    y_out, dx_out, gate_out, grad0, grad1, grad2, grad3,
    weight, y_acc, dx_acc, gate_rows, acc,
):
    step = pl.program_id(0)
    steps = pl.num_programs(0)
    expert = order[step]
    tiles = order[steps + step]
    size = w0.shape[1]
    span = x0.shape[0]
    hidden_width = w0.shape[2] // 3
    both = 2 * hidden_width
    tokens = ranks.shape[1]
    xs = (x0, x1, x2, x3)
    gs = (g0, g1, g2, g3)

    @pl.when(step == 0)
    def _():
        y_acc[...] = jnp.zeros_like(y_acc)
        dx_acc[...] = jnp.zeros_like(dx_acc)
        gate_out[...] = jnp.zeros_like(gate_out)
        for i, ref in enumerate((s0, s1, s2, s3)):
            gate_rows[:, i * span : (i + 1) * span] = ref[...]

    weight[:size] = w0[0]
    weight[size : 2 * size] = w1[0]

    @pl.when(step < steps // 2)
    def _():
        weight[2 * size : 3 * size] = near2[0]
        weight[3 * size :] = near3[0]

    @pl.when(step >= steps // 2)
    def _():
        weight[2 * size : 3 * size] = far2[0]
        weight[3 * size :] = far3[0]

    rank = ranks[pl.ds(expert, 1), :]
    hit0 = routes[0:1] == expert
    hit1 = routes[1:2] == expert
    gate_row = jnp.where(hit0, gate_rows[0:1], 0.0) + jnp.where(hit1, gate_rows[1:2], 0.0)

    def tile(index, carry):
        slots = lax.broadcasted_iota(jnp.int32, (TILE, tokens), 0) + index * TILE
        hot = slots == rank
        pick = hot.astype(F32).astype(BF16)
        gate = jnp.sum(jnp.where(hot, gate_row, 0.0), axis=1, keepdims=True)
        rows = jnp.zeros((TILE, x0.shape[1]), F32)
        flow = jnp.zeros((TILE, x0.shape[1]), F32)
        for i in range(4):
            cut = pick[:, i * span : (i + 1) * span]
            rows = rows + mm(cut, xs[i][...], 1, 0)
            flow = flow + mm(cut, gs[i][...], 1, 0)
        rows = rows.astype(BF16)
        flow = flow.astype(BF16)
        gate_up = mm(rows, weight[:, :both], 1, 0)
        pre = gate_up[:, :hidden_width]
        up = gate_up[:, hidden_width:]
        sigma = 1.0 / (1.0 + jnp.exp(-pre))
        lifted = pre * sigma
        hidden = lifted * up
        scaled = (hidden * gate).astype(BF16)
        back = mm(flow, weight[:, both:], 1, 0)
        grad_gate = jnp.sum(hidden * back, axis=1, keepdims=True)
        back = back * gate
        grad_pre = back * up * sigma * (1.0 + pre * (1.0 - sigma))
        grad_up = back * lifted
        grad_both = jnp.concatenate([grad_pre.astype(BF16), grad_up.astype(BF16)], axis=1)
        y = mm(scaled, weight[:, both:], 1, 1).astype(BF16)
        dx = mm(grad_both, weight[:, :both], 1, 1).astype(BF16)
        for i in range(4):
            cut = pick[:, i * span : (i + 1) * span]
            y_acc[i * span : (i + 1) * span] += mm(cut, y, 0, 0)
            dx_acc[i * span : (i + 1) * span] += mm(cut, dx, 0, 0)
        row = jnp.sum(jnp.where(hot, grad_gate, 0.0), axis=0, keepdims=True)
        gate_out[0:1] += jnp.where(hit0, row, 0.0)
        gate_out[1:2] += jnp.where(hit1, row, 0.0)
        grad_weight = mm(rows, grad_both, 0, 0)
        grad_down = mm(flow, scaled, 0, 0)

        @pl.when(index == 0)
        def _():
            acc[:, :both] = grad_weight
            acc[:, both:] = grad_down

        @pl.when(index > 0)
        def _():
            acc[:, :both] += grad_weight
            acc[:, both:] += grad_down

        return carry

    lax.fori_loop(0, tiles, tile, 0)
    for k, ref in enumerate((grad0, grad1, grad2, grad3)):
        ref[0] = acc[k * size : (k + 1) * size].astype(BF16)

    @pl.when(step == steps - 1)
    def _():
        y_out[...] = y_acc[...].astype(BF16)
        dx_out[...] = dx_acc[...].astype(BF16)


def run_experts(order, xs, gs, gate_parts, ranks, routes, w0, w1, near2, far2, near3, far3):
    experts, size, wide = w0.shape
    half = experts // 2
    tokens = ranks.shape[1]
    full = xs[0].shape[1]

    def whole(array):
        zeros = (0,) * array.ndim
        return pl.BlockSpec(array.shape, lambda e, s: zeros)

    args = (*xs, *gs, *gate_parts, ranks, routes, w0, w1, near2, far2, near3, far3)
    near = pl.BlockSpec((1, size, wide), lambda e, s: (jnp.minimum(e, half - 1), 0, 0))
    far = pl.BlockSpec((1, size, wide), lambda e, s: (jnp.maximum(e - half, 0), 0, 0))
    mine = pl.BlockSpec((1, size, wide), lambda e, s: (s[e], 0, 0))
    specs = [whole(a) for a in args[:-6]] + [mine, mine, near, far, near, far]
    grad = pl.BlockSpec((1, size, wide), lambda e, s: (e, 0, 0))
    rows = pl.BlockSpec((tokens, full), lambda e, s: (0, 0))
    return pl.pallas_call(
        experts_kernel,
        name="experts",
        grid_spec=pltpu.PrefetchScalarGridSpec(
            num_scalar_prefetch=1,
            grid=(experts,),
            in_specs=specs,
            out_specs=[rows, rows, pl.BlockSpec((8, tokens), lambda e, s: (0, 0))] + [grad] * 4,
            scratch_shapes=[
                pltpu.VMEM((full, wide), BF16),
                pltpu.VMEM((tokens, full), F32),
                pltpu.VMEM((tokens, full), F32),
                pltpu.VMEM((8, tokens), F32),
                pltpu.VMEM((full, wide), F32),
            ],
        ),
        out_shape=[
            jax.ShapeDtypeStruct((tokens, full), BF16),
            jax.ShapeDtypeStruct((tokens, full), BF16),
            jax.ShapeDtypeStruct((8, tokens), F32),
        ]
        + [jax.ShapeDtypeStruct((experts, size, wide), BF16)] * 4,
        compiler_params=pltpu.CompilerParams(vmem_limit_bytes=VMEM_LIMIT),
    )(order, *args)


def shards(
    tokens,
    prev_logits,
    routes,
    prefix_len,
    norm1_gain,
    qkv_weight,
    out_weight,
    norm2_gain,
    router_weight,
    const_weight,
    const_values,
    gate_weight,
    up_weight,
    down_weight,
    cotangent,
):
    row = lax.axis_index("row")
    col = lax.axis_index("col")
    rows = lax.axis_size("row")
    cols = lax.axis_size("col")
    groups = lax.axis_size("dp")
    length, size = tokens.shape
    span = length // cols
    kinds = router_weight.shape[1]
    experts = gate_weight.shape[0]
    half = experts // 2
    hidden_width = gate_weight.shape[2]
    first_half = lax.axis_index("dp") if groups == 2 else jnp.int32(0)
    prefix = lax.dynamic_index_in_dim(prefix_len, row, 0, False)
    place = jnp.stack([row, col, prefix, jnp.int32(experts)]).astype(jnp.int32)
    flat = [(i // cols, i % cols) for i in range(rows * cols)]

    def spread(value, turn):
        pairs = [(c * cols + (c ^ r ^ turn), r * cols + c) for r, c in flat]
        return lax.ppermute(value, ("row", "col"), pairs)

    def collect(value, turn):
        pairs = [(r * cols + c, c * cols + (r ^ turn)) for r, c in flat]
        return lax.ppermute(value, ("row", "col"), pairs)

    toks = col_gather(tokens.T)
    packed = jnp.concatenate(
        [
            router_weight.astype(F32),
            const_weight.astype(F32),
            norm1_gain[:, None],
            norm2_gain[:, None],
            const_values.T,
            jnp.zeros((size, 128 - kinds - 8), F32),
        ],
        axis=1,
    )
    params = col_gather(packed)
    piece = jnp.concatenate([qkv_weight[0], qkv_weight[1], qkv_weight[2]], axis=1)
    weight = jnp.stack([spread(piece, m) for m in range(rows)])
    proj_piece = after(out_weight.T, piece)
    proj = jnp.stack([spread(proj_piece, m) for m in range(rows)])
    halves = HD // 2
    freq = 10000.0 ** (-jnp.arange(halves, dtype=F32) / halves)
    angle = freq[:, None] * jnp.arange(length, dtype=F32)[None, :]
    cosine = jnp.cos(angle)
    sine = jnp.sin(angle)

    own = jnp.concatenate([gate_weight, up_weight, down_weight.transpose(0, 2, 1)], axis=2)
    side = col_swap(own, 1)
    near_mine = lax.dynamic_slice_in_dim(own, first_half * half, half, 0)
    near_two = col_swap(near_mine, 2)
    if groups == 2:
        far_two = lax.ppermute(near_two, "dp", [(0, 1), (1, 0)])
    else:
        far_two = col_swap(lax.dynamic_slice_in_dim(own, half, half, 0), 2)
    near_three = col_swap(near_two, 1)
    far_three = col_swap(far_two, 1)

    flow = cotangent.T.reshape(size, cols, span)
    flow_parts = [lax.dynamic_index_in_dim(flow, col ^ k, 1, False) for k in range(cols)]
    flow_quarter = jnp.concatenate(
        [flow_parts[0]] + [col_swap(flow_parts[k], k) for k in range(1, cols)], axis=0
    )
    flow_rows = row_gather(flow_quarter.T)

    routes_t = routes.T
    share = lax.dynamic_index_in_dim(routes_t.reshape(2, rows, cols, span), col, 2, False)
    turned = (row - jnp.arange(rows)) % rows
    share = jnp.take(share, turned, axis=1).reshape(2, rows * span)
    ids = jnp.arange(experts, dtype=jnp.int32)[:, None]
    hits = (share[0][None] == ids) | (share[1][None] == ids)
    counts = jnp.cumsum(hits.astype(jnp.int32), axis=1)
    ranks = jnp.where(hits, counts - 1, -1)
    order = (first_half * half + jnp.arange(experts, dtype=jnp.int32)) % experts
    tiles = jnp.maximum((counts[:, -1] + TILE - 1) // TILE, 1)
    order = jnp.concatenate([order, jnp.take(tiles, order)]).astype(jnp.int32)

    query, keys, values, attn, logsum = attend(place, toks, params, weight, cosine, sine)
    parts = [attn[0]] + [col_swap(attn[k], k) for k in range(1, cols)]
    projs = col_gather(proj)
    mid, in_rows, stats = middle(place, toks, params, parts, projs, prev_logits.T, routes_t)
    x_rows = row_gather(in_rows)
    gate_parts = row_gather(stats)
    y, dx, gate_grad, *weight_grads = run_experts(
        order, x_rows, flow_rows, gate_parts, ranks, share,
        own, side, near_two, far_two, near_three, far_three,
    )

    def row_scatter(value, axis):
        pieces = [lax.slice_in_dim(value, s * span, (s + 1) * span, axis=axis) for s in range(rows)]
        return [pieces[0]] + [row_shift(pieces[s], -s) for s in range(1, rows)]

    low, grad_mid, grad_logits, small = middle_back(
        place, params, mid, flow_quarter, stats, routes_t,
        row_scatter(dx, 0), row_scatter(gate_grad, 1), kinds,
    )
    lows = col_gather(low)
    tokens_parts, qkv_parts, proj_parts, gain_parts = attend_back(
        place, toks, params, weight, proj, cosine, sine,
        query, keys, values, attn, logsum, lows, grad_mid,
    )

    def col_scatter(value):
        total = value[0].astype(F32)
        for k in range(1, cols):
            total = total + col_swap(value[k], k).astype(F32)
        return total

    grad_tokens = col_scatter(tokens_parts).T

    def weight_total(value):
        total = collect(value[0], 0).astype(F32)
        for m in range(1, rows):
            total = total + collect(value[m], m).astype(F32)
        return dp_total(total.astype(BF16))

    qkv_sum = weight_total(qkv_parts)
    qkv_sum = jnp.stack([qkv_sum[:, j * size : (j + 1) * size] for j in range(3)])
    proj_sum = weight_total(proj_parts).T

    small = dp_total(row_total(col_scatter(small)))
    gain1 = dp_total(row_total(col_scatter(gain_parts)))[0]

    from_side = col_swap(weight_grads[1], 1)
    across = col_swap(weight_grads[3], 1)
    kept = weight_grads[0].astype(F32) + from_side.astype(F32)
    sent = (weight_grads[2].astype(F32) + across.astype(F32)).astype(BF16)
    kept = (kept + col_swap(sent, 2).astype(F32)).astype(BF16)
    first = first_half == 0
    if groups == 2:
        ahead = lax.ppermute(kept[:half], "dp", [(0, 1), (1, 0)]).astype(F32)
        behind = lax.ppermute(kept[half:], "dp", [(0, 1), (1, 0)]).astype(F32)
        near = kept[:half].astype(F32) + behind
        far = kept[half:].astype(F32) + ahead
    else:
        both = lax.psum(kept.astype(F32), "dp")
        near, far = both[:half], both[half:]
    summed = jnp.concatenate([jnp.where(first, near, far), jnp.where(first, far, near)])

    def col_join(value, axis):
        got = [value(0)] + [col_swap(value(k), k) for k in range(1, cols)]
        stacked = jnp.stack(got)
        stacked = jnp.take(stacked, col ^ jnp.arange(cols), axis=0)
        return jnp.concatenate([stacked[i] for i in range(cols)], axis=axis)

    out = result(place, params, mid, stats, routes_t, row_scatter(y, 0))
    layer_out = col_join(lambda k: out[k], 1).T
    prev_grad = col_join(lambda k: grad_logits, 1).T

    return (
        layer_out,
        grad_tokens,
        prev_grad,
        gain1,
        qkv_sum,
        proj_sum,
        small[GAIN2],
        small[:kinds].T,
        small[kinds : kinds + 4].T,
        small[VALUE0 : VALUE1 + 1],
        summed[:, :, :hidden_width],
        summed[:, :, hidden_width : 2 * hidden_width],
        summed[:, :, 2 * hidden_width :].transpose(0, 2, 1),
    )


def solution(mesh):
    return jax.shard_map(
        shards,
        mesh=mesh,
        in_specs=(
            P(("dp", "row"), "col"),
            P(("dp", "row"), None),
            P("dp", None),
            P("dp"),
            P("col"),
            P(None, "col", "row"),
            P("row", "col"),
            P("col"),
            P("col", None),
            P("col", None),
            P(None, "col"),
            P(None, "col", "row"),
            P(None, "col", "row"),
            P(None, "row", "col"),
            P(("dp", "row"), "col"),
        ),
        out_specs=(
            P(("dp", "row"), "col"),
            P(("dp", "row"), "col"),
            P(("dp", "row"), None),
            P("col"),
            P(None, "col", "row"),
            P("row", "col"),
            P("col"),
            P("col", None),
            P("col", None),
            P(None, "col"),
            P(None, "col", "row"),
            P(None, "col", "row"),
            P(None, "row", "col"),
            P(None, "row", "col"),
        )[:13],
        check_vma=False,
    )
```

```python
import jax
import jax.numpy as jnp
from jax import lax
from jax.experimental import pallas as pl
from jax.experimental.pallas import tpu as pltpu
from jax.sharding import PartitionSpec as P

HD = 64
LEN = 1024
EPS = 1e-06
HIGH = lax.Precision.HIGHEST
NEGATIVE = -1e30
TILE = 256
VMEM_LIMIT = 60 * 1024 * 1024
F32 = jnp.float32
BF16 = jnp.bfloat16
PARAMS = 128
GAIN1, GAIN2, VALUE0, VALUE1 = 16, 19, 22, 25
SUM_GAIN2, SUM_VALUE0, SUM_VALUE1, SUM_GAIN1 = 16, 17, 18, 19
EXTRA = 16


def mm(left, right, over_left, over_right, precision=None):
    return lax.dot_general(
        left,
        right,
        (((over_left,), (over_right,)), ((), ())),
        preferred_element_type=F32,
        precision=precision,
    )


def parts_of(value):
    high = lax.reduce_precision(value, 8, 7)
    middle = lax.reduce_precision(value - high, 8, 7)
    return [high.astype(BF16), middle.astype(BF16), (value - high - middle).astype(BF16)]


def column(params, first):
    low = params[:, first : first + 3].astype(F32)
    return low[:, 0:1] + low[:, 1:2] + low[:, 2:3]


def pack_rows(rows, width):
    out = []
    for row in rows:
        high = row.astype(BF16).astype(F32)
        middle = (row - high).astype(BF16).astype(F32)
        out += [high, middle, row - high - middle]
    out.append(jnp.zeros((EXTRA - len(out), rows[0].shape[1]), F32))
    packed = jnp.concatenate(out, axis=0)
    rest = jnp.zeros((EXTRA, width - packed.shape[1]), F32)
    return jnp.concatenate([packed, rest], axis=1).astype(BF16)


def unpack_row(ref, base, span, k):
    parts = ref[base : base + EXTRA, :span].astype(F32)
    return parts[3 * k : 3 * k + 1] + parts[3 * k + 1 : 3 * k + 2] + parts[3 * k + 2 : 3 * k + 3]


def join(*values):
    return lax.optimization_barrier(values)


def col_swap(value, bits):
    count = lax.axis_size("col")
    return lax.ppermute(value, "col", [(i, i ^ bits) for i in range(count)])


def row_swap(value, bits):
    count = lax.axis_size("row")
    return lax.ppermute(value, "row", [(i, i ^ bits) for i in range(count)])


def row_shift(value, steps):
    count = lax.axis_size("row")
    return lax.ppermute(value, "row", [(i, (i + steps) % count) for i in range(count)])


def col_gather(value):
    count = lax.axis_size("col")
    found = {0: value}
    bit = count // 2
    while bit:
        found.update({k | bit: col_swap(v, bit) for k, v in found.items()})
        bit //= 2
    return [found[k] for k in range(count)]


def row_gather(value):
    count = lax.axis_size("row")
    return [value] + [row_shift(value, s) for s in range(1, count)]


def dp_total(value):
    count = lax.axis_size("dp")
    if count == 2:
        other = lax.ppermute(value, "dp", [(0, 1), (1, 0)])
        return value.astype(F32) + other.astype(F32)
    return lax.psum(value.astype(F32), "dp")


def row_total(value):
    bit = 1
    while bit < lax.axis_size("row"):
        value = value + row_swap(value, bit)
        bit *= 2
    return value


def rotate_halves(block, cosine, sine):
    half = HD // 2
    out = []
    for head in range(block.shape[0] // HD):
        first = block[head * HD : head * HD + half]
        second = block[head * HD + half : (head + 1) * HD]
        out.append(first * cosine - second * sine)
        out.append(second * cosine + first * sine)
    return jnp.concatenate(out, axis=0)


def attend_kernel(
    place, t0, t1, t2, t3, weight, cosine, sine,
    query_out, key_out, value_out, attn_out, logsum_out, act, w_all,
):
    block = pl.program_id(0)
    row = place[0]
    prefix = place[2]
    size = t0.shape[0]
    heads = query_out.shape[1] // HD
    width = heads * HD
    count = query_out.shape[0]
    span = query_out.shape[2]
    length = key_out.shape[1]

    @pl.when(block == 0)
    def _():
        square = jnp.zeros((1, length), F32)
        for ref in (t0, t1, t2, t3):
            hidden = ref[:, :length].astype(F32)
            square = square + jnp.sum(hidden * hidden, axis=0, keepdims=True)
        inverse = lax.rsqrt(square / (size * 4) + EPS)
        for k, ref in enumerate((t0, t1, t2, t3)):
            gain = column(ref[:, length:], GAIN1)
            hidden = ref[:, :length].astype(F32)
            act[k * size : (k + 1) * size] = (hidden * inverse * gain).astype(BF16)
            w_all[k * size : (k + 1) * size] = weight[row ^ k, :, : 3 * width]
        qkv = mm(w_all[...], act[...], 0, 0)
        query = rotate_halves(qkv[:width], cosine[...], sine[...]).astype(BF16)
        keys = rotate_halves(qkv[width : 2 * width], cosine[...], sine[...]).astype(BF16)
        for i in range(count):
            query_out[i] = query[:, i * span : (i + 1) * span]
        key_out[...] = keys
        value_out[...] = qkv[2 * width :].astype(BF16)

    places = lax.broadcasted_iota(jnp.int32, (length, span), 0)
    mine = lax.broadcasted_iota(jnp.int32, (1, span), 1) + block * span
    seen = places <= jnp.maximum(mine, prefix - 1)
    rows = []
    for head in range(heads):
        cut = slice(head * HD, (head + 1) * HD)
        query = (query_out[block, cut].astype(F32) * HD ** (-0.5)).astype(BF16)
        scores = jnp.where(seen, mm(key_out[cut], query, 0, 0), NEGATIVE)
        top = jnp.max(scores, axis=0, keepdims=True)
        weights = jnp.exp(scores - top)
        total = jnp.sum(weights, axis=0, keepdims=True)
        mixed = mm(value_out[cut], weights.astype(BF16), 1, 0)
        attn_out[0, cut] = (mixed / total).astype(BF16)
        rows.append(top + jnp.log(total))
    rows.append(jnp.zeros((8 - heads, span), F32))
    logsum_out[...] = jnp.concatenate(rows, axis=0)


def attend(place, toks, weight, cosine, sine):
    size = toks[0].shape[0]
    length = cosine.shape[1]
    count = lax.axis_size("col")
    span = length // count
    width = weight.shape[2] // 4

    def whole(array):
        zeros = (0,) * array.ndim
        return pl.BlockSpec(array.shape, lambda q, s: zeros)

    args = (*toks, weight, cosine, sine)
    return pl.pallas_call(
        attend_kernel,
        name="attend",
        grid_spec=pltpu.PrefetchScalarGridSpec(
            num_scalar_prefetch=1,
            grid=(count,),
            in_specs=[whole(a) for a in args],
            out_specs=[
                pl.BlockSpec((count, width, span), lambda q, s: (0, 0, 0)),
                pl.BlockSpec((width, length), lambda q, s: (0, 0)),
                pl.BlockSpec((width, length), lambda q, s: (0, 0)),
                pl.BlockSpec((1, width, span), lambda q, s: (q ^ s[1], 0, 0)),
                pl.BlockSpec((8, span), lambda q, s: (0, q)),
            ],
            scratch_shapes=[
                pltpu.VMEM((size * count, length), BF16),
                pltpu.VMEM((size * count, 3 * width), BF16),
            ],
        ),
        out_shape=[
            jax.ShapeDtypeStruct((count, width, span), BF16),
            jax.ShapeDtypeStruct((width, length), BF16),
            jax.ShapeDtypeStruct((width, length), BF16),
            jax.ShapeDtypeStruct((count, width, span), BF16),
            jax.ShapeDtypeStruct((8, length), F32),
        ],
        compiler_params=pltpu.CompilerParams(vmem_limit_bytes=VMEM_LIMIT),
    )(place, *args)


def attend_back_kernel(
    place, t0, t1, t2, t3, weight, cosine, sine,
    query, keys, values, attn, logsum, d0, d1, d2, d3, grad_mid, small,
    tokens_out, weight_out, small_out,
    dmid, proj_all, proj_acc, key_acc, value_acc, grad_all,
):
    block = pl.program_id(0)
    row = place[0]
    col = place[1]
    prefix = place[2]
    size = t0.shape[0]
    length = cosine.shape[1]
    count, width, span = query.shape
    heads = width // HD
    last = count - 1

    @pl.when(block == 0)
    def _():
        for k in range(count):
            proj_all[k * size : (k + 1) * size] = weight[row ^ k, :, 3 * width :]
        proj_acc[...] = jnp.zeros_like(proj_acc)
        key_acc[...] = jnp.zeros_like(key_acc)
        value_acc[...] = jnp.zeros_like(value_acc)

    for k, ref in enumerate((d0, d1, d2, d3)):

        @pl.when((block ^ col) == k)
        def _():
            for j in range(count):
                dmid[j * size : (j + 1) * size] = ref[(k ^ j) * size : ((k ^ j) + 1) * size]

    low = dmid[...]
    grad_attn = mm(proj_all[...], low, 0, 0).astype(BF16)
    proj_acc[...] += mm(low, attn[0], 1, 1)
    places = lax.broadcasted_iota(jnp.int32, (length, span), 0)
    mine = lax.broadcasted_iota(jnp.int32, (1, span), 1) + block * span
    seen = places <= jnp.maximum(mine, prefix - 1)
    scale = HD ** (-0.5)
    parts = []
    for head in range(heads):
        cut = slice(head * HD, (head + 1) * HD)
        plain = query[block, cut]
        scaled = (plain.astype(F32) * scale).astype(BF16)
        scores = mm(keys[cut], scaled, 0, 0)
        probs = jnp.where(seen, jnp.exp(scores - logsum[head : head + 1]), 0.0)
        above = grad_attn[cut]
        grad_probs = mm(values[cut], above, 0, 0)
        inner = jnp.sum(probs * grad_probs, axis=0, keepdims=True)
        grad_scores = (probs * (grad_probs - inner)).astype(BF16)
        parts.append(mm(keys[cut], grad_scores, 1, 0) * scale)
        key_acc[cut] += mm(plain, grad_scores, 1, 1)
        value_acc[cut] += mm(above, probs.astype(BF16), 1, 1)
    for i in range(count):

        @pl.when(block == i)
        def _():
            here = slice(i * span, (i + 1) * span)
            turned = rotate_halves(
                jnp.concatenate(parts, axis=0), cosine[:, here], -sine[:, here]
            )
            grad_all[:width, here] = turned.astype(BF16)

    @pl.when(block == last)
    def _():
        turned = rotate_halves(key_acc[...] * scale, cosine[...], -sine[...])
        grad_all[width : 2 * width] = turned.astype(BF16)
        grad_all[2 * width :] = value_acc[...].astype(BF16)
        refs = (t0, t1, t2, t3)
        gains = [column(ref[:, length:], GAIN1) for ref in refs]
        square = jnp.zeros((1, length), F32)
        for ref in refs:
            hidden = ref[:, :length].astype(F32)
            square = square + jnp.sum(hidden * hidden, axis=0, keepdims=True)
        inverse = lax.rsqrt(square / (size * count) + EPS)
        backs = []
        inner = jnp.zeros((1, length), F32)
        for k in range(count):
            hidden = refs[k][:, :length].astype(F32)
            act = (hidden * inverse * gains[k]).astype(BF16)
            weight_out[row ^ col ^ k, :, : 3 * width] = mm(act, grad_all[...], 1, 1).astype(BF16)
            weight_out[row ^ col ^ k, :, 3 * width :] = proj_acc[
                k * size : (k + 1) * size
            ].astype(BF16)
            back = mm(weight[row ^ k, :, : 3 * width], grad_all[...], 1, 0)
            inner = inner + jnp.sum(hidden * gains[k] * back, axis=0, keepdims=True)
            summed = jnp.sum(hidden * inverse * back, axis=1, keepdims=True)
            turned = jnp.transpose(jnp.broadcast_to(summed, (size, 128)))[: small.shape[1]]
            places = lax.broadcasted_iota(jnp.int32, turned.shape, 0)
            small_out[k] = jnp.where(places == SUM_GAIN1, turned, small[k])
            backs.append(back)
        inner = inner * (inverse * inverse * inverse) / (size * count)
        for k in range(count):
            hidden = refs[k][:, :length].astype(F32)
            grad = inverse * gains[k] * backs[k] - hidden * inner
            for i in range(count):
                here = slice(i * span, (i + 1) * span)
                extra = jnp.where(col == i, grad_mid[k * size : (k + 1) * size], 0.0)
                tokens_out[k, :, here] = (grad[:, here] + extra).astype(BF16)


def attend_back(
    place, toks, weight, cosine, sine, query, keys, values, attn, logsum, lows, grad_mid, small
):
    size = toks[0].shape[0]
    length = cosine.shape[1]
    count, width, span = query.shape

    def whole(array):
        zeros = (0,) * array.ndim
        return pl.BlockSpec(array.shape, lambda q, s: zeros)

    args = (
        *toks, weight, cosine, sine, query, keys, values, attn, logsum, *lows, grad_mid, small,
    )
    specs = [whole(a) for a in args]
    at = len(toks) + 3 + 3
    specs[at] = pl.BlockSpec((1, width, span), lambda q, s: (q ^ s[1], 0, 0))
    specs[at + 1] = pl.BlockSpec((8, span), lambda q, s: (0, q))
    return pl.pallas_call(
        attend_back_kernel,
        name="attend_back",
        grid_spec=pltpu.PrefetchScalarGridSpec(
            num_scalar_prefetch=1,
            grid=(count,),
            in_specs=specs,
            out_specs=[
                pl.BlockSpec((count, size, length), lambda q, s: (0, 0, 0)),
                pl.BlockSpec((count, size, 4 * width), lambda q, s: (0, 0, 0)),
                pl.BlockSpec(small.shape, lambda q, s: (0, 0, 0)),
            ],
            scratch_shapes=[
                pltpu.VMEM((size * count, span), BF16),
                pltpu.VMEM((size * count, width), BF16),
                pltpu.VMEM((size * count, width), F32),
                pltpu.VMEM((width, length), F32),
                pltpu.VMEM((width, length), F32),
                pltpu.VMEM((3 * width, length), BF16),
            ],
        ),
        out_shape=[
            jax.ShapeDtypeStruct((count, size, length), BF16),
            jax.ShapeDtypeStruct((count, size, 4 * width), BF16),
            jax.ShapeDtypeStruct(small.shape, F32),
        ],
        compiler_params=pltpu.CompilerParams(vmem_limit_bytes=VMEM_LIMIT),
    )(place, *args)


def route_rows(routes, logits):
    places = lax.broadcasted_iota(jnp.int32, logits.shape, 0)
    hots = [places == routes[k : k + 1] for k in range(2)]
    return hots, [jnp.sum(jnp.where(hot, logits, 0.0), axis=0, keepdims=True) for hot in hots]


def pair_softmax(first, second):
    top = jnp.maximum(first, second)
    first = jnp.exp(first - top)
    second = jnp.exp(second - top)
    total = first + second
    return first / total, second / total


def middle_kernel(
    place, t0, t1, t2, t3, p0, p1, p2, p3, a0, a1, a2, a3, o0, o1, o2, o3, previous, routes,
    mid_out, rows_out, stats_out,
):
    row = place[0]
    size, span = t0.shape
    params = (p0, p1, p2, p3)
    kinds = previous.shape[0]
    square = jnp.zeros((1, span), F32)
    for j, ref in enumerate((t0, t1, t2, t3)):
        mid = ref[...].astype(F32)
        for k, (part, proj) in enumerate(((a0, o0), (a1, o1), (a2, o2), (a3, o3))):
            mid = mid + mm(proj[row ^ k ^ j], part[...], 1, 0)
        square = square + jnp.sum(mid * mid, axis=0, keepdims=True)
        mid_out[j * size : (j + 1) * size] = mid
    inverse = lax.rsqrt(square / (size * 4) + EPS)
    summed = jnp.zeros((128, span), F32)
    normed = []
    for j in range(4):
        norm = mid_out[j * size : (j + 1) * size] * inverse * column(params[j], GAIN2)
        summed = summed + mm(params[j][...].astype(F32), norm, 0, 0, HIGH)
        normed.append(norm)
    rows_out[:span] = jnp.transpose(jnp.concatenate(normed, axis=0)).astype(BF16)
    logits = summed[:kinds] + previous[...]
    _, chosen = route_rows(routes[...], logits)
    gates = pair_softmax(*chosen)
    rows_out[span:] = pack_rows(gates, rows_out.shape[1])
    alpha = [
        *pair_softmax(summed[12:13], summed[13:14]),
        *pair_softmax(summed[14:15], summed[15:16]),
    ]
    stats_out[...] = jnp.concatenate([*gates, inverse, *alpha, jnp.zeros((1, span), F32)], axis=0)


def param_spec(array):
    size, width = array.shape
    return pl.BlockSpec((size, PARAMS), lambda i, s: (0, width // PARAMS - 1))


def middle(place, toks, parts, projs, previous, routes):
    size = toks[0].shape[0]
    span = parts[0].shape[1]
    count = lax.axis_size("col")

    def whole(array):
        zeros = (0,) * array.ndim
        return pl.BlockSpec(array.shape, lambda i, s: zeros)

    args = (*toks, *toks, *parts, *projs, previous, routes)
    specs = [pl.BlockSpec((size, span), lambda i, s: (0, s[1])) for _ in toks]
    specs += [param_spec(a) for a in toks]
    specs += [whole(a) for a in (*parts, *projs)]
    specs += [
        pl.BlockSpec((previous.shape[0], span), lambda i, s: (0, s[1])),
        pl.BlockSpec((2, span), lambda i, s: (0, s[0] * count + s[1])),
    ]
    full = size * count
    return pl.pallas_call(
        middle_kernel,
        name="middle",
        grid_spec=pltpu.PrefetchScalarGridSpec(
            num_scalar_prefetch=1,
            grid=(1,),
            in_specs=specs,
            out_specs=[
                pl.BlockSpec((full, span), lambda i, s: (0, 0)),
                pl.BlockSpec((span + EXTRA, full), lambda i, s: (0, 0)),
                pl.BlockSpec((8, span), lambda i, s: (0, 0)),
            ],
        ),
        out_shape=[
            jax.ShapeDtypeStruct((full, span), F32),
            jax.ShapeDtypeStruct((span + EXTRA, full), BF16),
            jax.ShapeDtypeStruct((8, span), F32),
        ],
        compiler_params=pltpu.CompilerParams(vmem_limit_bytes=VMEM_LIMIT),
    )(place, *args)


def middle_back_kernel(
    place, p0, p1, p2, p3, mid, grad, stats, routes, x0, x1, x2, x3,
    low_out, mid_out, logits_out, small_out,
):
    params = (p0, p1, p2, p3)
    full, span = mid.shape
    size = p0.shape[0]
    kinds = logits_out.shape[0]
    gates = [stats[0:1], stats[1:2]]
    inverse = stats[2:3]
    alpha = [stats[3:4], stats[4:5], stats[5:6], stats[6:7]]
    names = [routes[0:1], routes[1:2]]
    xs = (x0, x1, x2, x3)
    moe = jnp.transpose(sum(x[:span].astype(F32) for x in xs))
    ffn = [sum(unpack_row(x, span, span, k) for x in xs) for k in range(2)]
    flow = grad[...].astype(F32)
    normed = []
    dot_norm = jnp.zeros((1, span), F32)
    dot_value = [jnp.zeros((1, span), F32), jnp.zeros((1, span), F32)]
    for j in range(4):
        here = slice(j * size, (j + 1) * size)
        norm = mid[here] * inverse * column(params[j], GAIN2)
        dot_norm = dot_norm + jnp.sum(flow[here] * norm, axis=0, keepdims=True)
        for c, first in enumerate((VALUE0, VALUE1)):
            value = column(params[j], first)
            dot_value[c] = dot_value[c] + jnp.sum(flow[here] * value, axis=0, keepdims=True)
        normed.append(norm)
    experts = kinds - 4
    is_copy = [(name == experts + 1).astype(F32) for name in names]
    is_const = [[(name == experts + 2 + c).astype(F32) for name in names] for c in range(2)]
    grad_gate = []
    for k in range(2):
        value = ffn[k] + is_copy[k] * dot_norm
        for c in range(2):
            value = value + is_const[c][k] * (
                alpha[2 * c] * dot_norm + alpha[2 * c + 1] * dot_value[c]
            )
        grad_gate.append(value)
    shared = gates[0] * grad_gate[0] + gates[1] * grad_gate[1]
    chosen = [gates[k] * (grad_gate[k] - shared) for k in range(2)]
    places = lax.broadcasted_iota(jnp.int32, (kinds, span), 0)
    logits = jnp.where(places == names[0], chosen[0], 0.0) + jnp.where(
        places == names[1], chosen[1], 0.0
    )
    logits_out[...] = logits
    direct = gates[0] * is_copy[0] + gates[1] * is_copy[1]
    rows = [logits]
    portions = []
    for c in range(2):
        portion = gates[0] * is_const[c][0] + gates[1] * is_const[c][1]
        first, second = alpha[2 * c], alpha[2 * c + 1]
        along = [portion * dot_norm, portion * dot_value[c]]
        mean = first * along[0] + second * along[1]
        rows += [first * (along[0] - mean), second * (along[1] - mean)]
        direct = direct + first * portion
        portions.append(second * portion)
    rows.append(jnp.zeros((128 - kinds - 4, span), F32))
    routed = jnp.concatenate(rows, axis=0)
    lanes = lax.broadcasted_iota(jnp.int32, (size, 128), 1)
    backs = []
    inner = jnp.zeros((1, span), F32)
    for j in range(4):
        here = slice(j * size, (j + 1) * size)
        back = moe[here] + direct * flow[here] + mm(params[j][...].astype(F32), routed, 1, 0, HIGH)
        small = mm(normed[j], routed, 1, 1, HIGH)
        columns = (
            (SUM_GAIN2, mid[here] * inverse * back),
            (SUM_VALUE0, portions[0] * flow[here]),
            (SUM_VALUE1, portions[1] * flow[here]),
        )
        for lane, terms in columns:
            total = jnp.sum(terms, axis=1, keepdims=True)
            small = jnp.where(lanes == lane, total, small)
        small_out[j] = jnp.transpose(small)[:24]
        gain = column(params[j], GAIN2)
        inner = inner + jnp.sum(mid[here] * gain * back, axis=0, keepdims=True)
        backs.append(back)
    inner = inner * (inverse * inverse * inverse) / full
    for j in range(4):
        here = slice(j * size, (j + 1) * size)
        gain = column(params[j], GAIN2)
        value = flow[here] + inverse * gain * backs[j] - mid[here] * inner
        mid_out[here] = value
        low_out[here] = value.astype(BF16)


def middle_back(place, toks, mid, grad, stats, routes, pieces, kinds):
    full, span = mid.shape
    count = lax.axis_size("col")
    size = full // count

    def whole(array):
        zeros = (0,) * array.ndim
        return pl.BlockSpec(array.shape, lambda i, s: zeros)

    args = (*toks, mid, grad, stats, routes, *pieces)
    specs = [param_spec(a) for a in toks] + [whole(a) for a in args[len(toks) :]]
    specs[len(toks) + 3] = pl.BlockSpec((2, span), lambda i, s: (0, s[0] * count + s[1]))
    return pl.pallas_call(
        middle_back_kernel,
        name="middle_back",
        grid_spec=pltpu.PrefetchScalarGridSpec(
            num_scalar_prefetch=1,
            grid=(1,),
            in_specs=specs,
            out_specs=[
                pl.BlockSpec((full, span), lambda i, s: (0, 0)),
                pl.BlockSpec((full, span), lambda i, s: (0, 0)),
                pl.BlockSpec((kinds, span), lambda i, s: (0, 0)),
                pl.BlockSpec((count, 24, size), lambda i, s: (0, 0, 0)),
            ],
        ),
        out_shape=[
            jax.ShapeDtypeStruct((full, span), BF16),
            jax.ShapeDtypeStruct((full, span), F32),
            jax.ShapeDtypeStruct((kinds, span), F32),
            jax.ShapeDtypeStruct((count, 24, size), F32),
        ],
        compiler_params=pltpu.CompilerParams(vmem_limit_bytes=VMEM_LIMIT),
    )(place, *args)


def result_kernel(place, p0, p1, p2, p3, mid, stats, routes, logits, y0, y1, y2, y3, out):
    params = (p0, p1, p2, p3)
    size = p0.shape[0]
    experts = place[3]
    inverse = stats[2:3]
    names = [routes[0:1], routes[1:2]]
    gates = [stats[0:1], stats[1:2]]

    def portion(kind):
        return jnp.where(names[0] == kind, gates[0], 0.0) + jnp.where(
            names[1] == kind, gates[1], 0.0
        )

    first, second = portion(experts + 2), portion(experts + 3)
    direct = portion(experts + 1) + first * stats[3:4] + second * stats[5:6]
    moe = y0[...].astype(F32) + y1[...].astype(F32) + y2[...].astype(F32) + y3[...].astype(F32)
    moe = jnp.transpose(moe)
    for j in range(4):
        here = slice(j * size, (j + 1) * size)
        norm = mid[here] * inverse * column(params[j], GAIN2)
        out[j, :size] = (
            mid[here]
            + moe[here]
            + direct * norm
            + first * stats[4:5] * column(params[j], VALUE0)
            + second * stats[6:7] * column(params[j], VALUE1)
        )
        out[j, size:] = jnp.concatenate(
            [logits[...], jnp.zeros((EXTRA - logits.shape[0], logits.shape[1]), F32)], axis=0
        )


def result(place, toks, mid, stats, routes, logits, pieces):
    full, span = mid.shape
    count = lax.axis_size("col")
    tall = full // count + EXTRA

    def whole(array):
        zeros = (0,) * array.ndim
        return pl.BlockSpec(array.shape, lambda i, s: zeros)

    args = (*toks, mid, stats, routes, logits, *pieces)
    specs = [param_spec(a) for a in toks] + [whole(a) for a in args[len(toks) :]]
    specs[len(toks) + 2] = pl.BlockSpec((2, span), lambda i, s: (0, s[0] * count + s[1]))
    return pl.pallas_call(
        result_kernel,
        name="result",
        grid_spec=pltpu.PrefetchScalarGridSpec(
            num_scalar_prefetch=1,
            grid=(1,),
            in_specs=specs,
            out_specs=pl.BlockSpec((count, tall, span), lambda i, s: (0, 0, 0)),
        ),
        out_shape=jax.ShapeDtypeStruct((count, tall, span), F32),
        compiler_params=pltpu.CompilerParams(vmem_limit_bytes=VMEM_LIMIT),
    )(place, *args)


def experts_kernel(chunks, last, *refs):
    order, x0, x1, x2, x3, g0, g1, g2, g3, ranks, routes, w0, w1 = refs[:13]
    refs = refs[13:]
    twos, refs = refs[: len(chunks)], refs[len(chunks) :]
    threes, refs = refs[: len(chunks)], refs[len(chunks) :]
    if last:
        y_in, dx_in, gate_in = refs[:3]
        refs = refs[3:]
    y_out, dx_out = refs[:2]
    refs = refs[2:]
    if not last:
        gate_out = refs[0]
        refs = refs[1:]
    grad0, grad1, grad2, grad3, weight, y_acc, dx_acc, gate_sum, gate_rows, acc = refs
    step = pl.program_id(0)
    steps = pl.num_programs(0)
    expert = order[step]
    tiles = order[steps + step]
    size = w0.shape[1]
    tokens = ranks.shape[1]
    span = tokens // 4
    full = x0.shape[1]
    hidden_width = w0.shape[2] // 3
    both = 2 * hidden_width
    xs = (x0, x1, x2, x3)
    gs = (g0, g1, g2, g3)

    @pl.when(step == 0)
    def _():
        if last:
            y_acc[...] = y_in[...]
            dx_acc[...] = dx_in[...]
            gate_sum[...] = gate_in[...]
        else:
            y_acc[...] = jnp.zeros_like(y_acc)
            dx_acc[...] = jnp.zeros_like(dx_acc)
            gate_sum[...] = jnp.zeros_like(gate_sum)
        for i, ref in enumerate(xs):
            for k in range(2):
                gate_rows[k : k + 1, i * span : (i + 1) * span] = unpack_row(ref, span, span, k)

    weight[:size] = w0[0]
    weight[size : 2 * size] = w1[0]
    start = 0
    for two, three, count in zip(twos, threes, chunks):

        @pl.when((step >= start) & (step < start + count))
        def _():
            weight[2 * size : 3 * size] = two[0]
            weight[3 * size :] = three[0]

        start += count

    rank = ranks[pl.ds(expert, 1), :]
    hit0 = routes[0:1] == expert
    hit1 = routes[1:2] == expert
    gate_row = jnp.where(hit0, gate_rows[0:1], 0.0) + jnp.where(hit1, gate_rows[1:2], 0.0)

    def tile(index, carry):
        slots = lax.broadcasted_iota(jnp.int32, (TILE, tokens), 0) + index * TILE
        hot = slots == rank
        pick = hot.astype(F32).astype(BF16)
        gate = jnp.sum(jnp.where(hot, gate_row, 0.0), axis=1, keepdims=True)
        rows = jnp.zeros((TILE, full), F32)
        flow = jnp.zeros((TILE, full), F32)
        for i in range(4):
            cut = pick[:, i * span : (i + 1) * span]
            rows = rows + mm(cut, xs[i][:span], 1, 0)
            flow = flow + mm(cut, gs[i][...], 1, 0)
        rows = rows.astype(BF16)
        flow = flow.astype(BF16)
        gate_up = mm(rows, weight[:, :both], 1, 0)
        pre = gate_up[:, :hidden_width]
        up = gate_up[:, hidden_width:]
        sigma = 1.0 / (1.0 + jnp.exp(-pre))
        lifted = pre * sigma
        hidden = lifted * up
        scaled = (hidden * gate).astype(BF16)
        back = mm(flow, weight[:, both:], 1, 0)
        grad_gate = jnp.sum(hidden * back, axis=1, keepdims=True)
        back = back * gate
        grad_pre = back * up * sigma * (1.0 + pre * (1.0 - sigma))
        grad_up = back * lifted
        grad_both = jnp.concatenate([grad_pre.astype(BF16), grad_up.astype(BF16)], axis=1)
        y = mm(scaled, weight[:, both:], 1, 1).astype(BF16)
        dx = mm(grad_both, weight[:, :both], 1, 1).astype(BF16)
        for i in range(4):
            cut = pick[:, i * span : (i + 1) * span]
            y_acc[i * span : (i + 1) * span] += mm(cut, y, 0, 0)
            dx_acc[i * span : (i + 1) * span] += mm(cut, dx, 0, 0)
        row = jnp.sum(jnp.where(hot, grad_gate, 0.0), axis=0, keepdims=True)
        gate_sum[0:1] += jnp.where(hit0, row, 0.0)
        gate_sum[1:2] += jnp.where(hit1, row, 0.0)
        grad_weight = mm(rows, grad_both, 0, 0)
        grad_down = mm(flow, scaled, 0, 0)

        @pl.when(index == 0)
        def _():
            acc[:, :both] = grad_weight
            acc[:, both:] = grad_down

        @pl.when(index > 0)
        def _():
            acc[:, :both] += grad_weight
            acc[:, both:] += grad_down

        return carry

    lax.fori_loop(0, tiles, tile, 0)
    for k, ref in enumerate((grad0, grad1, grad2, grad3)):
        ref[0] = acc[k * size : (k + 1) * size].astype(BF16)

    @pl.when(step == steps - 1)
    def _():
        if last:
            for i in range(4):
                here = slice(i * span, (i + 1) * span)
                y_out[i] = y_acc[here].astype(BF16)
                dx_out[i, :span] = dx_acc[here].astype(BF16)
                rows = [gate_sum[0:1, here], gate_sum[1:2, here]]
                dx_out[i, span:] = pack_rows(rows, full)
        else:
            y_out[...] = y_acc[...]
            dx_out[...] = dx_acc[...]
            gate_out[...] = gate_sum[...]


def run_experts(order, xs, gs, ranks, routes, w0, w1, twos, threes, carried):
    size, wide = w0.shape[1:]
    tokens = ranks.shape[1]
    span = tokens // 4
    full = xs[0].shape[1]
    chunks = tuple(a.shape[0] for a in twos)
    steps = sum(chunks)
    last = carried is not None

    def whole(shape):
        zeros = (0,) * len(shape)
        return pl.BlockSpec(shape, lambda e, s: zeros)

    def chunk(start, count):
        return pl.BlockSpec(
            (1, size, wide), lambda e, s: (jnp.clip(e - start, 0, count - 1), 0, 0)
        )

    mine = pl.BlockSpec((1, size, wide), lambda e, s: (s[e], 0, 0))
    pieces = [chunk(sum(chunks[:i]), count) for i, count in enumerate(chunks)]
    args = (*xs, *gs, ranks, routes, w0, w1, *twos, *threes)
    specs = [whole(a.shape) for a in args[:10]] + [mine, mine] + pieces + pieces
    if last:
        args += tuple(carried)
        specs += [whole(a.shape) for a in carried]
        shapes = [((4, span, full), BF16), ((4, span + EXTRA, full), BF16)]
    else:
        shapes = [((tokens, full), F32), ((tokens, full), F32), ((8, tokens), F32)]
    grad = pl.BlockSpec((1, size, wide), lambda e, s: (e, 0, 0))

    def body(*refs):
        experts_kernel(chunks, last, *refs)

    return pl.pallas_call(
        body,
        name="experts",
        grid_spec=pltpu.PrefetchScalarGridSpec(
            num_scalar_prefetch=1,
            grid=(steps,),
            in_specs=specs,
            out_specs=[whole(shape) for shape, _ in shapes] + [grad] * 4,
            scratch_shapes=[
                pltpu.VMEM((full, wide), BF16),
                pltpu.VMEM((tokens, full), F32),
                pltpu.VMEM((tokens, full), F32),
                pltpu.VMEM((8, tokens), F32),
                pltpu.VMEM((8, tokens), F32),
                pltpu.VMEM((full, wide), F32),
            ],
        ),
        out_shape=[jax.ShapeDtypeStruct(shape, dtype) for shape, dtype in shapes]
        + [jax.ShapeDtypeStruct((steps, size, wide), BF16)] * 4,
        compiler_params=pltpu.CompilerParams(vmem_limit_bytes=VMEM_LIMIT),
    )(order, *args)


def shards(
    tokens,
    prev_logits,
    routes,
    prefix_len,
    norm1_gain,
    qkv_weight,
    out_weight,
    norm2_gain,
    router_weight,
    const_weight,
    const_values,
    gate_weight,
    up_weight,
    down_weight,
    cotangent,
):
    row = lax.axis_index("row")
    col = lax.axis_index("col")
    rows = lax.axis_size("row")
    cols = lax.axis_size("col")
    groups = lax.axis_size("dp")
    length, size = tokens.shape
    span = length // cols
    kinds = router_weight.shape[1]
    experts = gate_weight.shape[0]
    half = experts // 2
    hidden_width = gate_weight.shape[2]
    first_half = lax.axis_index("dp") if groups == 2 else jnp.int32(0)
    prefix = lax.dynamic_index_in_dim(prefix_len, row, 0, False)
    place = jnp.stack([row, col, prefix, jnp.int32(experts)]).astype(jnp.int32)
    flat = [(i // cols, i % cols) for i in range(rows * cols)]

    def spread(value, turn):
        pairs = [(c * cols + (c ^ r ^ turn), r * cols + c) for r, c in flat]
        return lax.ppermute(value, ("row", "col"), pairs)

    def collect(value, turn):
        pairs = [(r * cols + c, c * cols + (r ^ turn)) for r, c in flat]
        return lax.ppermute(value, ("row", "col"), pairs)

    def across_groups(value):
        return lax.ppermute(value, "dp", [(0, 1), (1, 0)])


    values = [norm1_gain, norm2_gain, const_values[0], const_values[1]]
    lanes = [router_weight, const_weight]
    for value in values:
        lanes += [part[:, None] for part in parts_of(value)]
    lanes.append(jnp.zeros((size, PARAMS - kinds - 4 - 3 * len(values)), BF16))
    toks = col_gather(jnp.concatenate([tokens.T] + lanes, axis=1))
    piece = jnp.concatenate([qkv_weight[0], qkv_weight[1], qkv_weight[2], out_weight.T], axis=1)
    weight = jnp.stack([spread(piece, m) for m in range(rows)])
    flow = cotangent.T.reshape(size, cols, span)
    flow_parts = [lax.dynamic_index_in_dim(flow, col ^ k, 1, False) for k in range(cols)]
    flow_quarter = jnp.concatenate(
        [flow_parts[0]] + [col_swap(flow_parts[k], k) for k in range(1, cols)], axis=0
    )
    own = jnp.concatenate([gate_weight, up_weight, down_weight.transpose(0, 2, 1)], axis=2)
    near_own = lax.dynamic_slice_in_dim(own, first_half * half, half, 0)
    two_a = col_swap(near_own[:1], 2)
    halves = HD // 2
    freq = 10000.0 ** (-jnp.arange(halves, dtype=F32) / halves)
    angle = freq[:, None] * jnp.arange(length, dtype=F32)[None, :]
    cosine = jnp.cos(angle)
    sine = jnp.sin(angle)

    routes_t = routes.T
    share = lax.dynamic_index_in_dim(routes_t.reshape(2, rows, cols, span), col, 2, False)
    turned = (row - jnp.arange(rows)) % rows
    share = jnp.take(share, turned, axis=1).reshape(2, rows * span)
    ids = jnp.arange(experts, dtype=jnp.int32)[:, None]
    hits = (share[0][None] == ids) | (share[1][None] == ids)
    counts = jnp.cumsum(hits.astype(jnp.int32), axis=1)
    ranks = jnp.where(hits, counts - 1, -1)
    order = (first_half * half + jnp.arange(experts, dtype=jnp.int32)) % experts
    tiles = jnp.take(jnp.maximum((counts[:, -1] + TILE - 1) // TILE, 1), order)
    order_near = jnp.concatenate([order[:half], tiles[:half]]).astype(jnp.int32)
    order_far = jnp.concatenate([order[half:], tiles[half:]]).astype(jnp.int32)
    toks, weight, flow_quarter, two_a, own, near_own, cosine, sine, ranks, share = join(
        toks, weight, flow_quarter, two_a, own, near_own, cosine, sine, ranks, share
    )

    projs = col_gather(weight[:, :, 3 * size :])
    flow_turned = flow_quarter.T
    flow_rows = {0: flow_turned, 1: row_shift(flow_turned, 1), 3: row_shift(flow_turned, 3)}
    side = col_swap(own, 1)
    three_a = col_swap(two_a, 1)
    query, keys, values, attn, logsum = attend(place, toks, weight, cosine, sine)
    attn, projs, flow_rows, side, three_a = join(attn, projs, flow_rows, side, three_a)

    parts = [attn[0]] + [col_swap(attn[k], k) for k in range(1, cols)]
    flow_rows[2] = row_shift(flow_rows[0], 2)
    two_b = col_swap(near_own[1:2], 2)
    if groups == 2:
        far_two_a = across_groups(two_a)
    else:
        far_two_a = col_swap(own[half : half + 1], 2)
    parts, flow_rows, two_b, far_two_a = join(parts, flow_rows, two_b, far_two_a)

    mid, in_rows, stats = middle(place, toks, parts, projs, prev_logits.T, routes_t)
    x_rows = row_gather(in_rows)
    two_c = col_swap(near_own[2:], 2)
    three_b = col_swap(two_b, 1)
    three_c = col_swap(two_c, 1)
    if groups == 2:
        far_two_b = across_groups(two_b)
    else:
        far_two_b = col_swap(own[half + 1 : half + 2], 2)
    far_three_a = col_swap(far_two_a, 1)
    far_three_b = col_swap(far_two_b, 1)
    x_rows, two_c, three_b, three_c, far_two_b, far_three_a, far_three_b = join(
        x_rows, two_c, three_b, three_c, far_two_b, far_three_a, far_three_b
    )
    flow_rows = [flow_rows[s] for s in range(rows)]

    if groups == 2:
        far_two_c = across_groups(two_c)
    else:
        far_two_c = col_swap(own[half + 2 :], 2)
    far_three_c = col_swap(far_two_c, 1)
    near_out = run_experts(
        order_near, x_rows, flow_rows, ranks, share, own, side,
        [two_a, two_b, two_c], [three_a, three_b, three_c], None,
    )
    near_out, far_two_c, far_three_c = join(near_out, far_two_c, far_three_c)
    *carried, near0, near1, near2, near3 = near_out

    near1 = col_swap(near1, 1)
    near3 = col_swap(near3, 1)
    far_out = run_experts(
        order_far, x_rows, flow_rows, ranks, share, own, side,
        [far_two_a, far_two_b, far_two_c], [far_three_a, far_three_b, far_three_c], carried,
    )
    far_out, near1, near3 = join(far_out, near1, near3)
    y, dx, far0, far1, far2, far3 = far_out

    def low_sum(left, right):
        return (left.astype(F32) + right.astype(F32)).astype(BF16)

    def row_scatter(value):
        return [value[0]] + [row_shift(value[s], -s) for s in range(1, rows)]

    quarter = half // 2
    dx = row_scatter(dx)
    near_sent = [low_sum(near2[:quarter], near3[:quarter]), low_sum(near2[quarter:], near3[quarter:])]
    near_kept = low_sum(near0, near1)
    near_got = [col_swap(near_sent[0], 2)]
    far1 = col_swap(far1, 1)
    far3 = col_swap(far3, 1)
    dx, near_got, near_sent, near_kept, far1, far3 = join(
        dx, near_got, near_sent, near_kept, far1, far3
    )

    low, grad_mid, grad_logits, small = middle_back(
        place, toks, mid, flow_quarter, stats, routes_t, dx, kinds
    )
    lows = col_gather(low)
    near_sum = [low_sum(near_kept[:quarter], near_got[0])]
    lows, near_sum = join(lows, near_sum)

    y = row_scatter(y)
    near_got.append(col_swap(near_sent[1], 2))
    if groups == 2:
        near_other = [across_groups(near_sum[0])]
    far_sent = [low_sum(far2[:quarter], far3[:quarter]), low_sum(far2[quarter:], far3[quarter:])]
    far_kept = low_sum(far0, far1)
    tokens_parts, weight_parts, small = attend_back(
        place, toks, weight, cosine, sine,
        query, keys, values, attn, logsum, lows, grad_mid, small,
    )
    y, near_got, far_sent, far_kept, tokens_parts, weight_parts, small = join(
        y, near_got, far_sent, far_kept, tokens_parts, weight_parts, small
    )
    if groups == 2:
        near_other, near_got = join(near_other, near_got)

    def col_scatter(value):
        total = value[0].astype(F32)
        for k in range(1, cols):
            total = total + col_swap(value[k], k).astype(F32)
        return total

    grad_tokens = col_scatter(tokens_parts)
    total = collect(weight_parts[0], 0).astype(F32)
    for m in range(1, rows):
        total = total + collect(weight_parts[m], m).astype(F32)
    small = col_scatter(small)
    near_sum.append(low_sum(near_kept[quarter:], near_got[1]))
    if groups == 2:
        near_other.append(across_groups(near_sum[1]))
    far_got = [col_swap(far_sent[0], 2)]
    out = result(place, toks, mid, stats, routes_t, grad_logits, y)
    grad_tokens, total, small, far_got, out = join(grad_tokens, total, small, far_got, out)

    far_sum = [low_sum(far_kept[:quarter], far_got[0])]
    far_got.append(col_swap(far_sent[1], 2))
    far_sum.append(low_sum(far_kept[quarter:], far_got[1]))
    total = dp_total(total.astype(BF16))
    qkv_sum = jnp.stack([total[:, j * size : (j + 1) * size] for j in range(3)])
    proj_sum = total[:, 3 * size :].T
    small = dp_total(row_total(small))
    out = jnp.stack([out[0]] + [col_swap(out[k], k) for k in range(1, cols)])
    out = jnp.take(out, col ^ jnp.arange(cols), axis=0)
    out = jnp.concatenate([out[i] for i in range(cols)], axis=1)
    if groups == 2:
        far_other = [across_groups(s) for s in far_sum]
        near_start = first_half * half
        far_start = half - near_start
        grads = []
        for j in range(3):
            wide = slice(j * hidden_width, (j + 1) * hidden_width)
            grad = jnp.zeros((experts, size, hidden_width), F32)
            for i in range(2):
                for start, mine, other in (
                    (near_start, near_sum[i], far_other[i]),
                    (far_start, far_sum[i], near_other[i]),
                ):
                    both = mine[:, :, wide].astype(F32) + other[:, :, wide].astype(F32)
                    grad = lax.dynamic_update_slice_in_dim(grad, both, start + i * quarter, 0)
            grads.append(grad)
    else:
        both = lax.psum(jnp.concatenate(near_sum + far_sum).astype(F32), "dp")
        grads = [both[:, :, j * hidden_width : (j + 1) * hidden_width] for j in range(3)]

    return (
        out[:size].T,
        grad_tokens.T,
        out[size : size + kinds].T,
        small[SUM_GAIN1],
        qkv_sum,
        proj_sum,
        small[SUM_GAIN2],
        small[:kinds].T,
        small[kinds : kinds + 4].T,
        small[SUM_VALUE0 : SUM_VALUE1 + 1],
        grads[0],
        grads[1],
        grads[2].transpose(0, 2, 1),
    )


def solution(mesh):
    return jax.shard_map(
        shards,
        mesh=mesh,
        in_specs=(
            P(("dp", "row"), "col"),
            P(("dp", "row"), None),
            P("dp", None),
            P("dp"),
            P("col"),
            P(None, "col", "row"),
            P("row", "col"),
            P("col"),
            P("col", None),
            P("col", None),
            P(None, "col"),
            P(None, "col", "row"),
            P(None, "col", "row"),
            P(None, "row", "col"),
            P(("dp", "row"), "col"),
        ),
        out_specs=(
            P(("dp", "row"), "col"),
            P(("dp", "row"), "col"),
            P(("dp", "row"), None),
            P("col"),
            P(None, "col", "row"),
            P("row", "col"),
            P("col"),
            P("col", None),
            P("col", None),
            P(None, "col"),
            P(None, "col", "row"),
            P(None, "col", "row"),
            P(None, "row", "col"),
        ),
        check_vma=False,
    )
```

```python
import jax
import jax.numpy as jnp
from jax import lax
from jax.experimental import pallas as pl
from jax.experimental.pallas import tpu as pltpu
from jax.sharding import PartitionSpec as P

HD = 64
LEN = 1024
EPS = 1e-06
HIGH = lax.Precision.HIGHEST
NEGATIVE = -1e30
TILE = 256
VMEM_LIMIT = 60 * 1024 * 1024
F32 = jnp.float32
BF16 = jnp.bfloat16
PARAMS = 128
GAIN1, GAIN2, VALUE0, VALUE1 = 16, 19, 22, 25
SUM_GAIN2, SUM_VALUE0, SUM_VALUE1, SUM_GAIN1 = 16, 17, 18, 19
EXTRA = 16


def mm(left, right, over_left, over_right, precision=None):
    return lax.dot_general(
        left,
        right,
        (((over_left,), (over_right,)), ((), ())),
        preferred_element_type=F32,
        precision=precision,
    )


def parts_of(value):
    high = lax.reduce_precision(value, 8, 7)
    middle = lax.reduce_precision(value - high, 8, 7)
    return [high.astype(BF16), middle.astype(BF16), (value - high - middle).astype(BF16)]


def column(params, first):
    low = params[:, first : first + 3].astype(F32)
    return low[:, 0:1] + low[:, 1:2] + low[:, 2:3]


def pack_rows(rows, width):
    out = []
    for row in rows:
        high = row.astype(BF16).astype(F32)
        middle = (row - high).astype(BF16).astype(F32)
        out += [high, middle, row - high - middle]
    out.append(jnp.zeros((EXTRA - len(out), rows[0].shape[1]), F32))
    packed = jnp.concatenate(out, axis=0)
    rest = jnp.zeros((EXTRA, width - packed.shape[1]), F32)
    return jnp.concatenate([packed, rest], axis=1).astype(BF16)


def unpack_row(ref, base, span, k):
    parts = ref[base : base + EXTRA, :span].astype(F32)
    return parts[3 * k : 3 * k + 1] + parts[3 * k + 1 : 3 * k + 2] + parts[3 * k + 2 : 3 * k + 3]


def span_of(micros):
    return pl.CostEstimate(
        flops=int(micros * 1.1e9), transcendentals=0, bytes_accessed=int(micros * 3.6e6)
    )


def after(value, *others):
    return lax.optimization_barrier((value,) + others)[0]


def join(*values):
    return lax.optimization_barrier(values)


def col_swap(value, bits):
    count = lax.axis_size("col")
    return lax.ppermute(value, "col", [(i, i ^ bits) for i in range(count)])


def row_swap(value, bits):
    count = lax.axis_size("row")
    return lax.ppermute(value, "row", [(i, i ^ bits) for i in range(count)])


def row_shift(value, steps):
    count = lax.axis_size("row")
    return lax.ppermute(value, "row", [(i, (i + steps) % count) for i in range(count)])


def col_gather(value):
    count = lax.axis_size("col")
    found = {0: value}
    bit = count // 2
    while bit:
        found.update({k | bit: col_swap(v, bit) for k, v in found.items()})
        bit //= 2
    return [found[k] for k in range(count)]


def row_gather(value):
    count = lax.axis_size("row")
    return [value] + [row_shift(value, s) for s in range(1, count)]


def dp_total(value):
    count = lax.axis_size("dp")
    if count == 2:
        other = lax.ppermute(value, "dp", [(0, 1), (1, 0)])
        return value.astype(F32) + other.astype(F32)
    return lax.psum(value.astype(F32), "dp")


def row_total(value):
    bit = 1
    while bit < lax.axis_size("row"):
        value = value + row_swap(value, bit)
        bit *= 2
    return value


def rotate_halves(block, cosine, sine):
    half = HD // 2
    out = []
    for head in range(block.shape[0] // HD):
        first = block[head * HD : head * HD + half]
        second = block[head * HD + half : (head + 1) * HD]
        out.append(first * cosine - second * sine)
        out.append(second * cosine + first * sine)
    return jnp.concatenate(out, axis=0)


def attend_kernel(
    place, t0, t1, t2, t3, weight, cosine, sine,
    query_out, key_out, value_out, attn_out, logsum_out, act, w_all,
):
    block = pl.program_id(0)
    row = place[0]
    prefix = place[2]
    size = t0.shape[0]
    heads = query_out.shape[1] // HD
    width = heads * HD
    count = query_out.shape[0]
    span = query_out.shape[2]
    length = key_out.shape[1]

    @pl.when(block == 0)
    def _():
        square = jnp.zeros((1, length), F32)
        for ref in (t0, t1, t2, t3):
            hidden = ref[:, :length].astype(F32)
            square = square + jnp.sum(hidden * hidden, axis=0, keepdims=True)
        inverse = lax.rsqrt(square / (size * 4) + EPS)
        for k, ref in enumerate((t0, t1, t2, t3)):
            gain = column(ref[:, length:], GAIN1)
            hidden = ref[:, :length].astype(F32)
            act[k * size : (k + 1) * size] = (hidden * inverse * gain).astype(BF16)
            w_all[k * size : (k + 1) * size] = weight[row ^ k, :, : 3 * width]
        qkv = mm(w_all[...], act[...], 0, 0)
        query = rotate_halves(qkv[:width], cosine[...], sine[...]).astype(BF16)
        keys = rotate_halves(qkv[width : 2 * width], cosine[...], sine[...]).astype(BF16)
        for i in range(count):
            query_out[i] = query[:, i * span : (i + 1) * span]
        key_out[...] = keys
        value_out[...] = qkv[2 * width :].astype(BF16)

    places = lax.broadcasted_iota(jnp.int32, (length, span), 0)
    mine = lax.broadcasted_iota(jnp.int32, (1, span), 1) + block * span
    seen = places <= jnp.maximum(mine, prefix - 1)
    rows = []
    for head in range(heads):
        cut = slice(head * HD, (head + 1) * HD)
        query = (query_out[block, cut].astype(F32) * HD ** (-0.5)).astype(BF16)
        scores = jnp.where(seen, mm(key_out[cut], query, 0, 0), NEGATIVE)
        top = jnp.max(scores, axis=0, keepdims=True)
        weights = jnp.exp(scores - top)
        total = jnp.sum(weights, axis=0, keepdims=True)
        mixed = mm(value_out[cut], weights.astype(BF16), 1, 0)
        attn_out[0, cut] = (mixed / total).astype(BF16)
        rows.append(top + jnp.log(total))
    rows.append(jnp.zeros((8 - heads, span), F32))
    logsum_out[...] = jnp.concatenate(rows, axis=0)


def attend(place, toks, weight, cosine, sine):
    size = toks[0].shape[0]
    length = cosine.shape[1]
    count = lax.axis_size("col")
    span = length // count
    width = weight.shape[2] // 4

    def whole(array):
        zeros = (0,) * array.ndim
        return pl.BlockSpec(array.shape, lambda q, s: zeros)

    args = (*toks, weight, cosine, sine)
    return pl.pallas_call(
        attend_kernel,
        name="attend",
        cost_estimate=span_of(14),
        grid_spec=pltpu.PrefetchScalarGridSpec(
            num_scalar_prefetch=1,
            grid=(count,),
            in_specs=[whole(a) for a in args],
            out_specs=[
                pl.BlockSpec((count, width, span), lambda q, s: (0, 0, 0)),
                pl.BlockSpec((width, length), lambda q, s: (0, 0)),
                pl.BlockSpec((width, length), lambda q, s: (0, 0)),
                pl.BlockSpec((1, width, span), lambda q, s: (q ^ s[1], 0, 0)),
                pl.BlockSpec((8, span), lambda q, s: (0, q)),
            ],
            scratch_shapes=[
                pltpu.VMEM((size * count, length), BF16),
                pltpu.VMEM((size * count, 3 * width), BF16),
            ],
        ),
        out_shape=[
            jax.ShapeDtypeStruct((count, width, span), BF16),
            jax.ShapeDtypeStruct((width, length), BF16),
            jax.ShapeDtypeStruct((width, length), BF16),
            jax.ShapeDtypeStruct((count, width, span), BF16),
            jax.ShapeDtypeStruct((8, length), F32),
        ],
        compiler_params=pltpu.CompilerParams(vmem_limit_bytes=VMEM_LIMIT),
    )(place, *args)


def attend_back_kernel(
    place, t0, t1, t2, t3, weight, cosine, sine,
    query, keys, values, attn, logsum, d0, d1, d2, d3, grad_mid, small,
    tokens_out, weight_out, small_out,
    dmid, proj_all, proj_acc, key_acc, value_acc, grad_all,
):
    block = pl.program_id(0)
    row = place[0]
    col = place[1]
    prefix = place[2]
    size = t0.shape[0]
    length = cosine.shape[1]
    count, width, span = query.shape
    heads = width // HD
    last = count - 1

    @pl.when(block == 0)
    def _():
        for k in range(count):
            proj_all[k * size : (k + 1) * size] = weight[row ^ k, :, 3 * width :]
        proj_acc[...] = jnp.zeros_like(proj_acc)
        key_acc[...] = jnp.zeros_like(key_acc)
        value_acc[...] = jnp.zeros_like(value_acc)

    for k, ref in enumerate((d0, d1, d2, d3)):

        @pl.when((block ^ col) == k)
        def _():
            for j in range(count):
                dmid[j * size : (j + 1) * size] = ref[(k ^ j) * size : ((k ^ j) + 1) * size]

    low = dmid[...]
    grad_attn = mm(proj_all[...], low, 0, 0).astype(BF16)
    proj_acc[...] += mm(low, attn[0], 1, 1)
    places = lax.broadcasted_iota(jnp.int32, (length, span), 0)
    mine = lax.broadcasted_iota(jnp.int32, (1, span), 1) + block * span
    seen = places <= jnp.maximum(mine, prefix - 1)
    scale = HD ** (-0.5)
    parts = []
    for head in range(heads):
        cut = slice(head * HD, (head + 1) * HD)
        plain = query[block, cut]
        scaled = (plain.astype(F32) * scale).astype(BF16)
        scores = mm(keys[cut], scaled, 0, 0)
        probs = jnp.where(seen, jnp.exp(scores - logsum[head : head + 1]), 0.0)
        above = grad_attn[cut]
        grad_probs = mm(values[cut], above, 0, 0)
        inner = jnp.sum(probs * grad_probs, axis=0, keepdims=True)
        grad_scores = (probs * (grad_probs - inner)).astype(BF16)
        parts.append(mm(keys[cut], grad_scores, 1, 0) * scale)
        key_acc[cut] += mm(plain, grad_scores, 1, 1)
        value_acc[cut] += mm(above, probs.astype(BF16), 1, 1)
    for i in range(count):

        @pl.when(block == i)
        def _():
            here = slice(i * span, (i + 1) * span)
            turned = rotate_halves(
                jnp.concatenate(parts, axis=0), cosine[:, here], -sine[:, here]
            )
            grad_all[:width, here] = turned.astype(BF16)

    @pl.when(block == last)
    def _():
        turned = rotate_halves(key_acc[...] * scale, cosine[...], -sine[...])
        grad_all[width : 2 * width] = turned.astype(BF16)
        grad_all[2 * width :] = value_acc[...].astype(BF16)
        refs = (t0, t1, t2, t3)
        gains = [column(ref[:, length:], GAIN1) for ref in refs]
        square = jnp.zeros((1, length), F32)
        for ref in refs:
            hidden = ref[:, :length].astype(F32)
            square = square + jnp.sum(hidden * hidden, axis=0, keepdims=True)
        inverse = lax.rsqrt(square / (size * count) + EPS)
        backs = []
        inner = jnp.zeros((1, length), F32)
        for k in range(count):
            hidden = refs[k][:, :length].astype(F32)
            act = (hidden * inverse * gains[k]).astype(BF16)
            weight_out[row ^ col ^ k, :, : 3 * width] = mm(act, grad_all[...], 1, 1).astype(BF16)
            weight_out[row ^ col ^ k, :, 3 * width :] = proj_acc[
                k * size : (k + 1) * size
            ].astype(BF16)
            back = mm(weight[row ^ k, :, : 3 * width], grad_all[...], 1, 0)
            inner = inner + jnp.sum(hidden * gains[k] * back, axis=0, keepdims=True)
            summed = jnp.sum(hidden * inverse * back, axis=1, keepdims=True)
            turned = jnp.transpose(jnp.broadcast_to(summed, (size, 128)))[: small.shape[1]]
            places = lax.broadcasted_iota(jnp.int32, turned.shape, 0)
            small_out[k] = jnp.where(places == SUM_GAIN1, turned, small[k])
            backs.append(back)
        inner = inner * (inverse * inverse * inverse) / (size * count)
        for k in range(count):
            hidden = refs[k][:, :length].astype(F32)
            grad = inverse * gains[k] * backs[k] - hidden * inner
            for i in range(count):
                here = slice(i * span, (i + 1) * span)
                extra = jnp.where(col == i, grad_mid[k * size : (k + 1) * size], 0.0)
                tokens_out[k, :, here] = (grad[:, here] + extra).astype(BF16)


def attend_back(
    place, toks, weight, cosine, sine, query, keys, values, attn, logsum, lows, grad_mid, small
):
    size = toks[0].shape[0]
    length = cosine.shape[1]
    count, width, span = query.shape

    def whole(array):
        zeros = (0,) * array.ndim
        return pl.BlockSpec(array.shape, lambda q, s: zeros)

    args = (
        *toks, weight, cosine, sine, query, keys, values, attn, logsum, *lows, grad_mid, small,
    )
    specs = [whole(a) for a in args]
    at = len(toks) + 3 + 3
    specs[at] = pl.BlockSpec((1, width, span), lambda q, s: (q ^ s[1], 0, 0))
    specs[at + 1] = pl.BlockSpec((8, span), lambda q, s: (0, q))
    return pl.pallas_call(
        attend_back_kernel,
        name="attend_back",
        cost_estimate=span_of(24),
        grid_spec=pltpu.PrefetchScalarGridSpec(
            num_scalar_prefetch=1,
            grid=(count,),
            in_specs=specs,
            out_specs=[
                pl.BlockSpec((count, size, length), lambda q, s: (0, 0, 0)),
                pl.BlockSpec((count, size, 4 * width), lambda q, s: (0, 0, 0)),
                pl.BlockSpec(small.shape, lambda q, s: (0, 0, 0)),
            ],
            scratch_shapes=[
                pltpu.VMEM((size * count, span), BF16),
                pltpu.VMEM((size * count, width), BF16),
                pltpu.VMEM((size * count, width), F32),
                pltpu.VMEM((width, length), F32),
                pltpu.VMEM((width, length), F32),
                pltpu.VMEM((3 * width, length), BF16),
            ],
        ),
        out_shape=[
            jax.ShapeDtypeStruct((count, size, length), BF16),
            jax.ShapeDtypeStruct((count, size, 4 * width), BF16),
            jax.ShapeDtypeStruct(small.shape, F32),
        ],
        compiler_params=pltpu.CompilerParams(vmem_limit_bytes=VMEM_LIMIT),
    )(place, *args)


def route_rows(routes, logits):
    places = lax.broadcasted_iota(jnp.int32, logits.shape, 0)
    hots = [places == routes[k : k + 1] for k in range(2)]
    return hots, [jnp.sum(jnp.where(hot, logits, 0.0), axis=0, keepdims=True) for hot in hots]


def pair_softmax(first, second):
    top = jnp.maximum(first, second)
    first = jnp.exp(first - top)
    second = jnp.exp(second - top)
    total = first + second
    return first / total, second / total


def middle_kernel(
    place, t0, t1, t2, t3, p0, p1, p2, p3, a0, a1, a2, a3, o0, o1, o2, o3, previous, routes,
    mid_out, rows_out, stats_out,
):
    row = place[0]
    size, span = t0.shape
    params = (p0, p1, p2, p3)
    kinds = previous.shape[0]
    square = jnp.zeros((1, span), F32)
    for j, ref in enumerate((t0, t1, t2, t3)):
        mid = ref[...].astype(F32)
        for k, (part, proj) in enumerate(((a0, o0), (a1, o1), (a2, o2), (a3, o3))):
            mid = mid + mm(proj[row ^ k ^ j], part[...], 1, 0)
        square = square + jnp.sum(mid * mid, axis=0, keepdims=True)
        mid_out[j * size : (j + 1) * size] = mid
    inverse = lax.rsqrt(square / (size * 4) + EPS)
    summed = jnp.zeros((128, span), F32)
    normed = []
    for j in range(4):
        norm = mid_out[j * size : (j + 1) * size] * inverse * column(params[j], GAIN2)
        summed = summed + mm(params[j][...].astype(F32), norm, 0, 0, HIGH)
        normed.append(norm)
    rows_out[:span] = jnp.transpose(jnp.concatenate(normed, axis=0)).astype(BF16)
    logits = summed[:kinds] + previous[...]
    _, chosen = route_rows(routes[...], logits)
    gates = pair_softmax(*chosen)
    rows_out[span:] = pack_rows(gates, rows_out.shape[1])
    alpha = [
        *pair_softmax(summed[12:13], summed[13:14]),
        *pair_softmax(summed[14:15], summed[15:16]),
    ]
    stats_out[...] = jnp.concatenate([*gates, inverse, *alpha, jnp.zeros((1, span), F32)], axis=0)


def param_spec(array):
    size, width = array.shape
    return pl.BlockSpec((size, PARAMS), lambda i, s: (0, width // PARAMS - 1))


def middle(place, toks, parts, projs, previous, routes):
    size = toks[0].shape[0]
    span = parts[0].shape[1]
    count = lax.axis_size("col")

    def whole(array):
        zeros = (0,) * array.ndim
        return pl.BlockSpec(array.shape, lambda i, s: zeros)

    args = (*toks, *toks, *parts, *projs, previous, routes)
    specs = [pl.BlockSpec((size, span), lambda i, s: (0, s[1])) for _ in toks]
    specs += [param_spec(a) for a in toks]
    specs += [whole(a) for a in (*parts, *projs)]
    specs += [
        pl.BlockSpec((previous.shape[0], span), lambda i, s: (0, s[1])),
        pl.BlockSpec((2, span), lambda i, s: (0, s[0] * count + s[1])),
    ]
    full = size * count
    return pl.pallas_call(
        middle_kernel,
        name="middle",
        cost_estimate=span_of(6),
        grid_spec=pltpu.PrefetchScalarGridSpec(
            num_scalar_prefetch=1,
            grid=(1,),
            in_specs=specs,
            out_specs=[
                pl.BlockSpec((full, span), lambda i, s: (0, 0)),
                pl.BlockSpec((span + EXTRA, full), lambda i, s: (0, 0)),
                pl.BlockSpec((8, span), lambda i, s: (0, 0)),
            ],
        ),
        out_shape=[
            jax.ShapeDtypeStruct((full, span), F32),
            jax.ShapeDtypeStruct((span + EXTRA, full), BF16),
            jax.ShapeDtypeStruct((8, span), F32),
        ],
        compiler_params=pltpu.CompilerParams(vmem_limit_bytes=VMEM_LIMIT),
    )(place, *args)


def middle_back_kernel(
    place, p0, p1, p2, p3, mid, grad, stats, routes, x0, x1, x2, x3,
    low_out, mid_out, logits_out, small_out,
):
    params = (p0, p1, p2, p3)
    full, span = mid.shape
    size = p0.shape[0]
    kinds = logits_out.shape[0]
    gates = [stats[0:1], stats[1:2]]
    inverse = stats[2:3]
    alpha = [stats[3:4], stats[4:5], stats[5:6], stats[6:7]]
    names = [routes[0:1], routes[1:2]]
    xs = (x0, x1, x2, x3)
    moe = jnp.transpose(sum(x[:span].astype(F32) for x in xs))
    ffn = [sum(unpack_row(x, span, span, k) for x in xs) for k in range(2)]
    flow = grad[...].astype(F32)
    normed = []
    dot_norm = jnp.zeros((1, span), F32)
    dot_value = [jnp.zeros((1, span), F32), jnp.zeros((1, span), F32)]
    for j in range(4):
        here = slice(j * size, (j + 1) * size)
        norm = mid[here] * inverse * column(params[j], GAIN2)
        dot_norm = dot_norm + jnp.sum(flow[here] * norm, axis=0, keepdims=True)
        for c, first in enumerate((VALUE0, VALUE1)):
            value = column(params[j], first)
            dot_value[c] = dot_value[c] + jnp.sum(flow[here] * value, axis=0, keepdims=True)
        normed.append(norm)
    experts = kinds - 4
    is_copy = [(name == experts + 1).astype(F32) for name in names]
    is_const = [[(name == experts + 2 + c).astype(F32) for name in names] for c in range(2)]
    grad_gate = []
    for k in range(2):
        value = ffn[k] + is_copy[k] * dot_norm
        for c in range(2):
            value = value + is_const[c][k] * (
                alpha[2 * c] * dot_norm + alpha[2 * c + 1] * dot_value[c]
            )
        grad_gate.append(value)
    shared = gates[0] * grad_gate[0] + gates[1] * grad_gate[1]
    chosen = [gates[k] * (grad_gate[k] - shared) for k in range(2)]
    places = lax.broadcasted_iota(jnp.int32, (kinds, span), 0)
    logits = jnp.where(places == names[0], chosen[0], 0.0) + jnp.where(
        places == names[1], chosen[1], 0.0
    )
    logits_out[...] = logits
    direct = gates[0] * is_copy[0] + gates[1] * is_copy[1]
    rows = [logits]
    portions = []
    for c in range(2):
        portion = gates[0] * is_const[c][0] + gates[1] * is_const[c][1]
        first, second = alpha[2 * c], alpha[2 * c + 1]
        along = [portion * dot_norm, portion * dot_value[c]]
        mean = first * along[0] + second * along[1]
        rows += [first * (along[0] - mean), second * (along[1] - mean)]
        direct = direct + first * portion
        portions.append(second * portion)
    rows.append(jnp.zeros((128 - kinds - 4, span), F32))
    routed = jnp.concatenate(rows, axis=0)
    lanes = lax.broadcasted_iota(jnp.int32, (size, 128), 1)
    backs = []
    inner = jnp.zeros((1, span), F32)
    for j in range(4):
        here = slice(j * size, (j + 1) * size)
        back = moe[here] + direct * flow[here] + mm(params[j][...].astype(F32), routed, 1, 0, HIGH)
        small = mm(normed[j], routed, 1, 1, HIGH)
        columns = (
            (SUM_GAIN2, mid[here] * inverse * back),
            (SUM_VALUE0, portions[0] * flow[here]),
            (SUM_VALUE1, portions[1] * flow[here]),
        )
        for lane, terms in columns:
            total = jnp.sum(terms, axis=1, keepdims=True)
            small = jnp.where(lanes == lane, total, small)
        small_out[j] = jnp.transpose(small)[:24]
        gain = column(params[j], GAIN2)
        inner = inner + jnp.sum(mid[here] * gain * back, axis=0, keepdims=True)
        backs.append(back)
    inner = inner * (inverse * inverse * inverse) / full
    for j in range(4):
        here = slice(j * size, (j + 1) * size)
        gain = column(params[j], GAIN2)
        value = flow[here] + inverse * gain * backs[j] - mid[here] * inner
        mid_out[here] = value
        low_out[here] = value.astype(BF16)


def middle_back(place, toks, mid, grad, stats, routes, pieces, kinds):
    full, span = mid.shape
    count = lax.axis_size("col")
    size = full // count

    def whole(array):
        zeros = (0,) * array.ndim
        return pl.BlockSpec(array.shape, lambda i, s: zeros)

    args = (*toks, mid, grad, stats, routes, *pieces)
    specs = [param_spec(a) for a in toks] + [whole(a) for a in args[len(toks) :]]
    specs[len(toks) + 3] = pl.BlockSpec((2, span), lambda i, s: (0, s[0] * count + s[1]))
    return pl.pallas_call(
        middle_back_kernel,
        name="middle_back",
        cost_estimate=span_of(7),
        grid_spec=pltpu.PrefetchScalarGridSpec(
            num_scalar_prefetch=1,
            grid=(1,),
            in_specs=specs,
            out_specs=[
                pl.BlockSpec((full, span), lambda i, s: (0, 0)),
                pl.BlockSpec((full, span), lambda i, s: (0, 0)),
                pl.BlockSpec((kinds, span), lambda i, s: (0, 0)),
                pl.BlockSpec((count, 24, size), lambda i, s: (0, 0, 0)),
            ],
        ),
        out_shape=[
            jax.ShapeDtypeStruct((full, span), BF16),
            jax.ShapeDtypeStruct((full, span), F32),
            jax.ShapeDtypeStruct((kinds, span), F32),
            jax.ShapeDtypeStruct((count, 24, size), F32),
        ],
        compiler_params=pltpu.CompilerParams(vmem_limit_bytes=VMEM_LIMIT),
    )(place, *args)


def result_kernel(place, p0, p1, p2, p3, mid, stats, routes, logits, y0, y1, y2, y3, out):
    params = (p0, p1, p2, p3)
    size = p0.shape[0]
    experts = place[3]
    inverse = stats[2:3]
    names = [routes[0:1], routes[1:2]]
    gates = [stats[0:1], stats[1:2]]

    def portion(kind):
        return jnp.where(names[0] == kind, gates[0], 0.0) + jnp.where(
            names[1] == kind, gates[1], 0.0
        )

    first, second = portion(experts + 2), portion(experts + 3)
    direct = portion(experts + 1) + first * stats[3:4] + second * stats[5:6]
    moe = y0[...].astype(F32) + y1[...].astype(F32) + y2[...].astype(F32) + y3[...].astype(F32)
    moe = jnp.transpose(moe)
    for j in range(4):
        here = slice(j * size, (j + 1) * size)
        norm = mid[here] * inverse * column(params[j], GAIN2)
        out[j, :size] = (
            mid[here]
            + moe[here]
            + direct * norm
            + first * stats[4:5] * column(params[j], VALUE0)
            + second * stats[6:7] * column(params[j], VALUE1)
        )
        out[j, size:] = jnp.concatenate(
            [logits[...], jnp.zeros((EXTRA - logits.shape[0], logits.shape[1]), F32)], axis=0
        )


def result(place, toks, mid, stats, routes, logits, pieces):
    full, span = mid.shape
    count = lax.axis_size("col")
    tall = full // count + EXTRA

    def whole(array):
        zeros = (0,) * array.ndim
        return pl.BlockSpec(array.shape, lambda i, s: zeros)

    args = (*toks, mid, stats, routes, logits, *pieces)
    specs = [param_spec(a) for a in toks] + [whole(a) for a in args[len(toks) :]]
    specs[len(toks) + 2] = pl.BlockSpec((2, span), lambda i, s: (0, s[0] * count + s[1]))
    return pl.pallas_call(
        result_kernel,
        name="result",
        cost_estimate=span_of(5),
        grid_spec=pltpu.PrefetchScalarGridSpec(
            num_scalar_prefetch=1,
            grid=(1,),
            in_specs=specs,
            out_specs=pl.BlockSpec((count, tall, span), lambda i, s: (0, 0, 0)),
        ),
        out_shape=jax.ShapeDtypeStruct((count, tall, span), F32),
        compiler_params=pltpu.CompilerParams(vmem_limit_bytes=VMEM_LIMIT),
    )(place, *args)


def experts_kernel(chunks, last, *refs):
    order, x0, x1, x2, x3, g0, g1, g2, g3, ranks, routes, w0, w1 = refs[:13]
    refs = refs[13:]
    twos, refs = refs[: len(chunks)], refs[len(chunks) :]
    threes, refs = refs[: len(chunks)], refs[len(chunks) :]
    if last:
        y_in, dx_in, gate_in = refs[:3]
        refs = refs[3:]
    y_out, dx_out = refs[:2]
    refs = refs[2:]
    if not last:
        gate_out = refs[0]
        refs = refs[1:]
    grad_mine, grad_next, weight, y_acc, dx_acc, gate_sum, gate_rows, acc = refs
    step = pl.program_id(0)
    steps = pl.num_programs(0)
    expert = order[step]
    tiles = order[steps + step]
    size = w0.shape[1]
    tokens = ranks.shape[1]
    span = tokens // 4
    full = x0.shape[1]
    hidden_width = w0.shape[2] // 3
    both = 2 * hidden_width
    xs = (x0, x1, x2, x3)
    gs = (g0, g1, g2, g3)

    @pl.when(step == 0)
    def _():
        if last:
            y_acc[...] = y_in[...]
            dx_acc[...] = dx_in[...]
            gate_sum[...] = gate_in[...]
        else:
            y_acc[...] = jnp.zeros_like(y_acc)
            dx_acc[...] = jnp.zeros_like(dx_acc)
            gate_sum[...] = jnp.zeros_like(gate_sum)
        for i, ref in enumerate(xs):
            for k in range(2):
                gate_rows[k : k + 1, i * span : (i + 1) * span] = unpack_row(ref, span, span, k)

    weight[:size] = w0[0]
    weight[size : 2 * size] = w1[0]
    start = 0
    for two, three, count in zip(twos, threes, chunks):

        @pl.when((step >= start) & (step < start + count))
        def _():
            weight[2 * size : 3 * size] = two[0]
            weight[3 * size :] = three[0]

        start += count

    rank = ranks[pl.ds(expert, 1), :]
    hit0 = routes[0:1] == expert
    hit1 = routes[1:2] == expert
    gate_row = jnp.where(hit0, gate_rows[0:1], 0.0) + jnp.where(hit1, gate_rows[1:2], 0.0)

    def tile(index, carry):
        slots = lax.broadcasted_iota(jnp.int32, (TILE, tokens), 0) + index * TILE
        hot = slots == rank
        pick = hot.astype(F32).astype(BF16)
        gate = jnp.sum(jnp.where(hot, gate_row, 0.0), axis=1, keepdims=True)
        rows = jnp.zeros((TILE, full), F32)
        flow = jnp.zeros((TILE, full), F32)
        for i in range(4):
            cut = pick[:, i * span : (i + 1) * span]
            rows = rows + mm(cut, xs[i][:span], 1, 0)
            flow = flow + mm(cut, gs[i][...], 1, 0)
        rows = rows.astype(BF16)
        flow = flow.astype(BF16)
        gate_up = mm(rows, weight[:, :both], 1, 0)
        pre = gate_up[:, :hidden_width]
        up = gate_up[:, hidden_width:]
        sigma = 1.0 / (1.0 + jnp.exp(-pre))
        lifted = pre * sigma
        hidden = lifted * up
        scaled = (hidden * gate).astype(BF16)
        back = mm(flow, weight[:, both:], 1, 0)
        grad_gate = jnp.sum(hidden * back, axis=1, keepdims=True)
        back = back * gate
        grad_pre = back * up * sigma * (1.0 + pre * (1.0 - sigma))
        grad_up = back * lifted
        grad_both = jnp.concatenate([grad_pre.astype(BF16), grad_up.astype(BF16)], axis=1)
        y = mm(scaled, weight[:, both:], 1, 1).astype(BF16)
        dx = mm(grad_both, weight[:, :both], 1, 1).astype(BF16)
        for i in range(4):
            cut = pick[:, i * span : (i + 1) * span]
            y_acc[i * span : (i + 1) * span] += mm(cut, y, 0, 0)
            dx_acc[i * span : (i + 1) * span] += mm(cut, dx, 0, 0)
        row = jnp.sum(jnp.where(hot, grad_gate, 0.0), axis=0, keepdims=True)
        gate_sum[0:1] += jnp.where(hit0, row, 0.0)
        gate_sum[1:2] += jnp.where(hit1, row, 0.0)
        grad_weight = mm(rows, grad_both, 0, 0)
        grad_down = mm(flow, scaled, 0, 0)

        @pl.when(index == 0)
        def _():
            acc[:, :both] = grad_weight
            acc[:, both:] = grad_down

        @pl.when(index > 0)
        def _():
            acc[:, :both] += grad_weight
            acc[:, both:] += grad_down

        return carry

    lax.fori_loop(0, tiles, tile, 0)
    for k in range(4):
        ref = grad_next if k % 2 else grad_mine
        ref[k // 2, 0] = acc[k * size : (k + 1) * size].astype(BF16)

    @pl.when(step == steps - 1)
    def _():
        if last:
            for i in range(4):
                here = slice(i * span, (i + 1) * span)
                y_out[i] = y_acc[here].astype(BF16)
                dx_out[i, :span] = dx_acc[here].astype(BF16)
                rows = [gate_sum[0:1, here], gate_sum[1:2, here]]
                dx_out[i, span:] = pack_rows(rows, full)
        else:
            y_out[...] = y_acc[...]
            dx_out[...] = dx_acc[...]
            gate_out[...] = gate_sum[...]


def run_experts(order, xs, gs, ranks, routes, w0, w1, twos, threes, carried):
    size, wide = w0.shape[1:]
    tokens = ranks.shape[1]
    span = tokens // 4
    full = xs[0].shape[1]
    chunks = tuple(a.shape[0] for a in twos)
    steps = sum(chunks)
    last = carried is not None

    def whole(shape):
        zeros = (0,) * len(shape)
        return pl.BlockSpec(shape, lambda e, s: zeros)

    def chunk(start, count):
        return pl.BlockSpec(
            (1, size, wide), lambda e, s: (jnp.clip(e - start, 0, count - 1), 0, 0)
        )

    mine = pl.BlockSpec((1, size, wide), lambda e, s: (s[e], 0, 0))
    pieces = [chunk(sum(chunks[:i]), count) for i, count in enumerate(chunks)]
    args = (*xs, *gs, ranks, routes, w0, w1, *twos, *threes)
    specs = [whole(a.shape) for a in args[:10]] + [mine, mine] + pieces + pieces
    if last:
        args += tuple(carried)
        specs += [whole(a.shape) for a in carried]
        shapes = [((4, span, full), BF16), ((4, span + EXTRA, full), BF16)]
    else:
        shapes = [((tokens, full), F32), ((tokens, full), F32), ((8, tokens), F32)]
    grad = pl.BlockSpec((2, 1, size, wide), lambda e, s: (0, e, 0, 0))

    def body(*refs):
        experts_kernel(chunks, last, *refs)

    return pl.pallas_call(
        body,
        name="experts",
        cost_estimate=span_of(36),
        grid_spec=pltpu.PrefetchScalarGridSpec(
            num_scalar_prefetch=1,
            grid=(steps,),
            in_specs=specs,
            out_specs=[whole(shape) for shape, _ in shapes] + [grad] * 2,
            scratch_shapes=[
                pltpu.VMEM((full, wide), BF16),
                pltpu.VMEM((tokens, full), F32),
                pltpu.VMEM((tokens, full), F32),
                pltpu.VMEM((8, tokens), F32),
                pltpu.VMEM((8, tokens), F32),
                pltpu.VMEM((full, wide), F32),
            ],
        ),
        out_shape=[jax.ShapeDtypeStruct(shape, dtype) for shape, dtype in shapes]
        + [jax.ShapeDtypeStruct((2, steps, size, wide), BF16)] * 2,
        compiler_params=pltpu.CompilerParams(vmem_limit_bytes=VMEM_LIMIT),
    )(order, *args)


def shards(
    tokens,
    prev_logits,
    routes,
    prefix_len,
    norm1_gain,
    qkv_weight,
    out_weight,
    norm2_gain,
    router_weight,
    const_weight,
    const_values,
    gate_weight,
    up_weight,
    down_weight,
    cotangent,
):
    row = lax.axis_index("row")
    col = lax.axis_index("col")
    rows = lax.axis_size("row")
    cols = lax.axis_size("col")
    groups = lax.axis_size("dp")
    length, size = tokens.shape
    span = length // cols
    kinds = router_weight.shape[1]
    experts = gate_weight.shape[0]
    half = experts // 2
    hidden_width = gate_weight.shape[2]
    first_half = lax.axis_index("dp") if groups == 2 else jnp.int32(0)
    prefix = lax.dynamic_index_in_dim(prefix_len, row, 0, False)
    place = jnp.stack([row, col, prefix, jnp.int32(experts)]).astype(jnp.int32)
    flat = [(i // cols, i % cols) for i in range(rows * cols)]

    def spread(value, turn):
        pairs = [(c * cols + (c ^ r ^ turn), r * cols + c) for r, c in flat]
        return lax.ppermute(value, ("row", "col"), pairs)

    def collect(value, turn):
        pairs = [(r * cols + c, c * cols + (r ^ turn)) for r, c in flat]
        return lax.ppermute(value, ("row", "col"), pairs)

    def across_groups(value):
        return lax.ppermute(value, "dp", [(0, 1), (1, 0)])


    values = [norm1_gain, norm2_gain, const_values[0], const_values[1]]
    lanes = [router_weight, const_weight]
    for value in values:
        lanes += [part[:, None] for part in parts_of(value)]
    lanes.append(jnp.zeros((size, PARAMS - kinds - 4 - 3 * len(values)), BF16))
    piece = jnp.concatenate([qkv_weight[0], qkv_weight[1], qkv_weight[2], out_weight.T], axis=1)
    toks = col_gather(jnp.concatenate([tokens.T] + lanes, axis=1))
    weight = jnp.stack([spread(piece, m) for m in range(rows)])
    halves = HD // 2
    freq = 10000.0 ** (-jnp.arange(halves, dtype=F32) / halves)
    angle = freq[:, None] * jnp.arange(length, dtype=F32)[None, :]
    cosine = jnp.cos(angle)
    sine = jnp.sin(angle)

    flow = after(cotangent.T, toks[2]).reshape(size, cols, span)
    flow_parts = [lax.dynamic_index_in_dim(flow, col ^ k, 1, False) for k in range(cols)]
    flow_quarter = jnp.concatenate(
        [flow_parts[0]] + [col_swap(flow_parts[k], k) for k in range(1, cols)], axis=0
    )
    flow_rows = row_gather(flow_quarter.T)

    own = jnp.concatenate([gate_weight, up_weight, down_weight.transpose(0, 2, 1)], axis=2)
    near_own = lax.dynamic_slice_in_dim(own, first_half * half, half, 0)
    pair = half // 2
    two_a = col_swap(after(near_own[:pair], flow_quarter), 2)
    side = col_swap(after(own, weight), 1)
    projs = col_gather(after(weight[:, :, 3 * size :], toks[2]))

    routes_t = routes.T
    share = lax.dynamic_index_in_dim(routes_t.reshape(2, rows, cols, span), col, 2, False)
    turned = (row - jnp.arange(rows)) % rows
    share = jnp.take(share, turned, axis=1).reshape(2, rows * span)
    ids = jnp.arange(experts, dtype=jnp.int32)[:, None]
    hits = (share[0][None] == ids) | (share[1][None] == ids)
    counts = jnp.cumsum(hits.astype(jnp.int32), axis=1)
    ranks = jnp.where(hits, counts - 1, -1)
    order = (first_half * half + jnp.arange(experts, dtype=jnp.int32)) % experts
    tiles = jnp.take(jnp.maximum((counts[:, -1] + TILE - 1) // TILE, 1), order)
    order_near = jnp.concatenate([order[:half], tiles[:half]]).astype(jnp.int32)
    order_far = jnp.concatenate([order[half:], tiles[half:]]).astype(jnp.int32)

    query, keys, values, attn, logsum = attend(place, toks, weight, cosine, sine)
    attn, two_a, flow_rows, projs, side = join(attn, two_a, flow_rows, projs, side)
    parts = [attn[0]] + [col_swap(attn[k], k) for k in range(1, cols)]
    two_b = col_swap(after(near_own[pair:], parts[1], parts[2], parts[3]), 2)
    if groups == 2:
        far_two_a = across_groups(two_a)
        far_two_b = across_groups(two_b)
    else:
        far_two_a = col_swap(own[half : half + pair], 2)
        far_two_b = col_swap(after(own[half + pair :], two_b), 2)
    mid, in_rows, stats = middle(place, toks, parts, projs, prev_logits.T, routes_t)
    x_rows = row_gather(in_rows)
    three_a = col_swap(after(two_a, parts[1], parts[2], parts[3]), 1)
    three_b = col_swap(after(two_b, mid), 1)
    far_three_a = col_swap(after(far_two_a, mid), 1)
    far_three_b = col_swap(far_two_b, 1)
    x_rows, far_two_a, far_three_a = join(x_rows, far_two_a, far_three_a)

    near_out = run_experts(
        order_near, x_rows, flow_rows, ranks, share, own, side,
        [two_a, two_b], [three_a, three_b], None,
    )
    *carried, near_mine, near_next = near_out
    near_next = col_swap(near_next, 1)
    y, dx, far_mine, far_next = run_experts(
        order_far, x_rows, flow_rows, ranks, share, own, side,
        [far_two_a, far_two_b], [far_three_a, far_three_b], carried,
    )

    def low_sum(left, right):
        return (left.astype(F32) + right.astype(F32)).astype(BF16)

    def row_scatter(value):
        return [value[0]] + [row_shift(value[s], -s) for s in range(1, rows)]

    def across_sums(sums):
        return [across_groups(s) for s in sums] if groups == 2 else sums

    near_next, dx, far_mine, far_next = join(near_next, dx, far_mine, far_next)
    dx = row_scatter(dx)
    near_kept, near_sent = low_sum(near_mine[0], near_next[0]), low_sum(near_mine[1], near_next[1])
    near_got = [col_swap(near_sent[:pair], 2), col_swap(after(near_sent[pair:], dx[1]), 2)]
    far_next = col_swap(far_next, 1)
    low, grad_mid, grad_logits, small = middle_back(
        place, toks, mid, flow_quarter, stats, routes_t, dx, kinds
    )
    near_sum = [low_sum(near_kept[:pair], near_got[0]), low_sum(near_kept[pair:], near_got[1])]
    near_other = across_sums(near_sum)
    lows = col_gather(low)
    lows, near_sum, near_other[0], far_next = join(lows, near_sum, near_other[0], far_next)

    y = row_scatter(after(y, dx[1], dx[2], dx[3]))
    far_kept, far_sent = low_sum(far_mine[0], far_next[0]), low_sum(far_mine[1], far_next[1])
    far_got = [col_swap(far_sent[:pair], 2), col_swap(far_sent[pair:], 2)]
    far_sum = [low_sum(far_kept[:pair], far_got[0]), low_sum(far_kept[pair:], far_got[1])]
    far_other = across_sums(far_sum)
    tokens_parts, weight_parts, small = attend_back(
        place, toks, weight, cosine, sine,
        query, keys, values, attn, logsum, lows, grad_mid, small,
    )
    tokens_parts, weight_parts, small, y, near_other, far_got[0] = join(
        tokens_parts, weight_parts, small, y, near_other, far_got[0]
    )
    out = result(place, toks, mid, stats, routes_t, grad_logits, y)
    tokens_parts, far_got[1] = join(tokens_parts, far_got[1])

    def col_scatter(value):
        total = value[0].astype(F32)
        for k in range(1, cols):
            total = total + col_swap(value[k], k).astype(F32)
        return total

    small = row_total(col_scatter(small))
    total = collect(weight_parts[0], 0).astype(F32)
    for m in range(1, rows):
        total = total + collect(weight_parts[m], m).astype(F32)
    small, total = dp_total(small), dp_total(total.astype(BF16))
    grad_tokens = col_scatter(tokens_parts)
    qkv_sum = jnp.stack([total[:, j * size : (j + 1) * size] for j in range(3)])
    proj_sum = total[:, 3 * size :].T
    out = jnp.stack([out[0]] + [col_swap(out[k], k) for k in range(1, cols)])
    out = jnp.take(out, col ^ jnp.arange(cols), axis=0)
    out = jnp.concatenate([out[i] for i in range(cols)], axis=1)
    if groups == 2:
        near_start = first_half * half
        far_start = half - near_start
        grads = []
        for j in range(3):
            wide = slice(j * hidden_width, (j + 1) * hidden_width)
            grad = jnp.zeros((experts, size, hidden_width), F32)
            for i in range(2):
                for start, mine, other in (
                    (near_start, near_sum[i], far_other[i]),
                    (far_start, far_sum[i], near_other[i]),
                ):
                    both = mine[:, :, wide].astype(F32) + other[:, :, wide].astype(F32)
                    grad = lax.dynamic_update_slice_in_dim(grad, both, start + i * pair, 0)
            grads.append(grad)
    else:
        both = lax.psum(jnp.concatenate(near_sum + far_sum).astype(F32), "dp")
        grads = [both[:, :, j * hidden_width : (j + 1) * hidden_width] for j in range(3)]

    return (
        out[:size].T,
        grad_tokens.T,
        out[size : size + kinds].T,
        small[SUM_GAIN1],
        qkv_sum,
        proj_sum,
        small[SUM_GAIN2],
        small[:kinds].T,
        small[kinds : kinds + 4].T,
        small[SUM_VALUE0 : SUM_VALUE1 + 1],
        grads[0],
        grads[1],
        grads[2].transpose(0, 2, 1),
    )


def solution(mesh):
    return jax.shard_map(
        shards,
        mesh=mesh,
        in_specs=(
            P(("dp", "row"), "col"),
            P(("dp", "row"), None),
            P("dp", None),
            P("dp"),
            P("col"),
            P(None, "col", "row"),
            P("row", "col"),
            P("col"),
            P("col", None),
            P("col", None),
            P(None, "col"),
            P(None, "col", "row"),
            P(None, "col", "row"),
            P(None, "row", "col"),
            P(("dp", "row"), "col"),
        ),
        out_specs=(
            P(("dp", "row"), "col"),
            P(("dp", "row"), "col"),
            P(("dp", "row"), None),
            P("col"),
            P(None, "col", "row"),
            P("row", "col"),
            P("col"),
            P("col", None),
            P("col", None),
            P(None, "col"),
            P(None, "col", "row"),
            P(None, "col", "row"),
            P(None, "row", "col"),
        ),
        check_vma=False,
    )
```

```python
import jax
import jax.numpy as jnp
from jax import lax
from jax.experimental import pallas as pl
from jax.experimental.pallas import tpu as pltpu
from jax.sharding import PartitionSpec as P

HD = 64
LEN = 1024
EPS = 1e-06
HIGH = lax.Precision.HIGHEST
NEGATIVE = -1e30
TILE = 256
VMEM_LIMIT = 60 * 1024 * 1024
F32 = jnp.float32
BF16 = jnp.bfloat16
PARAMS = 128
GAIN1, GAIN2, VALUE0, VALUE1 = 16, 19, 22, 25
SUM_GAIN2, SUM_VALUE0, SUM_VALUE1, SUM_GAIN1 = 16, 17, 18, 19
EXTRA = 16
SMALL = 24


def mm(left, right, over_left, over_right, precision=None):
    return lax.dot_general(
        left,
        right,
        (((over_left,), (over_right,)), ((), ())),
        preferred_element_type=F32,
        precision=precision,
    )


def parts_of(value):
    high = lax.reduce_precision(value, 8, 7)
    middle = lax.reduce_precision(value - high, 8, 7)
    return [high.astype(BF16), middle.astype(BF16), (value - high - middle).astype(BF16)]


def column(params, first):
    low = params[:, first : first + 3].astype(F32)
    return low[:, 0:1] + low[:, 1:2] + low[:, 2:3]


def pack_rows(rows, width):
    out = []
    for row in rows:
        high = row.astype(BF16).astype(F32)
        middle = (row - high).astype(BF16).astype(F32)
        out += [high, middle, row - high - middle]
    out.append(jnp.zeros((EXTRA - len(out), rows[0].shape[1]), F32))
    packed = jnp.concatenate(out, axis=0)
    rest = jnp.zeros((EXTRA, width - packed.shape[1]), F32)
    return jnp.concatenate([packed, rest], axis=1).astype(BF16)


def parts_in_rows(value, height):
    high = value.astype(BF16).astype(F32)
    middle = (value - high).astype(BF16).astype(F32)
    rest = jnp.zeros((height - 3 * value.shape[0], value.shape[1]), F32)
    return jnp.concatenate([high, middle, value - high - middle, rest], axis=0)


def unpack_row(ref, base, span, k):
    parts = ref[base : base + EXTRA, :span].astype(F32)
    return parts[3 * k : 3 * k + 1] + parts[3 * k + 1 : 3 * k + 2] + parts[3 * k + 2 : 3 * k + 3]


def span_of(micros):
    return pl.CostEstimate(
        flops=int(micros * 1.1e9), transcendentals=0, bytes_accessed=int(micros * 3.6e6)
    )


def after(value, *others):
    return lax.optimization_barrier((value,) + others)[0]


def join(*values):
    return lax.optimization_barrier(values)


def col_swap(value, bits):
    count = lax.axis_size("col")
    return lax.ppermute(value, "col", [(i, i ^ bits) for i in range(count)])


def row_swap(value, bits):
    count = lax.axis_size("row")
    return lax.ppermute(value, "row", [(i, i ^ bits) for i in range(count)])


def row_shift(value, steps):
    count = lax.axis_size("row")
    return lax.ppermute(value, "row", [(i, (i + steps) % count) for i in range(count)])


def col_gather(value):
    count = lax.axis_size("col")
    found = {0: value}
    bit = count // 2
    while bit:
        found.update({k | bit: col_swap(v, bit) for k, v in found.items()})
        bit //= 2
    return [found[k] for k in range(count)]


def row_gather(value):
    count = lax.axis_size("row")
    return [value] + [row_shift(value, s) for s in range(1, count)]


def dp_total(value):
    count = lax.axis_size("dp")
    if count == 2:
        other = lax.ppermute(value, "dp", [(0, 1), (1, 0)])
        return value.astype(F32) + other.astype(F32)
    return lax.psum(value.astype(F32), "dp")


def row_total(value):
    bit = 1
    while bit < lax.axis_size("row"):
        value = value + row_swap(value, bit)
        bit *= 2
    return value


def rotate_halves(block, cosine, sine):
    half = HD // 2
    out = []
    for head in range(block.shape[0] // HD):
        first = block[head * HD : head * HD + half]
        second = block[head * HD + half : (head + 1) * HD]
        out.append(first * cosine - second * sine)
        out.append(second * cosine + first * sine)
    return jnp.concatenate(out, axis=0)


def attend_kernel(
    place, t0, t1, t2, t3, weight, cosine, sine,
    query_out, key_out, value_out, attn_out, logsum_out, act, w_all,
):
    block = pl.program_id(0)
    row = place[0]
    prefix = place[2]
    size = t0.shape[0]
    heads = query_out.shape[1] // HD
    width = heads * HD
    count = query_out.shape[0]
    span = query_out.shape[2]
    length = key_out.shape[1]

    @pl.when(block == 0)
    def _():
        square = jnp.zeros((1, length), F32)
        for ref in (t0, t1, t2, t3):
            hidden = ref[:, :length].astype(F32)
            square = square + jnp.sum(hidden * hidden, axis=0, keepdims=True)
        inverse = lax.rsqrt(square / (size * 4) + EPS)
        for k, ref in enumerate((t0, t1, t2, t3)):
            gain = column(ref[:, length:], GAIN1)
            hidden = ref[:, :length].astype(F32)
            act[k * size : (k + 1) * size] = (hidden * inverse * gain).astype(BF16)
            w_all[k * size : (k + 1) * size] = weight[row ^ k, :, : 3 * width]
        qkv = mm(w_all[...], act[...], 0, 0)
        query = rotate_halves(qkv[:width], cosine[...], sine[...]).astype(BF16)
        keys = rotate_halves(qkv[width : 2 * width], cosine[...], sine[...]).astype(BF16)
        for i in range(count):
            query_out[i] = query[:, i * span : (i + 1) * span]
        key_out[...] = keys
        value_out[...] = qkv[2 * width :].astype(BF16)

    places = lax.broadcasted_iota(jnp.int32, (length, span), 0)
    mine = lax.broadcasted_iota(jnp.int32, (1, span), 1) + block * span
    seen = places <= jnp.maximum(mine, prefix - 1)
    rows = []
    for head in range(heads):
        cut = slice(head * HD, (head + 1) * HD)
        query = (query_out[block, cut].astype(F32) * HD ** (-0.5)).astype(BF16)
        scores = jnp.where(seen, mm(key_out[cut], query, 0, 0), NEGATIVE)
        top = jnp.max(scores, axis=0, keepdims=True)
        weights = jnp.exp(scores - top)
        total = jnp.sum(weights, axis=0, keepdims=True)
        mixed = mm(value_out[cut], weights.astype(BF16), 1, 0)
        attn_out[0, cut] = (mixed / total).astype(BF16)
        rows.append(top + jnp.log(total))
    rows.append(jnp.zeros((8 - heads, span), F32))
    logsum_out[...] = jnp.concatenate(rows, axis=0)


def attend(place, toks, weight, cosine, sine):
    size = toks[0].shape[0]
    length = cosine.shape[1]
    count = lax.axis_size("col")
    span = length // count
    width = weight.shape[2] // 4

    def whole(array):
        zeros = (0,) * array.ndim
        return pl.BlockSpec(array.shape, lambda q, s: zeros)

    args = (*toks, weight, cosine, sine)
    return pl.pallas_call(
        attend_kernel,
        name="attend",
        cost_estimate=span_of(14),
        grid_spec=pltpu.PrefetchScalarGridSpec(
            num_scalar_prefetch=1,
            grid=(count,),
            in_specs=[whole(a) for a in args],
            out_specs=[
                pl.BlockSpec((count, width, span), lambda q, s: (0, 0, 0)),
                pl.BlockSpec((width, length), lambda q, s: (0, 0)),
                pl.BlockSpec((width, length), lambda q, s: (0, 0)),
                pl.BlockSpec((1, width, span), lambda q, s: (q ^ s[1], 0, 0)),
                pl.BlockSpec((8, span), lambda q, s: (0, q)),
            ],
            scratch_shapes=[
                pltpu.VMEM((size * count, length), BF16),
                pltpu.VMEM((size * count, 3 * width), BF16),
            ],
        ),
        out_shape=[
            jax.ShapeDtypeStruct((count, width, span), BF16),
            jax.ShapeDtypeStruct((width, length), BF16),
            jax.ShapeDtypeStruct((width, length), BF16),
            jax.ShapeDtypeStruct((count, width, span), BF16),
            jax.ShapeDtypeStruct((8, length), F32),
        ],
        compiler_params=pltpu.CompilerParams(vmem_limit_bytes=VMEM_LIMIT),
    )(place, *args)


def attend_back_kernel(
    place, t0, t1, t2, t3, weight, cosine, sine,
    query, keys, values, attn, logsum, d0, d1, d2, d3, grad_mid, small,
    tokens_out, weight_out,
    dmid, proj_all, proj_acc, key_acc, value_acc, grad_all,
):
    block = pl.program_id(0)
    row = place[0]
    col = place[1]
    prefix = place[2]
    size = t0.shape[0]
    length = cosine.shape[1]
    count, width, span = query.shape
    heads = width // HD
    last = count - 1

    @pl.when(block == 0)
    def _():
        for k in range(count):
            proj_all[k * size : (k + 1) * size] = weight[row ^ k, :, 3 * width :]
        proj_acc[...] = jnp.zeros_like(proj_acc)
        key_acc[...] = jnp.zeros_like(key_acc)
        value_acc[...] = jnp.zeros_like(value_acc)

    for k, ref in enumerate((d0, d1, d2, d3)):

        @pl.when((block ^ col) == k)
        def _():
            for j in range(count):
                dmid[j * size : (j + 1) * size] = ref[(k ^ j) * size : ((k ^ j) + 1) * size]

    low = dmid[...]
    grad_attn = mm(proj_all[...], low, 0, 0).astype(BF16)
    proj_acc[...] += mm(low, attn[0], 1, 1)
    places = lax.broadcasted_iota(jnp.int32, (length, span), 0)
    mine = lax.broadcasted_iota(jnp.int32, (1, span), 1) + block * span
    seen = places <= jnp.maximum(mine, prefix - 1)
    scale = HD ** (-0.5)
    parts = []
    for head in range(heads):
        cut = slice(head * HD, (head + 1) * HD)
        plain = query[block, cut]
        scaled = (plain.astype(F32) * scale).astype(BF16)
        scores = mm(keys[cut], scaled, 0, 0)
        probs = jnp.where(seen, jnp.exp(scores - logsum[head : head + 1]), 0.0)
        above = grad_attn[cut]
        grad_probs = mm(values[cut], above, 0, 0)
        inner = jnp.sum(probs * grad_probs, axis=0, keepdims=True)
        grad_scores = (probs * (grad_probs - inner)).astype(BF16)
        parts.append(mm(keys[cut], grad_scores, 1, 0) * scale)
        key_acc[cut] += mm(plain, grad_scores, 1, 1)
        value_acc[cut] += mm(above, probs.astype(BF16), 1, 1)
    for i in range(count):

        @pl.when(block == i)
        def _():
            here = slice(i * span, (i + 1) * span)
            turned = rotate_halves(
                jnp.concatenate(parts, axis=0), cosine[:, here], -sine[:, here]
            )
            grad_all[:width, here] = turned.astype(BF16)

    @pl.when(block == last)
    def _():
        turned = rotate_halves(key_acc[...] * scale, cosine[...], -sine[...])
        grad_all[width : 2 * width] = turned.astype(BF16)
        grad_all[2 * width :] = value_acc[...].astype(BF16)
        refs = (t0, t1, t2, t3)
        gains = [column(ref[:, length:], GAIN1) for ref in refs]
        square = jnp.zeros((1, length), F32)
        for ref in refs:
            hidden = ref[:, :length].astype(F32)
            square = square + jnp.sum(hidden * hidden, axis=0, keepdims=True)
        inverse = lax.rsqrt(square / (size * count) + EPS)
        backs = []
        inner = jnp.zeros((1, length), F32)
        for k in range(count):
            hidden = refs[k][:, :length].astype(F32)
            act = (hidden * inverse * gains[k]).astype(BF16)
            weight_out[row ^ col ^ k, :, : 3 * width] = mm(act, grad_all[...], 1, 1).astype(BF16)
            weight_out[row ^ col ^ k, :, 3 * width : 4 * width] = proj_acc[
                k * size : (k + 1) * size
            ].astype(BF16)
            back = mm(weight[row ^ k, :, : 3 * width], grad_all[...], 1, 0)
            inner = inner + jnp.sum(hidden * gains[k] * back, axis=0, keepdims=True)
            summed = jnp.sum(hidden * inverse * back, axis=1, keepdims=True)
            turned = jnp.transpose(jnp.broadcast_to(summed, (size, 128)))[: small.shape[1]]
            places = lax.broadcasted_iota(jnp.int32, turned.shape, 0)
            rows = parts_in_rows(jnp.where(places == SUM_GAIN1, turned, small[k]), PARAMS)
            weight_out[row ^ col ^ k, :, 4 * width :] = jnp.transpose(rows).astype(BF16)
            backs.append(back)
        inner = inner * (inverse * inverse * inverse) / (size * count)
        for k in range(count):
            hidden = refs[k][:, :length].astype(F32)
            grad = inverse * gains[k] * backs[k] - hidden * inner
            for i in range(count):
                here = slice(i * span, (i + 1) * span)
                extra = jnp.where(col == i, grad_mid[k * size : (k + 1) * size], 0.0)
                tokens_out[k, :, here] = (grad[:, here] + extra).astype(BF16)


def attend_back(
    place, toks, weight, cosine, sine, query, keys, values, attn, logsum, lows, grad_mid, small
):
    size = toks[0].shape[0]
    length = cosine.shape[1]
    count, width, span = query.shape

    def whole(array):
        zeros = (0,) * array.ndim
        return pl.BlockSpec(array.shape, lambda q, s: zeros)

    args = (
        *toks, weight, cosine, sine, query, keys, values, attn, logsum, *lows, grad_mid, small,
    )
    specs = [whole(a) for a in args]
    at = len(toks) + 3 + 3
    specs[at] = pl.BlockSpec((1, width, span), lambda q, s: (q ^ s[1], 0, 0))
    specs[at + 1] = pl.BlockSpec((8, span), lambda q, s: (0, q))
    return pl.pallas_call(
        attend_back_kernel,
        name="attend_back",
        cost_estimate=span_of(24),
        grid_spec=pltpu.PrefetchScalarGridSpec(
            num_scalar_prefetch=1,
            grid=(count,),
            in_specs=specs,
            out_specs=[
                pl.BlockSpec((count, size, length), lambda q, s: (0, 0, 0)),
                pl.BlockSpec((count, size, 4 * width + PARAMS), lambda q, s: (0, 0, 0)),
            ],
            scratch_shapes=[
                pltpu.VMEM((size * count, span), BF16),
                pltpu.VMEM((size * count, width), BF16),
                pltpu.VMEM((size * count, width), F32),
                pltpu.VMEM((width, length), F32),
                pltpu.VMEM((width, length), F32),
                pltpu.VMEM((3 * width, length), BF16),
            ],
        ),
        out_shape=[
            jax.ShapeDtypeStruct((count, size, length), BF16),
            jax.ShapeDtypeStruct((count, size, 4 * width + PARAMS), BF16),
        ],
        compiler_params=pltpu.CompilerParams(vmem_limit_bytes=VMEM_LIMIT),
    )(place, *args)


def route_rows(routes, logits):
    places = lax.broadcasted_iota(jnp.int32, logits.shape, 0)
    hots = [places == routes[k : k + 1] for k in range(2)]
    return hots, [jnp.sum(jnp.where(hot, logits, 0.0), axis=0, keepdims=True) for hot in hots]


def pair_softmax(first, second):
    top = jnp.maximum(first, second)
    first = jnp.exp(first - top)
    second = jnp.exp(second - top)
    total = first + second
    return first / total, second / total


def middle_kernel(
    place, t0, t1, t2, t3, p0, p1, p2, p3, a0, a1, a2, a3, o0, o1, o2, o3, previous, routes,
    mid_out, rows_out, stats_out,
):
    row = place[0]
    size, span = t0.shape
    params = (p0, p1, p2, p3)
    kinds = previous.shape[0]
    square = jnp.zeros((1, span), F32)
    for j, ref in enumerate((t0, t1, t2, t3)):
        mid = ref[...].astype(F32)
        for k, (part, proj) in enumerate(((a0, o0), (a1, o1), (a2, o2), (a3, o3))):
            mid = mid + mm(proj[row ^ k ^ j], part[...], 1, 0)
        square = square + jnp.sum(mid * mid, axis=0, keepdims=True)
        mid_out[j * size : (j + 1) * size] = mid
    inverse = lax.rsqrt(square / (size * 4) + EPS)
    summed = jnp.zeros((128, span), F32)
    normed = []
    for j in range(4):
        norm = mid_out[j * size : (j + 1) * size] * inverse * column(params[j], GAIN2)
        summed = summed + mm(params[j][...].astype(F32), norm, 0, 0, HIGH)
        normed.append(norm)
    rows_out[:span] = jnp.transpose(jnp.concatenate(normed, axis=0)).astype(BF16)
    logits = summed[:kinds] + previous[...]
    _, chosen = route_rows(routes[...], logits)
    gates = pair_softmax(*chosen)
    rows_out[span:] = pack_rows(gates, rows_out.shape[1])
    alpha = [
        *pair_softmax(summed[12:13], summed[13:14]),
        *pair_softmax(summed[14:15], summed[15:16]),
    ]
    stats_out[...] = jnp.concatenate([*gates, inverse, *alpha, jnp.zeros((1, span), F32)], axis=0)


def param_spec(array):
    size, width = array.shape
    return pl.BlockSpec((size, PARAMS), lambda i, s: (0, width // PARAMS - 1))


def middle(place, toks, parts, projs, previous, routes):
    size = toks[0].shape[0]
    span = parts[0].shape[1]
    count = lax.axis_size("col")

    def whole(array):
        zeros = (0,) * array.ndim
        return pl.BlockSpec(array.shape, lambda i, s: zeros)

    args = (*toks, *toks, *parts, *projs, previous, routes)
    specs = [pl.BlockSpec((size, span), lambda i, s: (0, s[1])) for _ in toks]
    specs += [param_spec(a) for a in toks]
    specs += [whole(a) for a in (*parts, *projs)]
    specs += [
        pl.BlockSpec((previous.shape[0], span), lambda i, s: (0, s[1])),
        pl.BlockSpec((2, span), lambda i, s: (0, s[0] * count + s[1])),
    ]
    full = size * count
    return pl.pallas_call(
        middle_kernel,
        name="middle",
        cost_estimate=span_of(6),
        grid_spec=pltpu.PrefetchScalarGridSpec(
            num_scalar_prefetch=1,
            grid=(1,),
            in_specs=specs,
            out_specs=[
                pl.BlockSpec((full, span), lambda i, s: (0, 0)),
                pl.BlockSpec((span + EXTRA, full), lambda i, s: (0, 0)),
                pl.BlockSpec((8, span), lambda i, s: (0, 0)),
            ],
        ),
        out_shape=[
            jax.ShapeDtypeStruct((full, span), F32),
            jax.ShapeDtypeStruct((span + EXTRA, full), BF16),
            jax.ShapeDtypeStruct((8, span), F32),
        ],
        compiler_params=pltpu.CompilerParams(vmem_limit_bytes=VMEM_LIMIT),
    )(place, *args)


def middle_back_kernel(
    place, p0, p1, p2, p3, mid, grad, stats, routes, x0, x1, x2, x3,
    low_out, mid_out, logits_out, small_out,
):
    params = (p0, p1, p2, p3)
    full, span = mid.shape
    size = p0.shape[0]
    kinds = logits_out.shape[0]
    gates = [stats[0:1], stats[1:2]]
    inverse = stats[2:3]
    alpha = [stats[3:4], stats[4:5], stats[5:6], stats[6:7]]
    names = [routes[0:1], routes[1:2]]
    xs = (x0, x1, x2, x3)
    moe = jnp.transpose(sum(x[:span].astype(F32) for x in xs))
    ffn = [sum(unpack_row(x, span, span, k) for x in xs) for k in range(2)]
    flow = grad[...].astype(F32)
    normed = []
    dot_norm = jnp.zeros((1, span), F32)
    dot_value = [jnp.zeros((1, span), F32), jnp.zeros((1, span), F32)]
    for j in range(4):
        here = slice(j * size, (j + 1) * size)
        norm = mid[here] * inverse * column(params[j], GAIN2)
        dot_norm = dot_norm + jnp.sum(flow[here] * norm, axis=0, keepdims=True)
        for c, first in enumerate((VALUE0, VALUE1)):
            value = column(params[j], first)
            dot_value[c] = dot_value[c] + jnp.sum(flow[here] * value, axis=0, keepdims=True)
        normed.append(norm)
    experts = kinds - 4
    is_copy = [(name == experts + 1).astype(F32) for name in names]
    is_const = [[(name == experts + 2 + c).astype(F32) for name in names] for c in range(2)]
    grad_gate = []
    for k in range(2):
        value = ffn[k] + is_copy[k] * dot_norm
        for c in range(2):
            value = value + is_const[c][k] * (
                alpha[2 * c] * dot_norm + alpha[2 * c + 1] * dot_value[c]
            )
        grad_gate.append(value)
    shared = gates[0] * grad_gate[0] + gates[1] * grad_gate[1]
    chosen = [gates[k] * (grad_gate[k] - shared) for k in range(2)]
    places = lax.broadcasted_iota(jnp.int32, (kinds, span), 0)
    logits = jnp.where(places == names[0], chosen[0], 0.0) + jnp.where(
        places == names[1], chosen[1], 0.0
    )
    logits_out[...] = logits
    direct = gates[0] * is_copy[0] + gates[1] * is_copy[1]
    rows = [logits]
    portions = []
    for c in range(2):
        portion = gates[0] * is_const[c][0] + gates[1] * is_const[c][1]
        first, second = alpha[2 * c], alpha[2 * c + 1]
        along = [portion * dot_norm, portion * dot_value[c]]
        mean = first * along[0] + second * along[1]
        rows += [first * (along[0] - mean), second * (along[1] - mean)]
        direct = direct + first * portion
        portions.append(second * portion)
    rows.append(jnp.zeros((128 - kinds - 4, span), F32))
    routed = jnp.concatenate(rows, axis=0)
    lanes = lax.broadcasted_iota(jnp.int32, (size, 128), 1)
    backs = []
    inner = jnp.zeros((1, span), F32)
    for j in range(4):
        here = slice(j * size, (j + 1) * size)
        back = moe[here] + direct * flow[here] + mm(params[j][...].astype(F32), routed, 1, 0, HIGH)
        small = mm(normed[j], routed, 1, 1, HIGH)
        columns = (
            (SUM_GAIN2, mid[here] * inverse * back),
            (SUM_VALUE0, portions[0] * flow[here]),
            (SUM_VALUE1, portions[1] * flow[here]),
        )
        for lane, terms in columns:
            total = jnp.sum(terms, axis=1, keepdims=True)
            small = jnp.where(lanes == lane, total, small)
        small_out[j] = jnp.transpose(small)[:SMALL]
        gain = column(params[j], GAIN2)
        inner = inner + jnp.sum(mid[here] * gain * back, axis=0, keepdims=True)
        backs.append(back)
    inner = inner * (inverse * inverse * inverse) / full
    for j in range(4):
        here = slice(j * size, (j + 1) * size)
        gain = column(params[j], GAIN2)
        value = flow[here] + inverse * gain * backs[j] - mid[here] * inner
        mid_out[here] = value
        low_out[here] = value.astype(BF16)


def middle_back(place, toks, mid, grad, stats, routes, pieces, kinds):
    full, span = mid.shape
    count = lax.axis_size("col")
    size = full // count

    def whole(array):
        zeros = (0,) * array.ndim
        return pl.BlockSpec(array.shape, lambda i, s: zeros)

    args = (*toks, mid, grad, stats, routes, *pieces)
    specs = [param_spec(a) for a in toks] + [whole(a) for a in args[len(toks) :]]
    specs[len(toks) + 3] = pl.BlockSpec((2, span), lambda i, s: (0, s[0] * count + s[1]))
    return pl.pallas_call(
        middle_back_kernel,
        name="middle_back",
        cost_estimate=span_of(7),
        grid_spec=pltpu.PrefetchScalarGridSpec(
            num_scalar_prefetch=1,
            grid=(1,),
            in_specs=specs,
            out_specs=[
                pl.BlockSpec((full, span), lambda i, s: (0, 0)),
                pl.BlockSpec((full, span), lambda i, s: (0, 0)),
                pl.BlockSpec((kinds, span), lambda i, s: (0, 0)),
                pl.BlockSpec((count, SMALL, size), lambda i, s: (0, 0, 0)),
            ],
        ),
        out_shape=[
            jax.ShapeDtypeStruct((full, span), BF16),
            jax.ShapeDtypeStruct((full, span), F32),
            jax.ShapeDtypeStruct((kinds, span), F32),
            jax.ShapeDtypeStruct((count, SMALL, size), F32),
        ],
        compiler_params=pltpu.CompilerParams(vmem_limit_bytes=VMEM_LIMIT),
    )(place, *args)


def result_kernel(place, p0, p1, p2, p3, mid, stats, routes, logits, y0, y1, y2, y3, out):
    params = (p0, p1, p2, p3)
    size = p0.shape[0]
    experts = place[3]
    inverse = stats[2:3]
    names = [routes[0:1], routes[1:2]]
    gates = [stats[0:1], stats[1:2]]

    def portion(kind):
        return jnp.where(names[0] == kind, gates[0], 0.0) + jnp.where(
            names[1] == kind, gates[1], 0.0
        )

    first, second = portion(experts + 2), portion(experts + 3)
    direct = portion(experts + 1) + first * stats[3:4] + second * stats[5:6]
    moe = y0[...].astype(F32) + y1[...].astype(F32) + y2[...].astype(F32) + y3[...].astype(F32)
    moe = jnp.transpose(moe)
    for j in range(4):
        here = slice(j * size, (j + 1) * size)
        norm = mid[here] * inverse * column(params[j], GAIN2)
        out[j, :size] = (
            mid[here]
            + moe[here]
            + direct * norm
            + first * stats[4:5] * column(params[j], VALUE0)
            + second * stats[6:7] * column(params[j], VALUE1)
        )
        out[j, size:] = jnp.concatenate(
            [logits[...], jnp.zeros((EXTRA - logits.shape[0], logits.shape[1]), F32)], axis=0
        )


def result(place, toks, mid, stats, routes, logits, pieces):
    full, span = mid.shape
    count = lax.axis_size("col")
    tall = full // count + EXTRA

    def whole(array):
        zeros = (0,) * array.ndim
        return pl.BlockSpec(array.shape, lambda i, s: zeros)

    args = (*toks, mid, stats, routes, logits, *pieces)
    specs = [param_spec(a) for a in toks] + [whole(a) for a in args[len(toks) :]]
    specs[len(toks) + 2] = pl.BlockSpec((2, span), lambda i, s: (0, s[0] * count + s[1]))
    return pl.pallas_call(
        result_kernel,
        name="result",
        cost_estimate=span_of(5),
        grid_spec=pltpu.PrefetchScalarGridSpec(
            num_scalar_prefetch=1,
            grid=(1,),
            in_specs=specs,
            out_specs=pl.BlockSpec((count, tall, span), lambda i, s: (0, 0, 0)),
        ),
        out_shape=jax.ShapeDtypeStruct((count, tall, span), F32),
        compiler_params=pltpu.CompilerParams(vmem_limit_bytes=VMEM_LIMIT),
    )(place, *args)


def experts_kernel(chunks, last, *refs):
    order, x0, x1, x2, x3, g0, g1, g2, g3, ranks, routes, w0, w1 = refs[:13]
    refs = refs[13:]
    twos, refs = refs[: len(chunks)], refs[len(chunks) :]
    threes, refs = refs[: len(chunks)], refs[len(chunks) :]
    if last:
        y_in, dx_in, gate_in = refs[:3]
        refs = refs[3:]
    y_out, dx_out = refs[:2]
    refs = refs[2:]
    if not last:
        gate_out = refs[0]
        refs = refs[1:]
    grad_mine, grad_next, weight, y_acc, dx_acc, gate_sum, gate_rows, acc = refs
    step = pl.program_id(0)
    steps = pl.num_programs(0)
    expert = order[step]
    tiles = order[steps + step]
    size = w0.shape[1]
    tokens = ranks.shape[1]
    span = tokens // 4
    full = x0.shape[1]
    hidden_width = w0.shape[2] // 3
    both = 2 * hidden_width
    xs = (x0, x1, x2, x3)
    gs = (g0, g1, g2, g3)

    @pl.when(step == 0)
    def _():
        if last:
            y_acc[...] = y_in[...]
            dx_acc[...] = dx_in[...]
            gate_sum[...] = gate_in[...]
        else:
            y_acc[...] = jnp.zeros_like(y_acc)
            dx_acc[...] = jnp.zeros_like(dx_acc)
            gate_sum[...] = jnp.zeros_like(gate_sum)
        for i, ref in enumerate(xs):
            for k in range(2):
                gate_rows[k : k + 1, i * span : (i + 1) * span] = unpack_row(ref, span, span, k)

    weight[:size] = w0[0]
    weight[size : 2 * size] = w1[0]
    start = 0
    for two, three, count in zip(twos, threes, chunks):

        @pl.when((step >= start) & (step < start + count))
        def _():
            weight[2 * size : 3 * size] = two[0]
            weight[3 * size :] = three[0]

        start += count

    rank = ranks[pl.ds(expert, 1), :]
    hit0 = routes[0:1] == expert
    hit1 = routes[1:2] == expert
    gate_row = jnp.where(hit0, gate_rows[0:1], 0.0) + jnp.where(hit1, gate_rows[1:2], 0.0)

    def tile(index, carry):
        slots = lax.broadcasted_iota(jnp.int32, (TILE, tokens), 0) + index * TILE
        hot = slots == rank
        pick = hot.astype(F32).astype(BF16)
        gate = jnp.sum(jnp.where(hot, gate_row, 0.0), axis=1, keepdims=True)
        rows = jnp.zeros((TILE, full), F32)
        flow = jnp.zeros((TILE, full), F32)
        for i in range(4):
            cut = pick[:, i * span : (i + 1) * span]
            rows = rows + mm(cut, xs[i][:span], 1, 0)
            flow = flow + mm(cut, gs[i][...], 1, 0)
        rows = rows.astype(BF16)
        flow = flow.astype(BF16)
        gate_up = mm(rows, weight[:, :both], 1, 0)
        pre = gate_up[:, :hidden_width]
        up = gate_up[:, hidden_width:]
        sigma = 1.0 / (1.0 + jnp.exp(-pre))
        lifted = pre * sigma
        hidden = lifted * up
        scaled = (hidden * gate).astype(BF16)
        back = mm(flow, weight[:, both:], 1, 0)
        grad_gate = jnp.sum(hidden * back, axis=1, keepdims=True)
        back = back * gate
        grad_pre = back * up * sigma * (1.0 + pre * (1.0 - sigma))
        grad_up = back * lifted
        grad_both = jnp.concatenate([grad_pre.astype(BF16), grad_up.astype(BF16)], axis=1)
        y = mm(scaled, weight[:, both:], 1, 1).astype(BF16)
        dx = mm(grad_both, weight[:, :both], 1, 1).astype(BF16)
        for i in range(4):
            cut = pick[:, i * span : (i + 1) * span]
            y_acc[i * span : (i + 1) * span] += mm(cut, y, 0, 0)
            dx_acc[i * span : (i + 1) * span] += mm(cut, dx, 0, 0)
        row = jnp.sum(jnp.where(hot, grad_gate, 0.0), axis=0, keepdims=True)
        gate_sum[0:1] += jnp.where(hit0, row, 0.0)
        gate_sum[1:2] += jnp.where(hit1, row, 0.0)
        grad_weight = mm(rows, grad_both, 0, 0)
        grad_down = mm(flow, scaled, 0, 0)

        @pl.when(index == 0)
        def _():
            acc[:, :both] = grad_weight
            acc[:, both:] = grad_down

        @pl.when(index > 0)
        def _():
            acc[:, :both] += grad_weight
            acc[:, both:] += grad_down

        return carry

    lax.fori_loop(0, tiles, tile, 0)
    for k in range(4):
        ref = grad_next if k % 2 else grad_mine
        ref[k // 2, 0] = acc[k * size : (k + 1) * size].astype(BF16)

    @pl.when(step == steps - 1)
    def _():
        if last:
            for i in range(4):
                here = slice(i * span, (i + 1) * span)
                y_out[i] = y_acc[here].astype(BF16)
                dx_out[i, :span] = dx_acc[here].astype(BF16)
                rows = [gate_sum[0:1, here], gate_sum[1:2, here]]
                dx_out[i, span:] = pack_rows(rows, full)
        else:
            y_out[...] = y_acc[...]
            dx_out[...] = dx_acc[...]
            gate_out[...] = gate_sum[...]


def run_experts(order, xs, gs, ranks, routes, w0, w1, twos, threes, carried):
    size, wide = w0.shape[1:]
    tokens = ranks.shape[1]
    span = tokens // 4
    full = xs[0].shape[1]
    chunks = tuple(a.shape[0] for a in twos)
    steps = sum(chunks)
    last = carried is not None

    def whole(shape):
        zeros = (0,) * len(shape)
        return pl.BlockSpec(shape, lambda e, s: zeros)

    def chunk(start, count):
        return pl.BlockSpec(
            (1, size, wide), lambda e, s: (jnp.clip(e - start, 0, count - 1), 0, 0)
        )

    mine = pl.BlockSpec((1, size, wide), lambda e, s: (s[e], 0, 0))
    pieces = [chunk(sum(chunks[:i]), count) for i, count in enumerate(chunks)]
    args = (*xs, *gs, ranks, routes, w0, w1, *twos, *threes)
    specs = [whole(a.shape) for a in args[:10]] + [mine, mine] + pieces + pieces
    if last:
        args += tuple(carried)
        specs += [whole(a.shape) for a in carried]
        shapes = [((4, span, full), BF16), ((4, span + EXTRA, full), BF16)]
    else:
        shapes = [((tokens, full), F32), ((tokens, full), F32), ((8, tokens), F32)]
    grad = pl.BlockSpec((2, 1, size, wide), lambda e, s: (0, e, 0, 0))

    def body(*refs):
        experts_kernel(chunks, last, *refs)

    return pl.pallas_call(
        body,
        name="experts",
        cost_estimate=span_of(36),
        grid_spec=pltpu.PrefetchScalarGridSpec(
            num_scalar_prefetch=1,
            grid=(steps,),
            in_specs=specs,
            out_specs=[whole(shape) for shape, _ in shapes] + [grad] * 2,
            scratch_shapes=[
                pltpu.VMEM((full, wide), BF16),
                pltpu.VMEM((tokens, full), F32),
                pltpu.VMEM((tokens, full), F32),
                pltpu.VMEM((8, tokens), F32),
                pltpu.VMEM((8, tokens), F32),
                pltpu.VMEM((full, wide), F32),
            ],
        ),
        out_shape=[jax.ShapeDtypeStruct(shape, dtype) for shape, dtype in shapes]
        + [jax.ShapeDtypeStruct((2, steps, size, wide), BF16)] * 2,
        compiler_params=pltpu.CompilerParams(vmem_limit_bytes=VMEM_LIMIT),
    )(order, *args)


def shards(
    tokens,
    prev_logits,
    routes,
    prefix_len,
    norm1_gain,
    qkv_weight,
    out_weight,
    norm2_gain,
    router_weight,
    const_weight,
    const_values,
    gate_weight,
    up_weight,
    down_weight,
    cotangent,
):
    row = lax.axis_index("row")
    col = lax.axis_index("col")
    rows = lax.axis_size("row")
    cols = lax.axis_size("col")
    groups = lax.axis_size("dp")
    length, size = tokens.shape
    span = length // cols
    kinds = router_weight.shape[1]
    experts = gate_weight.shape[0]
    half = experts // 2
    hidden_width = gate_weight.shape[2]
    first_half = lax.axis_index("dp") if groups == 2 else jnp.int32(0)
    prefix = lax.dynamic_index_in_dim(prefix_len, row, 0, False)
    place = jnp.stack([row, col, prefix, jnp.int32(experts)]).astype(jnp.int32)
    flat = [(i // cols, i % cols) for i in range(rows * cols)]

    def spread(value, turn):
        pairs = [(c * cols + (c ^ r ^ turn), r * cols + c) for r, c in flat]
        return lax.ppermute(value, ("row", "col"), pairs)

    def collect(value, turn):
        pairs = [(r * cols + c, c * cols + (r ^ turn)) for r, c in flat]
        return lax.ppermute(value, ("row", "col"), pairs)

    def across_groups(value):
        return lax.ppermute(value, "dp", [(0, 1), (1, 0)])


    values = [norm1_gain, norm2_gain, const_values[0], const_values[1]]
    lanes = [router_weight, const_weight]
    for value in values:
        lanes += [part[:, None] for part in parts_of(value)]
    lanes.append(jnp.zeros((size, PARAMS - kinds - 4 - 3 * len(values)), BF16))
    piece = jnp.concatenate([qkv_weight[0], qkv_weight[1], qkv_weight[2], out_weight.T], axis=1)
    toks = col_gather(jnp.concatenate([tokens.T] + lanes, axis=1))
    weight = jnp.stack([spread(piece, m) for m in range(rows)])
    halves = HD // 2
    freq = 10000.0 ** (-jnp.arange(halves, dtype=F32) / halves)
    angle = freq[:, None] * jnp.arange(length, dtype=F32)[None, :]
    cosine = jnp.cos(angle)
    sine = jnp.sin(angle)

    flow = after(cotangent.T, toks[2]).reshape(size, cols, span)
    flow_parts = [lax.dynamic_index_in_dim(flow, col ^ k, 1, False) for k in range(cols)]
    flow_quarter = jnp.concatenate(
        [flow_parts[0]] + [col_swap(flow_parts[k], k) for k in range(1, cols)], axis=0
    )
    flow_rows = row_gather(flow_quarter.T)

    own = jnp.concatenate([gate_weight, up_weight, down_weight.transpose(0, 2, 1)], axis=2)
    near_own = lax.dynamic_slice_in_dim(own, first_half * half, half, 0)
    pair = half // 2
    two_a = col_swap(after(near_own[:pair], flow_quarter), 2)
    projs = col_gather(after(weight[:, :, 3 * size :], toks[2]))

    routes_t = routes.T
    share = lax.dynamic_index_in_dim(routes_t.reshape(2, rows, cols, span), col, 2, False)
    turned = (row - jnp.arange(rows)) % rows
    share = jnp.take(share, turned, axis=1).reshape(2, rows * span)
    ids = jnp.arange(experts, dtype=jnp.int32)[:, None]
    hits = (share[0][None] == ids) | (share[1][None] == ids)
    counts = jnp.cumsum(hits.astype(jnp.int32), axis=1)
    ranks = jnp.where(hits, counts - 1, -1)
    order = (first_half * half + jnp.arange(experts, dtype=jnp.int32)) % experts
    tiles = jnp.take(jnp.maximum((counts[:, -1] + TILE - 1) // TILE, 1), order)
    order_near = jnp.concatenate([order[:half], tiles[:half]]).astype(jnp.int32)
    order_far = jnp.concatenate([order[half:], tiles[half:]]).astype(jnp.int32)

    query, keys, values, attn, logsum = attend(place, toks, weight, cosine, sine)
    attn, two_a, flow_rows, projs = join(attn, two_a, flow_rows, projs)
    parts = [attn[0]] + [col_swap(attn[k], k) for k in range(1, cols)]
    two_b = col_swap(after(near_own[pair:], parts[1], parts[2], parts[3]), 2)
    if groups == 2:
        far_two_a = across_groups(two_a)
    else:
        far_two_a = col_swap(own[half : half + pair], 2)
    side = col_swap(after(own, attn), 1)
    mid, in_rows, stats = middle(place, toks, parts, projs, prev_logits.T, routes_t)
    x_rows = row_gather(in_rows)
    three_a = col_swap(after(two_a, parts[1], parts[2], parts[3]), 1)
    two_b, far_two_a = join(after(two_b, *x_rows[1:]), after(far_two_a, *x_rows[1:]))
    if groups == 2:
        far_two_b = across_groups(two_b)
    else:
        far_two_b = col_swap(own[half + pair :], 2)
    three_b = col_swap(two_b, 1)
    far_three_a = col_swap(far_two_a, 1)
    x_rows, far_three_a = join(x_rows, far_three_a)

    near_out = run_experts(
        order_near, x_rows, flow_rows, ranks, share, own, side,
        [two_a, two_b], [three_a, three_b], None,
    )
    near_out, far_two_b = join(near_out, far_two_b)
    *carried, near_mine, near_next = near_out
    far_three_b = col_swap(far_two_b, 1)
    near_next = col_swap(after(near_next, far_three_b), 1)
    y, dx, far_mine, far_next = run_experts(
        order_far, x_rows, flow_rows, ranks, share, own, side,
        [far_two_a, far_two_b], [far_three_a, far_three_b], carried,
    )

    def low_sum(left, right):
        return (left.astype(F32) + right.astype(F32)).astype(BF16)

    def row_scatter(value):
        return [value[0]] + [row_shift(value[s], -s) for s in range(1, rows)]

    def across_sums(sums):
        return [across_groups(s) for s in sums] if groups == 2 else list(sums)

    near_kept, near_sent = low_sum(near_mine[0], near_next[0]), low_sum(near_mine[1], near_next[1])
    dx_first = row_shift(dx[1], -1)
    dx, dx_first, near_sent, near_kept, far_next = join(
        dx, dx_first, near_sent, near_kept, far_next
    )
    near_got = [col_swap(near_sent[:pair], 2), col_swap(near_sent[pair:], 2)]
    dx = [dx[0], dx_first] + [row_shift(dx[s], -s) for s in range(2, rows)]
    far_next = col_swap(far_next, 1)
    dx, near_got[0] = join(dx, near_got[0])
    near_sum = [low_sum(near_kept[:pair], near_got[0])]
    near_other = across_sums(near_sum)
    low, grad_mid, grad_logits, small = middle_back(
        place, toks, mid, flow_quarter, stats, routes_t, dx, kinds
    )
    lows = col_gather(low)
    near_sum.append(low_sum(after(near_kept, low)[pair:], near_got[1]))
    lows, near_sum, near_other, far_mine, far_next = join(
        lows, near_sum, near_other, far_mine, far_next
    )
    near_other += across_sums(near_sum[1:])

    y = row_scatter(after(y, dx[1], dx[2], dx[3]))
    far_kept, far_sent = low_sum(far_mine[0], far_next[0]), low_sum(far_mine[1], far_next[1])
    far_got = [col_swap(far_sent[:pair], 2)]
    tokens_parts, weight_parts = attend_back(
        place, toks, weight, cosine, sine,
        query, keys, values, attn, logsum, lows, grad_mid, small,
    )
    tokens_parts, weight_parts, y, near_other, far_got[0], far_sent = join(
        tokens_parts, weight_parts, y, near_other, far_got[0], far_sent
    )
    far_got.append(col_swap(far_sent[pair:], 2))
    far_sum = [low_sum(far_kept[:pair], far_got[0])]
    far_other = across_sums(far_sum)
    out = result(place, toks, mid, stats, routes_t, grad_logits, y)
    tokens_parts, weight_parts, out, far_got[1], far_other[0] = join(
        tokens_parts, weight_parts, out, far_got[1], far_other[0]
    )
    far_sum.append(low_sum(far_kept[pair:], far_got[1]))
    far_other += across_sums(far_sum[1:])

    def col_scatter(value):
        total = value[0].astype(F32)
        for k in range(1, cols):
            total = total + col_swap(value[k], k).astype(F32)
        return total

    total = collect(weight_parts[0], 0).astype(F32)
    for m in range(1, rows):
        total = total + collect(weight_parts[m], m).astype(F32)
    packed = total[:, 4 * size : 4 * size + 3 * SMALL]
    small = packed[:, :SMALL] + packed[:, SMALL : 2 * SMALL] + packed[:, 2 * SMALL :]
    small = dp_total(row_total(small.T))
    total, far_other = join(total, far_other)
    total = dp_total(total[:, : 4 * size].astype(BF16))
    grad_tokens = col_scatter(tokens_parts)
    qkv_sum = jnp.stack([total[:, j * size : (j + 1) * size] for j in range(3)])
    proj_sum = total[:, 3 * size :].T
    out = jnp.stack([out[0]] + [col_swap(out[k], k) for k in range(1, cols)])
    out = jnp.take(out, col ^ jnp.arange(cols), axis=0)
    out = jnp.concatenate([out[i] for i in range(cols)], axis=1)
    if groups == 2:
        near_start = first_half * half
        far_start = half - near_start
        grads = []
        for j in range(3):
            wide = slice(j * hidden_width, (j + 1) * hidden_width)
            grad = jnp.zeros((experts, size, hidden_width), F32)
            for i in range(2):
                for start, mine, other in (
                    (near_start, near_sum[i], far_other[i]),
                    (far_start, far_sum[i], near_other[i]),
                ):
                    both = mine[:, :, wide].astype(F32) + other[:, :, wide].astype(F32)
                    grad = lax.dynamic_update_slice_in_dim(grad, both, start + i * pair, 0)
            grads.append(grad)
    else:
        both = lax.psum(jnp.concatenate(near_sum + far_sum).astype(F32), "dp")
        grads = [both[:, :, j * hidden_width : (j + 1) * hidden_width] for j in range(3)]

    return (
        out[:size].T,
        grad_tokens.T,
        out[size : size + kinds].T,
        small[SUM_GAIN1],
        qkv_sum,
        proj_sum,
        small[SUM_GAIN2],
        small[:kinds].T,
        small[kinds : kinds + 4].T,
        small[SUM_VALUE0 : SUM_VALUE1 + 1],
        grads[0],
        grads[1],
        grads[2].transpose(0, 2, 1),
    )


def solution(mesh):
    return jax.shard_map(
        shards,
        mesh=mesh,
        in_specs=(
            P(("dp", "row"), "col"),
            P(("dp", "row"), None),
            P("dp", None),
            P("dp"),
            P("col"),
            P(None, "col", "row"),
            P("row", "col"),
            P("col"),
            P("col", None),
            P("col", None),
            P(None, "col"),
            P(None, "col", "row"),
            P(None, "col", "row"),
            P(None, "row", "col"),
            P(("dp", "row"), "col"),
        ),
        out_specs=(
            P(("dp", "row"), "col"),
            P(("dp", "row"), "col"),
            P(("dp", "row"), None),
            P("col"),
            P(None, "col", "row"),
            P("row", "col"),
            P("col"),
            P("col", None),
            P("col", None),
            P(None, "col"),
            P(None, "col", "row"),
            P(None, "col", "row"),
            P(None, "row", "col"),
        ),
        check_vma=False,
    )
```

```python
import jax
import jax.numpy as jnp
from jax import lax
from jax.experimental import pallas as pl
from jax.experimental.pallas import tpu as pltpu
from jax.sharding import PartitionSpec as P

HD = 64
LEN = 1024
EPS = 1e-06
HIGH = lax.Precision.HIGHEST
NEGATIVE = -1e30
TILE = 256
VMEM_LIMIT = 60 * 1024 * 1024
F32 = jnp.float32
BF16 = jnp.bfloat16
PARAMS = 128
GAIN1, GAIN2, VALUE0, VALUE1 = 16, 19, 22, 25
SUM_GAIN2, SUM_VALUE0, SUM_VALUE1, SUM_GAIN1 = 16, 17, 18, 19
EXTRA = 16
SMALL = 24


def mm(left, right, over_left, over_right, precision=None):
    return lax.dot_general(
        left,
        right,
        (((over_left,), (over_right,)), ((), ())),
        preferred_element_type=F32,
        precision=precision,
    )


def parts_of(value):
    high = lax.reduce_precision(value, 8, 7)
    middle = lax.reduce_precision(value - high, 8, 7)
    return [high.astype(BF16), middle.astype(BF16), (value - high - middle).astype(BF16)]


def column(params, first):
    low = params[:, first : first + 3].astype(F32)
    return low[:, 0:1] + low[:, 1:2] + low[:, 2:3]


def pack_rows(rows, width):
    out = []
    for row in rows:
        high = row.astype(BF16).astype(F32)
        middle = (row - high).astype(BF16).astype(F32)
        out += [high, middle, row - high - middle]
    out.append(jnp.zeros((EXTRA - len(out), rows[0].shape[1]), F32))
    packed = jnp.concatenate(out, axis=0)
    rest = jnp.zeros((EXTRA, width - packed.shape[1]), F32)
    return jnp.concatenate([packed, rest], axis=1).astype(BF16)


def parts_in_rows(value, height):
    high = value.astype(BF16).astype(F32)
    middle = (value - high).astype(BF16).astype(F32)
    rest = jnp.zeros((height - 3 * value.shape[0], value.shape[1]), F32)
    return jnp.concatenate([high, middle, value - high - middle, rest], axis=0)


def unpack_row(ref, base, span, k):
    parts = ref[base : base + EXTRA, :span].astype(F32)
    return parts[3 * k : 3 * k + 1] + parts[3 * k + 1 : 3 * k + 2] + parts[3 * k + 2 : 3 * k + 3]


def span_of(micros):
    return pl.CostEstimate(
        flops=int(micros * 1.1e9), transcendentals=0, bytes_accessed=int(micros * 3.6e6)
    )


def after(value, *others):
    return lax.optimization_barrier((value,) + others)[0]


def join(*values):
    return lax.optimization_barrier(values)


def col_swap(value, bits):
    count = lax.axis_size("col")
    return lax.ppermute(value, "col", [(i, i ^ bits) for i in range(count)])


def row_swap(value, bits):
    count = lax.axis_size("row")
    return lax.ppermute(value, "row", [(i, i ^ bits) for i in range(count)])


def row_shift(value, steps):
    count = lax.axis_size("row")
    return lax.ppermute(value, "row", [(i, (i + steps) % count) for i in range(count)])


def col_gather(value):
    count = lax.axis_size("col")
    found = {0: value}
    bit = count // 2
    while bit:
        found.update({k | bit: col_swap(v, bit) for k, v in found.items()})
        bit //= 2
    return [found[k] for k in range(count)]


def row_gather(value):
    count = lax.axis_size("row")
    return [value] + [row_shift(value, s) for s in range(1, count)]


def dp_total(value):
    count = lax.axis_size("dp")
    if count == 2:
        other = lax.ppermute(value, "dp", [(0, 1), (1, 0)])
        return value.astype(F32) + other.astype(F32)
    return lax.psum(value.astype(F32), "dp")


def row_total(value):
    bit = 1
    while bit < lax.axis_size("row"):
        value = value + row_swap(value, bit)
        bit *= 2
    return value


def rotate_halves(block, cosine, sine):
    half = HD // 2
    out = []
    for head in range(block.shape[0] // HD):
        first = block[head * HD : head * HD + half]
        second = block[head * HD + half : (head + 1) * HD]
        out.append(first * cosine - second * sine)
        out.append(second * cosine + first * sine)
    return jnp.concatenate(out, axis=0)


def attend_kernel(
    place, t0, t1, t2, t3, weight, cosine, sine,
    query_out, key_out, value_out, attn_out, logsum_out, act, w_all,
):
    block = pl.program_id(0)
    row = place[0]
    prefix = place[2]
    size = t0.shape[0]
    heads = query_out.shape[1] // HD
    width = heads * HD
    count = query_out.shape[0]
    span = query_out.shape[2]
    length = key_out.shape[1]

    @pl.when(block == 0)
    def _():
        square = jnp.zeros((1, length), F32)
        for ref in (t0, t1, t2, t3):
            hidden = ref[:, :length].astype(F32)
            square = square + jnp.sum(hidden * hidden, axis=0, keepdims=True)
        inverse = lax.rsqrt(square / (size * 4) + EPS)
        for k, ref in enumerate((t0, t1, t2, t3)):
            gain = column(ref[:, length:], GAIN1)
            hidden = ref[:, :length].astype(F32)
            act[k * size : (k + 1) * size] = (hidden * inverse * gain).astype(BF16)
            w_all[k * size : (k + 1) * size] = weight[row ^ k, :, : 3 * width]
        qkv = mm(w_all[...], act[...], 0, 0)
        query = rotate_halves(qkv[:width], cosine[...], sine[...]).astype(BF16)
        keys = rotate_halves(qkv[width : 2 * width], cosine[...], sine[...]).astype(BF16)
        for i in range(count):
            query_out[i] = query[:, i * span : (i + 1) * span]
        key_out[...] = keys
        value_out[...] = qkv[2 * width :].astype(BF16)

    places = lax.broadcasted_iota(jnp.int32, (length, span), 0)
    mine = lax.broadcasted_iota(jnp.int32, (1, span), 1) + block * span
    seen = places <= jnp.maximum(mine, prefix - 1)
    rows = []
    for head in range(heads):
        cut = slice(head * HD, (head + 1) * HD)
        query = (query_out[block, cut].astype(F32) * HD ** (-0.5)).astype(BF16)
        scores = jnp.where(seen, mm(key_out[cut], query, 0, 0), NEGATIVE)
        top = jnp.max(scores, axis=0, keepdims=True)
        weights = jnp.exp(scores - top)
        total = jnp.sum(weights, axis=0, keepdims=True)
        mixed = mm(value_out[cut], weights.astype(BF16), 1, 0)
        attn_out[0, cut] = (mixed / total).astype(BF16)
        rows.append(top + jnp.log(total))
    rows.append(jnp.zeros((8 - heads, span), F32))
    logsum_out[...] = jnp.concatenate(rows, axis=0)


def attend(place, toks, weight, cosine, sine):
    size = toks[0].shape[0]
    length = cosine.shape[1]
    count = lax.axis_size("col")
    span = length // count
    width = weight.shape[2] // 4

    def whole(array):
        zeros = (0,) * array.ndim
        return pl.BlockSpec(array.shape, lambda q, s: zeros)

    args = (*toks, weight, cosine, sine)
    return pl.pallas_call(
        attend_kernel,
        name="attend",
        cost_estimate=span_of(14),
        grid_spec=pltpu.PrefetchScalarGridSpec(
            num_scalar_prefetch=1,
            grid=(count,),
            in_specs=[whole(a) for a in args],
            out_specs=[
                pl.BlockSpec((count, width, span), lambda q, s: (0, 0, 0)),
                pl.BlockSpec((width, length), lambda q, s: (0, 0)),
                pl.BlockSpec((width, length), lambda q, s: (0, 0)),
                pl.BlockSpec((1, width, span), lambda q, s: (q ^ s[1], 0, 0)),
                pl.BlockSpec((8, span), lambda q, s: (0, q)),
            ],
            scratch_shapes=[
                pltpu.VMEM((size * count, length), BF16),
                pltpu.VMEM((size * count, 3 * width), BF16),
            ],
        ),
        out_shape=[
            jax.ShapeDtypeStruct((count, width, span), BF16),
            jax.ShapeDtypeStruct((width, length), BF16),
            jax.ShapeDtypeStruct((width, length), BF16),
            jax.ShapeDtypeStruct((count, width, span), BF16),
            jax.ShapeDtypeStruct((8, length), F32),
        ],
        compiler_params=pltpu.CompilerParams(vmem_limit_bytes=VMEM_LIMIT),
    )(place, *args)


def attend_back_kernel(
    place, t0, t1, t2, t3, weight, cosine, sine,
    query, keys, values, attn, logsum, d0, d1, d2, d3, grad_mid, small,
    tokens_out, weight_out,
    dmid, proj_all, proj_acc, key_acc, value_acc, grad_all,
):
    block = pl.program_id(0)
    row = place[0]
    col = place[1]
    prefix = place[2]
    size = t0.shape[0]
    length = cosine.shape[1]
    count, width, span = query.shape
    heads = width // HD
    last = count - 1

    @pl.when(block == 0)
    def _():
        for k in range(count):
            proj_all[k * size : (k + 1) * size] = weight[row ^ k, :, 3 * width :]
        proj_acc[...] = jnp.zeros_like(proj_acc)
        key_acc[...] = jnp.zeros_like(key_acc)
        value_acc[...] = jnp.zeros_like(value_acc)

    for k, ref in enumerate((d0, d1, d2, d3)):

        @pl.when((block ^ col) == k)
        def _():
            for j in range(count):
                dmid[j * size : (j + 1) * size] = ref[(k ^ j) * size : ((k ^ j) + 1) * size]

    low = dmid[...]
    grad_attn = mm(proj_all[...], low, 0, 0).astype(BF16)
    proj_acc[...] += mm(low, attn[0], 1, 1)
    places = lax.broadcasted_iota(jnp.int32, (length, span), 0)
    mine = lax.broadcasted_iota(jnp.int32, (1, span), 1) + block * span
    seen = places <= jnp.maximum(mine, prefix - 1)
    scale = HD ** (-0.5)
    parts = []
    for head in range(heads):
        cut = slice(head * HD, (head + 1) * HD)
        plain = query[block, cut]
        scaled = (plain.astype(F32) * scale).astype(BF16)
        scores = mm(keys[cut], scaled, 0, 0)
        probs = jnp.where(seen, jnp.exp(scores - logsum[head : head + 1]), 0.0)
        above = grad_attn[cut]
        grad_probs = mm(values[cut], above, 0, 0)
        inner = jnp.sum(probs * grad_probs, axis=0, keepdims=True)
        grad_scores = (probs * (grad_probs - inner)).astype(BF16)
        parts.append(mm(keys[cut], grad_scores, 1, 0) * scale)
        key_acc[cut] += mm(plain, grad_scores, 1, 1)
        value_acc[cut] += mm(above, probs.astype(BF16), 1, 1)
    for i in range(count):

        @pl.when(block == i)
        def _():
            here = slice(i * span, (i + 1) * span)
            turned = rotate_halves(
                jnp.concatenate(parts, axis=0), cosine[:, here], -sine[:, here]
            )
            grad_all[:width, here] = turned.astype(BF16)

    @pl.when(block == last)
    def _():
        turned = rotate_halves(key_acc[...] * scale, cosine[...], -sine[...])
        grad_all[width : 2 * width] = turned.astype(BF16)
        grad_all[2 * width :] = value_acc[...].astype(BF16)
        refs = (t0, t1, t2, t3)
        gains = [column(ref[:, length:], GAIN1) for ref in refs]
        square = jnp.zeros((1, length), F32)
        for ref in refs:
            hidden = ref[:, :length].astype(F32)
            square = square + jnp.sum(hidden * hidden, axis=0, keepdims=True)
        inverse = lax.rsqrt(square / (size * count) + EPS)
        backs = []
        inner = jnp.zeros((1, length), F32)
        for k in range(count):
            hidden = refs[k][:, :length].astype(F32)
            act = (hidden * inverse * gains[k]).astype(BF16)
            weight_out[row ^ col ^ k, :, : 3 * width] = mm(act, grad_all[...], 1, 1).astype(BF16)
            weight_out[row ^ col ^ k, :, 3 * width : 4 * width] = proj_acc[
                k * size : (k + 1) * size
            ].astype(BF16)
            back = mm(weight[row ^ k, :, : 3 * width], grad_all[...], 1, 0)
            inner = inner + jnp.sum(hidden * gains[k] * back, axis=0, keepdims=True)
            summed = jnp.sum(hidden * inverse * back, axis=1, keepdims=True)
            turned = jnp.transpose(jnp.broadcast_to(summed, (size, 128)))[: small.shape[1]]
            places = lax.broadcasted_iota(jnp.int32, turned.shape, 0)
            rows = parts_in_rows(jnp.where(places == SUM_GAIN1, turned, small[k]), PARAMS)
            weight_out[row ^ col ^ k, :, 4 * width :] = jnp.transpose(rows).astype(BF16)
            backs.append(back)
        inner = inner * (inverse * inverse * inverse) / (size * count)
        for k in range(count):
            hidden = refs[k][:, :length].astype(F32)
            grad = inverse * gains[k] * backs[k] - hidden * inner
            for i in range(count):
                here = slice(i * span, (i + 1) * span)
                extra = jnp.where(col == i, grad_mid[k * size : (k + 1) * size], 0.0)
                tokens_out[k, :, here] = (grad[:, here] + extra).astype(BF16)


def attend_back(
    place, toks, weight, cosine, sine, query, keys, values, attn, logsum, lows, grad_mid, small
):
    size = toks[0].shape[0]
    length = cosine.shape[1]
    count, width, span = query.shape

    def whole(array):
        zeros = (0,) * array.ndim
        return pl.BlockSpec(array.shape, lambda q, s: zeros)

    args = (
        *toks, weight, cosine, sine, query, keys, values, attn, logsum, *lows, grad_mid, small,
    )
    specs = [whole(a) for a in args]
    at = len(toks) + 3 + 3
    specs[at] = pl.BlockSpec((1, width, span), lambda q, s: (q ^ s[1], 0, 0))
    specs[at + 1] = pl.BlockSpec((8, span), lambda q, s: (0, q))
    return pl.pallas_call(
        attend_back_kernel,
        name="attend_back",
        cost_estimate=span_of(24),
        grid_spec=pltpu.PrefetchScalarGridSpec(
            num_scalar_prefetch=1,
            grid=(count,),
            in_specs=specs,
            out_specs=[
                pl.BlockSpec((count, size, length), lambda q, s: (0, 0, 0)),
                pl.BlockSpec((count, size, 4 * width + PARAMS), lambda q, s: (0, 0, 0)),
            ],
            scratch_shapes=[
                pltpu.VMEM((size * count, span), BF16),
                pltpu.VMEM((size * count, width), BF16),
                pltpu.VMEM((size * count, width), F32),
                pltpu.VMEM((width, length), F32),
                pltpu.VMEM((width, length), F32),
                pltpu.VMEM((3 * width, length), BF16),
            ],
        ),
        out_shape=[
            jax.ShapeDtypeStruct((count, size, length), BF16),
            jax.ShapeDtypeStruct((count, size, 4 * width + PARAMS), BF16),
        ],
        compiler_params=pltpu.CompilerParams(vmem_limit_bytes=VMEM_LIMIT),
    )(place, *args)


def route_rows(routes, logits):
    places = lax.broadcasted_iota(jnp.int32, logits.shape, 0)
    hots = [places == routes[k : k + 1] for k in range(2)]
    return hots, [jnp.sum(jnp.where(hot, logits, 0.0), axis=0, keepdims=True) for hot in hots]


def pair_softmax(first, second):
    top = jnp.maximum(first, second)
    first = jnp.exp(first - top)
    second = jnp.exp(second - top)
    total = first + second
    return first / total, second / total


def middle_kernel(
    place, t0, t1, t2, t3, p0, p1, p2, p3, a0, a1, a2, a3, o0, o1, o2, o3, previous, routes,
    mid_out, rows_out, stats_out,
):
    row = place[0]
    size, span = t0.shape
    params = (p0, p1, p2, p3)
    kinds = previous.shape[0]
    square = jnp.zeros((1, span), F32)
    for j, ref in enumerate((t0, t1, t2, t3)):
        mid = ref[...].astype(F32)
        for k, (part, proj) in enumerate(((a0, o0), (a1, o1), (a2, o2), (a3, o3))):
            mid = mid + mm(proj[row ^ k ^ j], part[...], 1, 0)
        square = square + jnp.sum(mid * mid, axis=0, keepdims=True)
        mid_out[j * size : (j + 1) * size] = mid
    inverse = lax.rsqrt(square / (size * 4) + EPS)
    summed = jnp.zeros((128, span), F32)
    normed = []
    for j in range(4):
        norm = mid_out[j * size : (j + 1) * size] * inverse * column(params[j], GAIN2)
        summed = summed + mm(params[j][...].astype(F32), norm, 0, 0, HIGH)
        normed.append(norm)
    rows_out[:span] = jnp.transpose(jnp.concatenate(normed, axis=0)).astype(BF16)
    logits = summed[:kinds] + previous[...]
    _, chosen = route_rows(routes[...], logits)
    gates = pair_softmax(*chosen)
    rows_out[span:] = pack_rows(gates, rows_out.shape[1])
    alpha = [
        *pair_softmax(summed[12:13], summed[13:14]),
        *pair_softmax(summed[14:15], summed[15:16]),
    ]
    stats_out[...] = jnp.concatenate([*gates, inverse, *alpha, jnp.zeros((1, span), F32)], axis=0)


def param_spec(array):
    size, width = array.shape
    return pl.BlockSpec((size, PARAMS), lambda i, s: (0, width // PARAMS - 1))


def middle(place, toks, parts, projs, previous, routes):
    size = toks[0].shape[0]
    span = parts[0].shape[1]
    count = lax.axis_size("col")

    def whole(array):
        zeros = (0,) * array.ndim
        return pl.BlockSpec(array.shape, lambda i, s: zeros)

    args = (*toks, *toks, *parts, *projs, previous, routes)
    specs = [pl.BlockSpec((size, span), lambda i, s: (0, s[1])) for _ in toks]
    specs += [param_spec(a) for a in toks]
    specs += [whole(a) for a in (*parts, *projs)]
    specs += [
        pl.BlockSpec((previous.shape[0], span), lambda i, s: (0, s[1])),
        pl.BlockSpec((2, span), lambda i, s: (0, s[0] * count + s[1])),
    ]
    full = size * count
    return pl.pallas_call(
        middle_kernel,
        name="middle",
        cost_estimate=span_of(6),
        grid_spec=pltpu.PrefetchScalarGridSpec(
            num_scalar_prefetch=1,
            grid=(1,),
            in_specs=specs,
            out_specs=[
                pl.BlockSpec((full, span), lambda i, s: (0, 0)),
                pl.BlockSpec((span + EXTRA, full), lambda i, s: (0, 0)),
                pl.BlockSpec((8, span), lambda i, s: (0, 0)),
            ],
        ),
        out_shape=[
            jax.ShapeDtypeStruct((full, span), F32),
            jax.ShapeDtypeStruct((span + EXTRA, full), BF16),
            jax.ShapeDtypeStruct((8, span), F32),
        ],
        compiler_params=pltpu.CompilerParams(vmem_limit_bytes=VMEM_LIMIT),
    )(place, *args)


def middle_back_kernel(
    place, p0, p1, p2, p3, mid, grad, stats, routes, x0, x1, x2, x3,
    low_out, mid_out, logits_out, small_out,
):
    params = (p0, p1, p2, p3)
    full, span = mid.shape
    size = p0.shape[0]
    kinds = logits_out.shape[0]
    gates = [stats[0:1], stats[1:2]]
    inverse = stats[2:3]
    alpha = [stats[3:4], stats[4:5], stats[5:6], stats[6:7]]
    names = [routes[0:1], routes[1:2]]
    xs = (x0, x1, x2, x3)
    moe = jnp.transpose(sum(x[:span].astype(F32) for x in xs))
    ffn = [sum(unpack_row(x, span, span, k) for x in xs) for k in range(2)]
    flow = grad[...].astype(F32)
    normed = []
    dot_norm = jnp.zeros((1, span), F32)
    dot_value = [jnp.zeros((1, span), F32), jnp.zeros((1, span), F32)]
    for j in range(4):
        here = slice(j * size, (j + 1) * size)
        norm = mid[here] * inverse * column(params[j], GAIN2)
        dot_norm = dot_norm + jnp.sum(flow[here] * norm, axis=0, keepdims=True)
        for c, first in enumerate((VALUE0, VALUE1)):
            value = column(params[j], first)
            dot_value[c] = dot_value[c] + jnp.sum(flow[here] * value, axis=0, keepdims=True)
        normed.append(norm)
    experts = kinds - 4
    is_copy = [(name == experts + 1).astype(F32) for name in names]
    is_const = [[(name == experts + 2 + c).astype(F32) for name in names] for c in range(2)]
    grad_gate = []
    for k in range(2):
        value = ffn[k] + is_copy[k] * dot_norm
        for c in range(2):
            value = value + is_const[c][k] * (
                alpha[2 * c] * dot_norm + alpha[2 * c + 1] * dot_value[c]
            )
        grad_gate.append(value)
    shared = gates[0] * grad_gate[0] + gates[1] * grad_gate[1]
    chosen = [gates[k] * (grad_gate[k] - shared) for k in range(2)]
    places = lax.broadcasted_iota(jnp.int32, (kinds, span), 0)
    logits = jnp.where(places == names[0], chosen[0], 0.0) + jnp.where(
        places == names[1], chosen[1], 0.0
    )
    logits_out[...] = logits
    direct = gates[0] * is_copy[0] + gates[1] * is_copy[1]
    rows = [logits]
    portions = []
    for c in range(2):
        portion = gates[0] * is_const[c][0] + gates[1] * is_const[c][1]
        first, second = alpha[2 * c], alpha[2 * c + 1]
        along = [portion * dot_norm, portion * dot_value[c]]
        mean = first * along[0] + second * along[1]
        rows += [first * (along[0] - mean), second * (along[1] - mean)]
        direct = direct + first * portion
        portions.append(second * portion)
    rows.append(jnp.zeros((128 - kinds - 4, span), F32))
    routed = jnp.concatenate(rows, axis=0)
    lanes = lax.broadcasted_iota(jnp.int32, (size, 128), 1)
    backs = []
    inner = jnp.zeros((1, span), F32)
    for j in range(4):
        here = slice(j * size, (j + 1) * size)
        back = moe[here] + direct * flow[here] + mm(params[j][...].astype(F32), routed, 1, 0, HIGH)
        small = mm(normed[j], routed, 1, 1, HIGH)
        columns = (
            (SUM_GAIN2, mid[here] * inverse * back),
            (SUM_VALUE0, portions[0] * flow[here]),
            (SUM_VALUE1, portions[1] * flow[here]),
        )
        for lane, terms in columns:
            total = jnp.sum(terms, axis=1, keepdims=True)
            small = jnp.where(lanes == lane, total, small)
        small_out[j] = jnp.transpose(small)[:SMALL]
        gain = column(params[j], GAIN2)
        inner = inner + jnp.sum(mid[here] * gain * back, axis=0, keepdims=True)
        backs.append(back)
    inner = inner * (inverse * inverse * inverse) / full
    for j in range(4):
        here = slice(j * size, (j + 1) * size)
        gain = column(params[j], GAIN2)
        value = flow[here] + inverse * gain * backs[j] - mid[here] * inner
        mid_out[here] = value
        low_out[here] = value.astype(BF16)


def middle_back(place, toks, mid, grad, stats, routes, pieces, kinds):
    full, span = mid.shape
    count = lax.axis_size("col")
    size = full // count

    def whole(array):
        zeros = (0,) * array.ndim
        return pl.BlockSpec(array.shape, lambda i, s: zeros)

    args = (*toks, mid, grad, stats, routes, *pieces)
    specs = [param_spec(a) for a in toks] + [whole(a) for a in args[len(toks) :]]
    specs[len(toks) + 3] = pl.BlockSpec((2, span), lambda i, s: (0, s[0] * count + s[1]))
    return pl.pallas_call(
        middle_back_kernel,
        name="middle_back",
        cost_estimate=span_of(7),
        grid_spec=pltpu.PrefetchScalarGridSpec(
            num_scalar_prefetch=1,
            grid=(1,),
            in_specs=specs,
            out_specs=[
                pl.BlockSpec((full, span), lambda i, s: (0, 0)),
                pl.BlockSpec((full, span), lambda i, s: (0, 0)),
                pl.BlockSpec((kinds, span), lambda i, s: (0, 0)),
                pl.BlockSpec((count, SMALL, size), lambda i, s: (0, 0, 0)),
            ],
        ),
        out_shape=[
            jax.ShapeDtypeStruct((full, span), BF16),
            jax.ShapeDtypeStruct((full, span), F32),
            jax.ShapeDtypeStruct((kinds, span), F32),
            jax.ShapeDtypeStruct((count, SMALL, size), F32),
        ],
        compiler_params=pltpu.CompilerParams(vmem_limit_bytes=VMEM_LIMIT),
    )(place, *args)


def result_kernel(place, p0, p1, p2, p3, mid, stats, routes, logits, y0, y1, y2, y3, out):
    params = (p0, p1, p2, p3)
    size = p0.shape[0]
    experts = place[3]
    inverse = stats[2:3]
    names = [routes[0:1], routes[1:2]]
    gates = [stats[0:1], stats[1:2]]

    def portion(kind):
        return jnp.where(names[0] == kind, gates[0], 0.0) + jnp.where(
            names[1] == kind, gates[1], 0.0
        )

    first, second = portion(experts + 2), portion(experts + 3)
    direct = portion(experts + 1) + first * stats[3:4] + second * stats[5:6]
    moe = y0[...].astype(F32) + y1[...].astype(F32) + y2[...].astype(F32) + y3[...].astype(F32)
    moe = jnp.transpose(moe)
    for j in range(4):
        here = slice(j * size, (j + 1) * size)
        norm = mid[here] * inverse * column(params[j], GAIN2)
        out[j, :size] = (
            mid[here]
            + moe[here]
            + direct * norm
            + first * stats[4:5] * column(params[j], VALUE0)
            + second * stats[6:7] * column(params[j], VALUE1)
        )
        out[j, size:] = jnp.concatenate(
            [logits[...], jnp.zeros((EXTRA - logits.shape[0], logits.shape[1]), F32)], axis=0
        )


def result(place, toks, mid, stats, routes, logits, pieces):
    full, span = mid.shape
    count = lax.axis_size("col")
    tall = full // count + EXTRA

    def whole(array):
        zeros = (0,) * array.ndim
        return pl.BlockSpec(array.shape, lambda i, s: zeros)

    args = (*toks, mid, stats, routes, logits, *pieces)
    specs = [param_spec(a) for a in toks] + [whole(a) for a in args[len(toks) :]]
    specs[len(toks) + 2] = pl.BlockSpec((2, span), lambda i, s: (0, s[0] * count + s[1]))
    return pl.pallas_call(
        result_kernel,
        name="result",
        cost_estimate=span_of(5),
        grid_spec=pltpu.PrefetchScalarGridSpec(
            num_scalar_prefetch=1,
            grid=(1,),
            in_specs=specs,
            out_specs=pl.BlockSpec((count, tall, span), lambda i, s: (0, 0, 0)),
        ),
        out_shape=jax.ShapeDtypeStruct((count, tall, span), F32),
        compiler_params=pltpu.CompilerParams(vmem_limit_bytes=VMEM_LIMIT),
    )(place, *args)


def experts_kernel(chunks, last, *refs):
    order, x0, x1, x2, x3, g0, g1, g2, g3, ranks, routes, w0, w1 = refs[:13]
    refs = refs[13:]
    twos, refs = refs[: len(chunks)], refs[len(chunks) :]
    threes, refs = refs[: len(chunks)], refs[len(chunks) :]
    if last:
        y_in, dx_in, gate_in = refs[:3]
        refs = refs[3:]
    y_out, dx_out = refs[:2]
    refs = refs[2:]
    if not last:
        gate_out = refs[0]
        refs = refs[1:]
    grad_mine, grad_next, weight, y_acc, dx_acc, gate_sum, gate_rows, acc = refs
    step = pl.program_id(0)
    steps = pl.num_programs(0)
    expert = order[step]
    tiles = order[steps + step]
    size = w0.shape[1]
    tokens = ranks.shape[1]
    span = tokens // 4
    full = x0.shape[1]
    hidden_width = w0.shape[2] // 3
    both = 2 * hidden_width
    xs = (x0, x1, x2, x3)
    gs = (g0, g1, g2, g3)

    @pl.when(step == 0)
    def _():
        if last:
            y_acc[...] = y_in[...]
            dx_acc[...] = dx_in[...]
            gate_sum[...] = gate_in[...]
        else:
            y_acc[...] = jnp.zeros_like(y_acc)
            dx_acc[...] = jnp.zeros_like(dx_acc)
            gate_sum[...] = jnp.zeros_like(gate_sum)
        for i, ref in enumerate(xs):
            for k in range(2):
                gate_rows[k : k + 1, i * span : (i + 1) * span] = unpack_row(ref, span, span, k)

    weight[:size] = w0[0]
    weight[size : 2 * size] = w1[0]
    start = 0
    for two, three, count in zip(twos, threes, chunks):

        @pl.when((step >= start) & (step < start + count))
        def _():
            weight[2 * size : 3 * size] = two[0]
            weight[3 * size :] = three[0]

        start += count

    rank = ranks[pl.ds(expert, 1), :]
    hit0 = routes[0:1] == expert
    hit1 = routes[1:2] == expert
    gate_row = jnp.where(hit0, gate_rows[0:1], 0.0) + jnp.where(hit1, gate_rows[1:2], 0.0)

    def tile(index, carry):
        slots = lax.broadcasted_iota(jnp.int32, (TILE, tokens), 0) + index * TILE
        hot = slots == rank
        pick = hot.astype(F32).astype(BF16)
        gate = jnp.sum(jnp.where(hot, gate_row, 0.0), axis=1, keepdims=True)
        rows = jnp.zeros((TILE, full), F32)
        flow = jnp.zeros((TILE, full), F32)
        for i in range(4):
            cut = pick[:, i * span : (i + 1) * span]
            rows = rows + mm(cut, xs[i][:span], 1, 0)
            flow = flow + mm(cut, gs[i][...], 1, 0)
        rows = rows.astype(BF16)
        flow = flow.astype(BF16)
        gate_up = mm(rows, weight[:, :both], 1, 0)
        pre = gate_up[:, :hidden_width]
        up = gate_up[:, hidden_width:]
        sigma = 1.0 / (1.0 + jnp.exp(-pre))
        lifted = pre * sigma
        hidden = lifted * up
        scaled = (hidden * gate).astype(BF16)
        back = mm(flow, weight[:, both:], 1, 0)
        grad_gate = jnp.sum(hidden * back, axis=1, keepdims=True)
        back = back * gate
        grad_pre = back * up * sigma * (1.0 + pre * (1.0 - sigma))
        grad_up = back * lifted
        grad_both = jnp.concatenate([grad_pre.astype(BF16), grad_up.astype(BF16)], axis=1)
        y = mm(scaled, weight[:, both:], 1, 1).astype(BF16)
        dx = mm(grad_both, weight[:, :both], 1, 1).astype(BF16)
        for i in range(4):
            cut = pick[:, i * span : (i + 1) * span]
            y_acc[i * span : (i + 1) * span] += mm(cut, y, 0, 0)
            dx_acc[i * span : (i + 1) * span] += mm(cut, dx, 0, 0)
        row = jnp.sum(jnp.where(hot, grad_gate, 0.0), axis=0, keepdims=True)
        gate_sum[0:1] += jnp.where(hit0, row, 0.0)
        gate_sum[1:2] += jnp.where(hit1, row, 0.0)
        grad_weight = mm(rows, grad_both, 0, 0)
        grad_down = mm(flow, scaled, 0, 0)

        @pl.when(index == 0)
        def _():
            acc[:, :both] = grad_weight
            acc[:, both:] = grad_down

        @pl.when(index > 0)
        def _():
            acc[:, :both] += grad_weight
            acc[:, both:] += grad_down

        return carry

    lax.fori_loop(0, tiles, tile, 0)
    for k in range(4):
        ref = grad_next if k % 2 else grad_mine
        ref[k // 2, 0] = acc[k * size : (k + 1) * size].astype(BF16)

    @pl.when(step == steps - 1)
    def _():
        if last:
            for i in range(4):
                here = slice(i * span, (i + 1) * span)
                y_out[i] = y_acc[here].astype(BF16)
                dx_out[i, :span] = dx_acc[here].astype(BF16)
                rows = [gate_sum[0:1, here], gate_sum[1:2, here]]
                dx_out[i, span:] = pack_rows(rows, full)
        else:
            y_out[...] = y_acc[...]
            dx_out[...] = dx_acc[...]
            gate_out[...] = gate_sum[...]


def run_experts(order, xs, gs, ranks, routes, w0, w1, twos, threes, carried):
    size, wide = w0.shape[1:]
    tokens = ranks.shape[1]
    span = tokens // 4
    full = xs[0].shape[1]
    chunks = tuple(a.shape[0] for a in twos)
    steps = sum(chunks)
    last = carried is not None

    def whole(shape):
        zeros = (0,) * len(shape)
        return pl.BlockSpec(shape, lambda e, s: zeros)

    def chunk(start, count):
        return pl.BlockSpec(
            (1, size, wide), lambda e, s: (jnp.clip(e - start, 0, count - 1), 0, 0)
        )

    mine = pl.BlockSpec((1, size, wide), lambda e, s: (s[e], 0, 0))
    pieces = [chunk(sum(chunks[:i]), count) for i, count in enumerate(chunks)]
    args = (*xs, *gs, ranks, routes, w0, w1, *twos, *threes)
    specs = [whole(a.shape) for a in args[:10]] + [mine, mine] + pieces + pieces
    if last:
        args += tuple(carried)
        specs += [whole(a.shape) for a in carried]
        shapes = [((4, span, full), BF16), ((4, span + EXTRA, full), BF16)]
    else:
        shapes = [((tokens, full), F32), ((tokens, full), F32), ((8, tokens), F32)]
    grad = pl.BlockSpec((2, 1, size, wide), lambda e, s: (0, e, 0, 0))

    def body(*refs):
        experts_kernel(chunks, last, *refs)

    return pl.pallas_call(
        body,
        name="experts",
        cost_estimate=span_of(36),
        grid_spec=pltpu.PrefetchScalarGridSpec(
            num_scalar_prefetch=1,
            grid=(steps,),
            in_specs=specs,
            out_specs=[whole(shape) for shape, _ in shapes] + [grad] * 2,
            scratch_shapes=[
                pltpu.VMEM((full, wide), BF16),
                pltpu.VMEM((tokens, full), F32),
                pltpu.VMEM((tokens, full), F32),
                pltpu.VMEM((8, tokens), F32),
                pltpu.VMEM((8, tokens), F32),
                pltpu.VMEM((full, wide), F32),
            ],
        ),
        out_shape=[jax.ShapeDtypeStruct(shape, dtype) for shape, dtype in shapes]
        + [jax.ShapeDtypeStruct((2, steps, size, wide), BF16)] * 2,
        compiler_params=pltpu.CompilerParams(vmem_limit_bytes=VMEM_LIMIT),
    )(order, *args)


def shards(
    tokens,
    prev_logits,
    routes,
    prefix_len,
    norm1_gain,
    qkv_weight,
    out_weight,
    norm2_gain,
    router_weight,
    const_weight,
    const_values,
    gate_weight,
    up_weight,
    down_weight,
    cotangent,
):
    row = lax.axis_index("row")
    col = lax.axis_index("col")
    rows = lax.axis_size("row")
    cols = lax.axis_size("col")
    groups = lax.axis_size("dp")
    length, size = tokens.shape
    span = length // cols
    kinds = router_weight.shape[1]
    experts = gate_weight.shape[0]
    half = experts // 2
    hidden_width = gate_weight.shape[2]
    first_half = lax.axis_index("dp") if groups == 2 else jnp.int32(0)
    prefix = lax.dynamic_index_in_dim(prefix_len, row, 0, False)
    place = jnp.stack([row, col, prefix, jnp.int32(experts)]).astype(jnp.int32)
    flat = [(i // cols, i % cols) for i in range(rows * cols)]

    def spread(value, turn):
        pairs = [(c * cols + (c ^ r ^ turn), r * cols + c) for r, c in flat]
        return lax.ppermute(value, ("row", "col"), pairs)

    def collect(value, turn):
        pairs = [(r * cols + c, c * cols + (r ^ turn)) for r, c in flat]
        return lax.ppermute(value, ("row", "col"), pairs)

    def across_groups(value):
        return lax.ppermute(value, "dp", [(0, 1), (1, 0)])


    values = [norm1_gain, norm2_gain, const_values[0], const_values[1]]
    lanes = [router_weight, const_weight]
    for value in values:
        lanes += [part[:, None] for part in parts_of(value)]
    lanes.append(jnp.zeros((size, PARAMS - kinds - 4 - 3 * len(values)), BF16))
    piece = jnp.concatenate([qkv_weight[0], qkv_weight[1], qkv_weight[2], out_weight.T], axis=1)
    toks = col_gather(jnp.concatenate([tokens.T] + lanes, axis=1))
    weight = jnp.stack([spread(piece, m) for m in range(rows)])
    halves = HD // 2
    freq = 10000.0 ** (-jnp.arange(halves, dtype=F32) / halves)
    angle = freq[:, None] * jnp.arange(length, dtype=F32)[None, :]
    cosine = jnp.cos(angle)
    sine = jnp.sin(angle)

    flow = after(cotangent.T, toks[2]).reshape(size, cols, span)
    flow_parts = [lax.dynamic_index_in_dim(flow, col ^ k, 1, False) for k in range(cols)]
    flow_quarter = jnp.concatenate(
        [flow_parts[0]] + [col_swap(flow_parts[k], k) for k in range(1, cols)], axis=0
    )
    flow_rows = row_gather(flow_quarter.T)

    own = jnp.concatenate([gate_weight, up_weight, down_weight.transpose(0, 2, 1)], axis=2)
    near_own = lax.dynamic_slice_in_dim(own, first_half * half, half, 0)
    pair = half // 2
    two_a = col_swap(after(near_own[:pair], flow_quarter), 2)
    projs = col_gather(after(weight[:, :, 3 * size :], toks[2]))

    routes_t = routes.T
    share = lax.dynamic_index_in_dim(routes_t.reshape(2, rows, cols, span), col, 2, False)
    turned = (row - jnp.arange(rows)) % rows
    share = jnp.take(share, turned, axis=1).reshape(2, rows * span)
    ids = jnp.arange(experts, dtype=jnp.int32)[:, None]
    hits = (share[0][None] == ids) | (share[1][None] == ids)
    counts = jnp.cumsum(hits.astype(jnp.int32), axis=1)
    ranks = jnp.where(hits, counts - 1, -1)
    order = (first_half * half + jnp.arange(experts, dtype=jnp.int32)) % experts
    tiles = jnp.take(jnp.maximum((counts[:, -1] + TILE - 1) // TILE, 1), order)
    order_near = jnp.concatenate([order[:half], tiles[:half]]).astype(jnp.int32)
    order_far = jnp.concatenate([order[half:], tiles[half:]]).astype(jnp.int32)

    query, keys, values, attn, logsum = attend(place, toks, weight, cosine, sine)
    attn, two_a, flow_rows, projs = join(attn, two_a, flow_rows, projs)
    parts = [attn[0]] + [col_swap(attn[k], k) for k in range(1, cols)]
    two_b = col_swap(after(near_own[pair:], parts[1], parts[2], parts[3]), 2)
    if groups == 2:
        far_two_a = across_groups(two_a)
    else:
        far_two_a = col_swap(own[half : half + pair], 2)
    side = col_swap(after(own, attn), 1)
    parts[1], side = join(parts[1], side)
    mid, in_rows, stats = middle(place, toks, parts, projs, prev_logits.T, routes_t)
    x_rows = row_gather(in_rows)
    three_a = col_swap(after(two_a, parts[1], parts[2], parts[3]), 1)
    two_b, far_two_a = join(after(two_b, *x_rows[1:]), after(far_two_a, *x_rows[1:]))
    if groups == 2:
        far_two_b = across_groups(two_b)
    else:
        far_two_b = col_swap(own[half + pair :], 2)
    three_b = col_swap(two_b, 1)
    far_three_a = col_swap(far_two_a, 1)
    x_rows, far_three_a = join(x_rows, far_three_a)

    near_out = run_experts(
        order_near, x_rows, flow_rows, ranks, share, own, side,
        [two_a, two_b], [three_a, three_b], None,
    )
    near_out, far_two_b = join(near_out, far_two_b)
    *carried, near_mine, near_next = near_out
    far_three_b = col_swap(far_two_b, 1)
    near_next = col_swap(after(near_next, far_three_b), 1)
    y, dx, far_mine, far_next = run_experts(
        order_far, x_rows, flow_rows, ranks, share, own, side,
        [far_two_a, far_two_b], [far_three_a, far_three_b], carried,
    )

    def low_sum(left, right):
        return (left.astype(F32) + right.astype(F32)).astype(BF16)

    def row_scatter(value):
        return [value[0]] + [row_shift(value[s], -s) for s in range(1, rows)]

    def across_sums(sums):
        return [across_groups(s) for s in sums] if groups == 2 else list(sums)

    dx = row_scatter(dx)
    near_mine = after(near_mine, dx[1])
    near_kept, near_sent = low_sum(near_mine[0], near_next[0]), low_sum(near_mine[1], near_next[1])
    near_sent, near_kept, far_next = join(near_sent, near_kept, far_next)
    near_got = [col_swap(near_sent[:pair], 2), col_swap(near_sent[pair:], 2)]
    far_next = col_swap(far_next, 1)
    dx, near_got[0] = join(dx, near_got[0])
    near_sum = [low_sum(near_kept[:pair], near_got[0])]
    near_other = across_sums(near_sum)
    low, grad_mid, grad_logits, small = middle_back(
        place, toks, mid, flow_quarter, stats, routes_t, dx, kinds
    )
    lows = col_gather(low)
    near_sum.append(low_sum(after(near_kept, low)[pair:], near_got[1]))
    lows, near_sum, near_other, far_mine, far_next = join(
        lows, near_sum, near_other, far_mine, far_next
    )
    near_other += across_sums(near_sum[1:])

    y = row_scatter(after(y, dx[1], dx[2], dx[3]))
    far_kept, far_sent = low_sum(far_mine[0], far_next[0]), low_sum(far_mine[1], far_next[1])
    far_got = [col_swap(far_sent[:pair], 2)]
    tokens_parts, weight_parts = attend_back(
        place, toks, weight, cosine, sine,
        query, keys, values, attn, logsum, lows, grad_mid, small,
    )
    tokens_parts, weight_parts, y, near_other, far_got[0], far_sent = join(
        tokens_parts, weight_parts, y, near_other, far_got[0], far_sent
    )
    far_got.append(col_swap(far_sent[pair:], 2))
    far_sum = [low_sum(far_kept[:pair], far_got[0])]
    far_other = across_sums(far_sum)
    out = result(place, toks, mid, stats, routes_t, grad_logits, y)
    weight_parts, out, far_kept = join(weight_parts, out, far_kept)
    totals = [collect(weight_parts[m], m) for m in range(rows)]
    far_sum.append(low_sum(far_kept[pair:], far_got[1]))
    far_other += across_sums(far_sum[1:])
    totals[-1] = after(totals[-1], *far_other)
    out = after(out, far_got[1])

    total = sum(part.astype(F32) for part in totals)
    packed = total[:, 4 * size : 4 * size + 3 * SMALL]
    small = packed[:, :SMALL] + packed[:, SMALL : 2 * SMALL] + packed[:, 2 * SMALL :]
    small = dp_total(row_total(small.T))
    tokens_got = [tokens_parts[0]] + [col_swap(tokens_parts[k], k) for k in range(1, cols)]
    out = [out[0]] + [col_swap(out[k], k) for k in range(1, cols)]
    total, tokens_got = join(total, tokens_got)
    total = dp_total(total[:, : 4 * size].astype(BF16))
    grad_tokens = sum(part.astype(F32) for part in tokens_got)
    qkv_sum = jnp.stack([total[:, j * size : (j + 1) * size] for j in range(3)])
    proj_sum = total[:, 3 * size :].T
    out = jnp.stack(out)
    out = jnp.take(out, col ^ jnp.arange(cols), axis=0)
    out = jnp.concatenate([out[i] for i in range(cols)], axis=1)
    if groups == 2:
        near_start = first_half * half
        far_start = half - near_start
        grads = []
        for j in range(3):
            wide = slice(j * hidden_width, (j + 1) * hidden_width)
            grad = jnp.zeros((experts, size, hidden_width), F32)
            for i in range(2):
                for start, mine, other in (
                    (near_start, near_sum[i], far_other[i]),
                    (far_start, far_sum[i], near_other[i]),
                ):
                    both = mine[:, :, wide].astype(F32) + other[:, :, wide].astype(F32)
                    grad = lax.dynamic_update_slice_in_dim(grad, both, start + i * pair, 0)
            grads.append(grad)
    else:
        both = lax.psum(jnp.concatenate(near_sum + far_sum).astype(F32), "dp")
        grads = [both[:, :, j * hidden_width : (j + 1) * hidden_width] for j in range(3)]

    return (
        out[:size].T,
        grad_tokens.T,
        out[size : size + kinds].T,
        small[SUM_GAIN1],
        qkv_sum,
        proj_sum,
        small[SUM_GAIN2],
        small[:kinds].T,
        small[kinds : kinds + 4].T,
        small[SUM_VALUE0 : SUM_VALUE1 + 1],
        grads[0],
        grads[1],
        grads[2].transpose(0, 2, 1),
    )


def solution(mesh):
    return jax.shard_map(
        shards,
        mesh=mesh,
        in_specs=(
            P(("dp", "row"), "col"),
            P(("dp", "row"), None),
            P("dp", None),
            P("dp"),
            P("col"),
            P(None, "col", "row"),
            P("row", "col"),
            P("col"),
            P("col", None),
            P("col", None),
            P(None, "col"),
            P(None, "col", "row"),
            P(None, "col", "row"),
            P(None, "row", "col"),
            P(("dp", "row"), "col"),
        ),
        out_specs=(
            P(("dp", "row"), "col"),
            P(("dp", "row"), "col"),
            P(("dp", "row"), None),
            P("col"),
            P(None, "col", "row"),
            P("row", "col"),
            P("col"),
            P("col", None),
            P("col", None),
            P(None, "col"),
            P(None, "col", "row"),
            P(None, "col", "row"),
            P(None, "row", "col"),
        ),
        check_vma=False,
    )
```

```python
import jax
import jax.numpy as jnp
from jax import lax
from jax.experimental import pallas as pl
from jax.experimental.pallas import tpu as pltpu
from jax.sharding import PartitionSpec as P

HD = 64
LEN = 1024
EPS = 1e-06
HIGH = lax.Precision.HIGHEST
NEGATIVE = -1e30
TILE = 256
VMEM_LIMIT = 60 * 1024 * 1024
F32 = jnp.float32
BF16 = jnp.bfloat16
PARAMS = 128
GAIN1, GAIN2, VALUE0, VALUE1 = 16, 19, 22, 25
SUM_GAIN2, SUM_VALUE0, SUM_VALUE1, SUM_GAIN1 = 16, 17, 18, 19
EXTRA = 16
SMALL = 24


def mm(left, right, over_left, over_right, precision=None):
    return lax.dot_general(
        left,
        right,
        (((over_left,), (over_right,)), ((), ())),
        preferred_element_type=F32,
        precision=precision,
    )


def parts_of(value):
    high = lax.reduce_precision(value, 8, 7)
    middle = lax.reduce_precision(value - high, 8, 7)
    return [high.astype(BF16), middle.astype(BF16), (value - high - middle).astype(BF16)]


def column(params, first):
    low = params[:, first : first + 3].astype(F32)
    return low[:, 0:1] + low[:, 1:2] + low[:, 2:3]


def pack_rows(rows, width):
    out = []
    for row in rows:
        high = row.astype(BF16).astype(F32)
        middle = (row - high).astype(BF16).astype(F32)
        out += [high, middle, row - high - middle]
    out.append(jnp.zeros((EXTRA - len(out), rows[0].shape[1]), F32))
    packed = jnp.concatenate(out, axis=0)
    rest = jnp.zeros((EXTRA, width - packed.shape[1]), F32)
    return jnp.concatenate([packed, rest], axis=1).astype(BF16)


def parts_in_rows(value, height):
    high = value.astype(BF16).astype(F32)
    middle = (value - high).astype(BF16).astype(F32)
    rest = jnp.zeros((height - 3 * value.shape[0], value.shape[1]), F32)
    return jnp.concatenate([high, middle, value - high - middle, rest], axis=0)


def unpack_row(ref, base, span, k):
    parts = ref[base : base + EXTRA, :span].astype(F32)
    return parts[3 * k : 3 * k + 1] + parts[3 * k + 1 : 3 * k + 2] + parts[3 * k + 2 : 3 * k + 3]


def span_of(micros):
    return pl.CostEstimate(
        flops=int(micros * 1.1e9), transcendentals=0, bytes_accessed=int(micros * 3.6e6)
    )


def after(value, *others):
    return lax.optimization_barrier((value,) + others)[0]


def join(*values):
    return lax.optimization_barrier(values)


def col_swap(value, bits):
    count = lax.axis_size("col")
    return lax.ppermute(value, "col", [(i, i ^ bits) for i in range(count)])


def row_swap(value, bits):
    count = lax.axis_size("row")
    return lax.ppermute(value, "row", [(i, i ^ bits) for i in range(count)])


def row_shift(value, steps):
    count = lax.axis_size("row")
    return lax.ppermute(value, "row", [(i, (i + steps) % count) for i in range(count)])


def col_gather(value):
    count = lax.axis_size("col")
    found = {0: value}
    bit = count // 2
    while bit:
        found.update({k | bit: col_swap(v, bit) for k, v in found.items()})
        bit //= 2
    return [found[k] for k in range(count)]


def row_gather(value):
    count = lax.axis_size("row")
    return [value] + [row_shift(value, s) for s in range(1, count)]


def dp_total(value):
    count = lax.axis_size("dp")
    if count == 2:
        other = lax.ppermute(value, "dp", [(0, 1), (1, 0)])
        return value.astype(F32) + other.astype(F32)
    return lax.psum(value.astype(F32), "dp")


def row_total(value, bit):
    while bit < lax.axis_size("row"):
        value = value + row_swap(value, bit)
        bit *= 2
    return value


def rotate_halves(block, cosine, sine):
    half = HD // 2
    out = []
    for head in range(block.shape[0] // HD):
        first = block[head * HD : head * HD + half]
        second = block[head * HD + half : (head + 1) * HD]
        out.append(first * cosine - second * sine)
        out.append(second * cosine + first * sine)
    return jnp.concatenate(out, axis=0)


def attend_kernel(
    place, t0, t1, t2, t3, weight, cosine, sine,
    query_out, key_out, value_out, attn_out, logsum_out, act, w_all,
):
    block = pl.program_id(0)
    row = place[0]
    prefix = place[2]
    size = t0.shape[0]
    heads = query_out.shape[1] // HD
    width = heads * HD
    count = query_out.shape[0]
    span = query_out.shape[2]
    length = key_out.shape[1]

    @pl.when(block == 0)
    def _():
        square = jnp.zeros((1, length), F32)
        for ref in (t0, t1, t2, t3):
            hidden = ref[:, :length].astype(F32)
            square = square + jnp.sum(hidden * hidden, axis=0, keepdims=True)
        inverse = lax.rsqrt(square / (size * 4) + EPS)
        for k, ref in enumerate((t0, t1, t2, t3)):
            gain = column(ref[:, length:], GAIN1)
            hidden = ref[:, :length].astype(F32)
            act[k * size : (k + 1) * size] = (hidden * inverse * gain).astype(BF16)
            w_all[k * size : (k + 1) * size] = weight[row ^ k, :, : 3 * width]
        qkv = mm(w_all[...], act[...], 0, 0)
        query = rotate_halves(qkv[:width], cosine[...], sine[...]).astype(BF16)
        keys = rotate_halves(qkv[width : 2 * width], cosine[...], sine[...]).astype(BF16)
        for i in range(count):
            query_out[i] = query[:, i * span : (i + 1) * span]
        key_out[...] = keys
        value_out[...] = qkv[2 * width :].astype(BF16)

    places = lax.broadcasted_iota(jnp.int32, (length, span), 0)
    mine = lax.broadcasted_iota(jnp.int32, (1, span), 1) + block * span
    seen = places <= jnp.maximum(mine, prefix - 1)
    rows = []
    for head in range(heads):
        cut = slice(head * HD, (head + 1) * HD)
        query = (query_out[block, cut].astype(F32) * HD ** (-0.5)).astype(BF16)
        scores = jnp.where(seen, mm(key_out[cut], query, 0, 0), NEGATIVE)
        top = jnp.max(scores, axis=0, keepdims=True)
        weights = jnp.exp(scores - top)
        total = jnp.sum(weights, axis=0, keepdims=True)
        mixed = mm(value_out[cut], weights.astype(BF16), 1, 0)
        attn_out[0, cut] = (mixed / total).astype(BF16)
        rows.append(top + jnp.log(total))
    rows.append(jnp.zeros((8 - heads, span), F32))
    logsum_out[...] = jnp.concatenate(rows, axis=0)


def attend(place, toks, weight, cosine, sine):
    size = toks[0].shape[0]
    length = cosine.shape[1]
    count = lax.axis_size("col")
    span = length // count
    width = weight.shape[2] // 4

    def whole(array):
        zeros = (0,) * array.ndim
        return pl.BlockSpec(array.shape, lambda q, s: zeros)

    args = (*toks, weight, cosine, sine)
    return pl.pallas_call(
        attend_kernel,
        name="attend",
        cost_estimate=span_of(14),
        grid_spec=pltpu.PrefetchScalarGridSpec(
            num_scalar_prefetch=1,
            grid=(count,),
            in_specs=[whole(a) for a in args],
            out_specs=[
                pl.BlockSpec((count, width, span), lambda q, s: (0, 0, 0)),
                pl.BlockSpec((width, length), lambda q, s: (0, 0)),
                pl.BlockSpec((width, length), lambda q, s: (0, 0)),
                pl.BlockSpec((1, width, span), lambda q, s: (q ^ s[1], 0, 0)),
                pl.BlockSpec((8, span), lambda q, s: (0, q)),
            ],
            scratch_shapes=[
                pltpu.VMEM((size * count, length), BF16),
                pltpu.VMEM((size * count, 3 * width), BF16),
            ],
        ),
        out_shape=[
            jax.ShapeDtypeStruct((count, width, span), BF16),
            jax.ShapeDtypeStruct((width, length), BF16),
            jax.ShapeDtypeStruct((width, length), BF16),
            jax.ShapeDtypeStruct((count, width, span), BF16),
            jax.ShapeDtypeStruct((8, length), F32),
        ],
        compiler_params=pltpu.CompilerParams(vmem_limit_bytes=VMEM_LIMIT),
    )(place, *args)


def attend_back_kernel(
    place, t0, t1, t2, t3, weight, cosine, sine,
    query, keys, values, attn, logsum, d0, d1, d2, d3, grad_mid, small,
    tokens_out, weight_out,
    dmid, proj_all, proj_acc, key_acc, value_acc, grad_all,
):
    block = pl.program_id(0)
    row = place[0]
    col = place[1]
    prefix = place[2]
    size = t0.shape[0]
    length = cosine.shape[1]
    count, width, span = query.shape
    heads = width // HD
    last = count - 1

    @pl.when(block == 0)
    def _():
        for k in range(count):
            proj_all[k * size : (k + 1) * size] = weight[row ^ k, :, 3 * width :]
        proj_acc[...] = jnp.zeros_like(proj_acc)
        key_acc[...] = jnp.zeros_like(key_acc)
        value_acc[...] = jnp.zeros_like(value_acc)

    for k, ref in enumerate((d0, d1, d2, d3)):

        @pl.when((block ^ col) == k)
        def _():
            for j in range(count):
                dmid[j * size : (j + 1) * size] = ref[(k ^ j) * size : ((k ^ j) + 1) * size]

    low = dmid[...]
    grad_attn = mm(proj_all[...], low, 0, 0).astype(BF16)
    proj_acc[...] += mm(low, attn[0], 1, 1)
    places = lax.broadcasted_iota(jnp.int32, (length, span), 0)
    mine = lax.broadcasted_iota(jnp.int32, (1, span), 1) + block * span
    seen = places <= jnp.maximum(mine, prefix - 1)
    scale = HD ** (-0.5)
    parts = []
    for head in range(heads):
        cut = slice(head * HD, (head + 1) * HD)
        plain = query[block, cut]
        scaled = (plain.astype(F32) * scale).astype(BF16)
        scores = mm(keys[cut], scaled, 0, 0)
        probs = jnp.where(seen, jnp.exp(scores - logsum[head : head + 1]), 0.0)
        above = grad_attn[cut]
        grad_probs = mm(values[cut], above, 0, 0)
        inner = jnp.sum(probs * grad_probs, axis=0, keepdims=True)
        grad_scores = (probs * (grad_probs - inner)).astype(BF16)
        parts.append(mm(keys[cut], grad_scores, 1, 0) * scale)
        key_acc[cut] += mm(plain, grad_scores, 1, 1)
        value_acc[cut] += mm(above, probs.astype(BF16), 1, 1)
    for i in range(count):

        @pl.when(block == i)
        def _():
            here = slice(i * span, (i + 1) * span)
            turned = rotate_halves(
                jnp.concatenate(parts, axis=0), cosine[:, here], -sine[:, here]
            )
            grad_all[:width, here] = turned.astype(BF16)

    @pl.when(block == last)
    def _():
        turned = rotate_halves(key_acc[...] * scale, cosine[...], -sine[...])
        grad_all[width : 2 * width] = turned.astype(BF16)
        grad_all[2 * width :] = value_acc[...].astype(BF16)
        refs = (t0, t1, t2, t3)
        gains = [column(ref[:, length:], GAIN1) for ref in refs]
        square = jnp.zeros((1, length), F32)
        for ref in refs:
            hidden = ref[:, :length].astype(F32)
            square = square + jnp.sum(hidden * hidden, axis=0, keepdims=True)
        inverse = lax.rsqrt(square / (size * count) + EPS)
        backs = []
        inner = jnp.zeros((1, length), F32)
        for k in range(count):
            hidden = refs[k][:, :length].astype(F32)
            act = (hidden * inverse * gains[k]).astype(BF16)
            weight_out[row ^ col ^ k, :, : 3 * width] = mm(act, grad_all[...], 1, 1).astype(BF16)
            weight_out[row ^ col ^ k, :, 3 * width : 4 * width] = proj_acc[
                k * size : (k + 1) * size
            ].astype(BF16)
            back = mm(weight[row ^ k, :, : 3 * width], grad_all[...], 1, 0)
            inner = inner + jnp.sum(hidden * gains[k] * back, axis=0, keepdims=True)
            summed = jnp.sum(hidden * inverse * back, axis=1, keepdims=True)
            turned = jnp.transpose(jnp.broadcast_to(summed, (size, 128)))[: small.shape[1]]
            places = lax.broadcasted_iota(jnp.int32, turned.shape, 0)
            rows = parts_in_rows(jnp.where(places == SUM_GAIN1, turned, small[k]), PARAMS)
            weight_out[row ^ col ^ k, :, 4 * width :] = jnp.transpose(rows).astype(BF16)
            backs.append(back)
        inner = inner * (inverse * inverse * inverse) / (size * count)
        for k in range(count):
            hidden = refs[k][:, :length].astype(F32)
            grad = inverse * gains[k] * backs[k] - hidden * inner
            for i in range(count):
                here = slice(i * span, (i + 1) * span)
                extra = jnp.where(col == i, grad_mid[k * size : (k + 1) * size], 0.0)
                tokens_out[k, :, here] = (grad[:, here] + extra).astype(BF16)


def attend_back(
    place, toks, weight, cosine, sine, query, keys, values, attn, logsum, lows, grad_mid, small
):
    size = toks[0].shape[0]
    length = cosine.shape[1]
    count, width, span = query.shape

    def whole(array):
        zeros = (0,) * array.ndim
        return pl.BlockSpec(array.shape, lambda q, s: zeros)

    args = (
        *toks, weight, cosine, sine, query, keys, values, attn, logsum, *lows, grad_mid, small,
    )
    specs = [whole(a) for a in args]
    at = len(toks) + 3 + 3
    specs[at] = pl.BlockSpec((1, width, span), lambda q, s: (q ^ s[1], 0, 0))
    specs[at + 1] = pl.BlockSpec((8, span), lambda q, s: (0, q))
    return pl.pallas_call(
        attend_back_kernel,
        name="attend_back",
        cost_estimate=span_of(24),
        grid_spec=pltpu.PrefetchScalarGridSpec(
            num_scalar_prefetch=1,
            grid=(count,),
            in_specs=specs,
            out_specs=[
                pl.BlockSpec((count, size, length), lambda q, s: (0, 0, 0)),
                pl.BlockSpec((count, size, 4 * width + PARAMS), lambda q, s: (0, 0, 0)),
            ],
            scratch_shapes=[
                pltpu.VMEM((size * count, span), BF16),
                pltpu.VMEM((size * count, width), BF16),
                pltpu.VMEM((size * count, width), F32),
                pltpu.VMEM((width, length), F32),
                pltpu.VMEM((width, length), F32),
                pltpu.VMEM((3 * width, length), BF16),
            ],
        ),
        out_shape=[
            jax.ShapeDtypeStruct((count, size, length), BF16),
            jax.ShapeDtypeStruct((count, size, 4 * width + PARAMS), BF16),
        ],
        compiler_params=pltpu.CompilerParams(vmem_limit_bytes=VMEM_LIMIT),
    )(place, *args)


def route_rows(routes, logits):
    places = lax.broadcasted_iota(jnp.int32, logits.shape, 0)
    hots = [places == routes[k : k + 1] for k in range(2)]
    return hots, [jnp.sum(jnp.where(hot, logits, 0.0), axis=0, keepdims=True) for hot in hots]


def pair_softmax(first, second):
    top = jnp.maximum(first, second)
    first = jnp.exp(first - top)
    second = jnp.exp(second - top)
    total = first + second
    return first / total, second / total


def middle_kernel(
    place, t0, t1, t2, t3, p0, p1, p2, p3, a0, a1, a2, a3, o0, o1, o2, o3, previous, routes,
    mid_out, rows_out, stats_out,
):
    row = place[0]
    size, span = t0.shape
    params = (p0, p1, p2, p3)
    kinds = previous.shape[0]
    square = jnp.zeros((1, span), F32)
    for j, ref in enumerate((t0, t1, t2, t3)):
        mid = ref[...].astype(F32)
        for k, (part, proj) in enumerate(((a0, o0), (a1, o1), (a2, o2), (a3, o3))):
            mid = mid + mm(proj[row ^ k ^ j], part[...], 1, 0)
        square = square + jnp.sum(mid * mid, axis=0, keepdims=True)
        mid_out[j * size : (j + 1) * size] = mid
    inverse = lax.rsqrt(square / (size * 4) + EPS)
    summed = jnp.zeros((128, span), F32)
    normed = []
    for j in range(4):
        norm = mid_out[j * size : (j + 1) * size] * inverse * column(params[j], GAIN2)
        summed = summed + mm(params[j][...].astype(F32), norm, 0, 0, HIGH)
        normed.append(norm)
    rows_out[:span] = jnp.transpose(jnp.concatenate(normed, axis=0)).astype(BF16)
    logits = summed[:kinds] + previous[...]
    _, chosen = route_rows(routes[...], logits)
    gates = pair_softmax(*chosen)
    rows_out[span:] = pack_rows(gates, rows_out.shape[1])
    alpha = [
        *pair_softmax(summed[12:13], summed[13:14]),
        *pair_softmax(summed[14:15], summed[15:16]),
    ]
    stats_out[...] = jnp.concatenate([*gates, inverse, *alpha, jnp.zeros((1, span), F32)], axis=0)


def param_spec(array):
    size, width = array.shape
    return pl.BlockSpec((size, PARAMS), lambda i, s: (0, width // PARAMS - 1))


def middle(place, toks, parts, projs, previous, routes):
    size = toks[0].shape[0]
    span = parts[0].shape[1]
    count = lax.axis_size("col")

    def whole(array):
        zeros = (0,) * array.ndim
        return pl.BlockSpec(array.shape, lambda i, s: zeros)

    args = (*toks, *toks, *parts, *projs, previous, routes)
    specs = [pl.BlockSpec((size, span), lambda i, s: (0, s[1])) for _ in toks]
    specs += [param_spec(a) for a in toks]
    specs += [whole(a) for a in (*parts, *projs)]
    specs += [
        pl.BlockSpec((previous.shape[0], span), lambda i, s: (0, s[1])),
        pl.BlockSpec((2, span), lambda i, s: (0, s[0] * count + s[1])),
    ]
    full = size * count
    return pl.pallas_call(
        middle_kernel,
        name="middle",
        cost_estimate=span_of(6),
        grid_spec=pltpu.PrefetchScalarGridSpec(
            num_scalar_prefetch=1,
            grid=(1,),
            in_specs=specs,
            out_specs=[
                pl.BlockSpec((full, span), lambda i, s: (0, 0)),
                pl.BlockSpec((span + EXTRA, full), lambda i, s: (0, 0)),
                pl.BlockSpec((8, span), lambda i, s: (0, 0)),
            ],
        ),
        out_shape=[
            jax.ShapeDtypeStruct((full, span), F32),
            jax.ShapeDtypeStruct((span + EXTRA, full), BF16),
            jax.ShapeDtypeStruct((8, span), F32),
        ],
        compiler_params=pltpu.CompilerParams(vmem_limit_bytes=VMEM_LIMIT),
    )(place, *args)


def middle_back_kernel(
    place, p0, p1, p2, p3, mid, grad, stats, routes, x0, x1, x2, x3,
    low_out, mid_out, logits_out, small_out,
):
    params = (p0, p1, p2, p3)
    full, span = mid.shape
    size = p0.shape[0]
    kinds = logits_out.shape[0]
    gates = [stats[0:1], stats[1:2]]
    inverse = stats[2:3]
    alpha = [stats[3:4], stats[4:5], stats[5:6], stats[6:7]]
    names = [routes[0:1], routes[1:2]]
    xs = (x0, x1, x2, x3)
    moe = jnp.transpose(sum(x[:span].astype(F32) for x in xs))
    ffn = [sum(unpack_row(x, span, span, k) for x in xs) for k in range(2)]
    flow = grad[...].astype(F32)
    normed = []
    dot_norm = jnp.zeros((1, span), F32)
    dot_value = [jnp.zeros((1, span), F32), jnp.zeros((1, span), F32)]
    for j in range(4):
        here = slice(j * size, (j + 1) * size)
        norm = mid[here] * inverse * column(params[j], GAIN2)
        dot_norm = dot_norm + jnp.sum(flow[here] * norm, axis=0, keepdims=True)
        for c, first in enumerate((VALUE0, VALUE1)):
            value = column(params[j], first)
            dot_value[c] = dot_value[c] + jnp.sum(flow[here] * value, axis=0, keepdims=True)
        normed.append(norm)
    experts = kinds - 4
    is_copy = [(name == experts + 1).astype(F32) for name in names]
    is_const = [[(name == experts + 2 + c).astype(F32) for name in names] for c in range(2)]
    grad_gate = []
    for k in range(2):
        value = ffn[k] + is_copy[k] * dot_norm
        for c in range(2):
            value = value + is_const[c][k] * (
                alpha[2 * c] * dot_norm + alpha[2 * c + 1] * dot_value[c]
            )
        grad_gate.append(value)
    shared = gates[0] * grad_gate[0] + gates[1] * grad_gate[1]
    chosen = [gates[k] * (grad_gate[k] - shared) for k in range(2)]
    places = lax.broadcasted_iota(jnp.int32, (kinds, span), 0)
    logits = jnp.where(places == names[0], chosen[0], 0.0) + jnp.where(
        places == names[1], chosen[1], 0.0
    )
    logits_out[...] = logits
    direct = gates[0] * is_copy[0] + gates[1] * is_copy[1]
    rows = [logits]
    portions = []
    for c in range(2):
        portion = gates[0] * is_const[c][0] + gates[1] * is_const[c][1]
        first, second = alpha[2 * c], alpha[2 * c + 1]
        along = [portion * dot_norm, portion * dot_value[c]]
        mean = first * along[0] + second * along[1]
        rows += [first * (along[0] - mean), second * (along[1] - mean)]
        direct = direct + first * portion
        portions.append(second * portion)
    rows.append(jnp.zeros((128 - kinds - 4, span), F32))
    routed = jnp.concatenate(rows, axis=0)
    lanes = lax.broadcasted_iota(jnp.int32, (size, 128), 1)
    backs = []
    inner = jnp.zeros((1, span), F32)
    for j in range(4):
        here = slice(j * size, (j + 1) * size)
        back = moe[here] + direct * flow[here] + mm(params[j][...].astype(F32), routed, 1, 0, HIGH)
        small = mm(normed[j], routed, 1, 1, HIGH)
        columns = (
            (SUM_GAIN2, mid[here] * inverse * back),
            (SUM_VALUE0, portions[0] * flow[here]),
            (SUM_VALUE1, portions[1] * flow[here]),
        )
        for lane, terms in columns:
            total = jnp.sum(terms, axis=1, keepdims=True)
            small = jnp.where(lanes == lane, total, small)
        small_out[j] = jnp.transpose(small)[:SMALL]
        gain = column(params[j], GAIN2)
        inner = inner + jnp.sum(mid[here] * gain * back, axis=0, keepdims=True)
        backs.append(back)
    inner = inner * (inverse * inverse * inverse) / full
    for j in range(4):
        here = slice(j * size, (j + 1) * size)
        gain = column(params[j], GAIN2)
        value = flow[here] + inverse * gain * backs[j] - mid[here] * inner
        mid_out[here] = value
        low_out[here] = value.astype(BF16)


def middle_back(place, toks, mid, grad, stats, routes, pieces, kinds):
    full, span = mid.shape
    count = lax.axis_size("col")
    size = full // count

    def whole(array):
        zeros = (0,) * array.ndim
        return pl.BlockSpec(array.shape, lambda i, s: zeros)

    args = (*toks, mid, grad, stats, routes, *pieces)
    specs = [param_spec(a) for a in toks] + [whole(a) for a in args[len(toks) :]]
    specs[len(toks) + 3] = pl.BlockSpec((2, span), lambda i, s: (0, s[0] * count + s[1]))
    return pl.pallas_call(
        middle_back_kernel,
        name="middle_back",
        cost_estimate=span_of(7),
        grid_spec=pltpu.PrefetchScalarGridSpec(
            num_scalar_prefetch=1,
            grid=(1,),
            in_specs=specs,
            out_specs=[
                pl.BlockSpec((full, span), lambda i, s: (0, 0)),
                pl.BlockSpec((full, span), lambda i, s: (0, 0)),
                pl.BlockSpec((kinds, span), lambda i, s: (0, 0)),
                pl.BlockSpec((count, SMALL, size), lambda i, s: (0, 0, 0)),
            ],
        ),
        out_shape=[
            jax.ShapeDtypeStruct((full, span), BF16),
            jax.ShapeDtypeStruct((full, span), F32),
            jax.ShapeDtypeStruct((kinds, span), F32),
            jax.ShapeDtypeStruct((count, SMALL, size), F32),
        ],
        compiler_params=pltpu.CompilerParams(vmem_limit_bytes=VMEM_LIMIT),
    )(place, *args)


def result_kernel(place, p0, p1, p2, p3, mid, stats, routes, logits, y0, y1, y2, y3, out):
    params = (p0, p1, p2, p3)
    size = p0.shape[0]
    experts = place[3]
    inverse = stats[2:3]
    names = [routes[0:1], routes[1:2]]
    gates = [stats[0:1], stats[1:2]]

    def portion(kind):
        return jnp.where(names[0] == kind, gates[0], 0.0) + jnp.where(
            names[1] == kind, gates[1], 0.0
        )

    first, second = portion(experts + 2), portion(experts + 3)
    direct = portion(experts + 1) + first * stats[3:4] + second * stats[5:6]
    moe = y0[...].astype(F32) + y1[...].astype(F32) + y2[...].astype(F32) + y3[...].astype(F32)
    moe = jnp.transpose(moe)
    for j in range(4):
        here = slice(j * size, (j + 1) * size)
        norm = mid[here] * inverse * column(params[j], GAIN2)
        out[j, :size] = (
            mid[here]
            + moe[here]
            + direct * norm
            + first * stats[4:5] * column(params[j], VALUE0)
            + second * stats[6:7] * column(params[j], VALUE1)
        )
        out[j, size:] = jnp.concatenate(
            [logits[...], jnp.zeros((EXTRA - logits.shape[0], logits.shape[1]), F32)], axis=0
        )


def result(place, toks, mid, stats, routes, logits, pieces):
    full, span = mid.shape
    count = lax.axis_size("col")
    tall = full // count + EXTRA

    def whole(array):
        zeros = (0,) * array.ndim
        return pl.BlockSpec(array.shape, lambda i, s: zeros)

    args = (*toks, mid, stats, routes, logits, *pieces)
    specs = [param_spec(a) for a in toks] + [whole(a) for a in args[len(toks) :]]
    specs[len(toks) + 2] = pl.BlockSpec((2, span), lambda i, s: (0, s[0] * count + s[1]))
    return pl.pallas_call(
        result_kernel,
        name="result",
        cost_estimate=span_of(5),
        grid_spec=pltpu.PrefetchScalarGridSpec(
            num_scalar_prefetch=1,
            grid=(1,),
            in_specs=specs,
            out_specs=pl.BlockSpec((count, tall, span), lambda i, s: (0, 0, 0)),
        ),
        out_shape=jax.ShapeDtypeStruct((count, tall, span), F32),
        compiler_params=pltpu.CompilerParams(vmem_limit_bytes=VMEM_LIMIT),
    )(place, *args)


def experts_kernel(chunks, last, *refs):
    order, x0, x1, x2, x3, g0, g1, g2, g3, ranks, routes, w0, w1 = refs[:13]
    refs = refs[13:]
    twos, refs = refs[: len(chunks)], refs[len(chunks) :]
    threes, refs = refs[: len(chunks)], refs[len(chunks) :]
    if last:
        y_in, dx_in, gate_in = refs[:3]
        refs = refs[3:]
    y_out, dx_out = refs[:2]
    refs = refs[2:]
    if not last:
        gate_out = refs[0]
        refs = refs[1:]
    grad_mine, grad_next, weight, y_acc, dx_acc, gate_sum, gate_rows, acc = refs
    step = pl.program_id(0)
    steps = pl.num_programs(0)
    expert = order[step]
    tiles = order[steps + step]
    size = w0.shape[1]
    tokens = ranks.shape[1]
    span = tokens // 4
    full = x0.shape[1]
    hidden_width = w0.shape[2] // 3
    both = 2 * hidden_width
    xs = (x0, x1, x2, x3)
    gs = (g0, g1, g2, g3)

    @pl.when(step == 0)
    def _():
        if last:
            y_acc[...] = y_in[...]
            dx_acc[...] = dx_in[...]
            gate_sum[...] = gate_in[...]
        else:
            y_acc[...] = jnp.zeros_like(y_acc)
            dx_acc[...] = jnp.zeros_like(dx_acc)
            gate_sum[...] = jnp.zeros_like(gate_sum)
        for i, ref in enumerate(xs):
            for k in range(2):
                gate_rows[k : k + 1, i * span : (i + 1) * span] = unpack_row(ref, span, span, k)

    weight[:size] = w0[0]
    weight[size : 2 * size] = w1[0]
    start = 0
    for two, three, count in zip(twos, threes, chunks):

        @pl.when((step >= start) & (step < start + count))
        def _():
            weight[2 * size : 3 * size] = two[0]
            weight[3 * size :] = three[0]

        start += count

    rank = ranks[pl.ds(expert, 1), :]
    hit0 = routes[0:1] == expert
    hit1 = routes[1:2] == expert
    gate_row = jnp.where(hit0, gate_rows[0:1], 0.0) + jnp.where(hit1, gate_rows[1:2], 0.0)

    def tile(index, carry):
        slots = lax.broadcasted_iota(jnp.int32, (TILE, tokens), 0) + index * TILE
        hot = slots == rank
        pick = hot.astype(F32).astype(BF16)
        gate = jnp.sum(jnp.where(hot, gate_row, 0.0), axis=1, keepdims=True)
        rows = jnp.zeros((TILE, full), F32)
        flow = jnp.zeros((TILE, full), F32)
        for i in range(4):
            cut = pick[:, i * span : (i + 1) * span]
            rows = rows + mm(cut, xs[i][:span], 1, 0)
            flow = flow + mm(cut, gs[i][...], 1, 0)
        rows = rows.astype(BF16)
        flow = flow.astype(BF16)
        gate_up = mm(rows, weight[:, :both], 1, 0)
        pre = gate_up[:, :hidden_width]
        up = gate_up[:, hidden_width:]
        sigma = 1.0 / (1.0 + jnp.exp(-pre))
        lifted = pre * sigma
        hidden = lifted * up
        scaled = (hidden * gate).astype(BF16)
        back = mm(flow, weight[:, both:], 1, 0)
        grad_gate = jnp.sum(hidden * back, axis=1, keepdims=True)
        back = back * gate
        grad_pre = back * up * sigma * (1.0 + pre * (1.0 - sigma))
        grad_up = back * lifted
        grad_both = jnp.concatenate([grad_pre.astype(BF16), grad_up.astype(BF16)], axis=1)
        y = mm(scaled, weight[:, both:], 1, 1).astype(BF16)
        dx = mm(grad_both, weight[:, :both], 1, 1).astype(BF16)
        for i in range(4):
            cut = pick[:, i * span : (i + 1) * span]
            y_acc[i * span : (i + 1) * span] += mm(cut, y, 0, 0)
            dx_acc[i * span : (i + 1) * span] += mm(cut, dx, 0, 0)
        row = jnp.sum(jnp.where(hot, grad_gate, 0.0), axis=0, keepdims=True)
        gate_sum[0:1] += jnp.where(hit0, row, 0.0)
        gate_sum[1:2] += jnp.where(hit1, row, 0.0)
        grad_weight = mm(rows, grad_both, 0, 0)
        grad_down = mm(flow, scaled, 0, 0)

        @pl.when(index == 0)
        def _():
            acc[:, :both] = grad_weight
            acc[:, both:] = grad_down

        @pl.when(index > 0)
        def _():
            acc[:, :both] += grad_weight
            acc[:, both:] += grad_down

        return carry

    lax.fori_loop(0, tiles, tile, 0)
    for k in range(4):
        ref = grad_next if k % 2 else grad_mine
        ref[k // 2, 0] = acc[k * size : (k + 1) * size].astype(BF16)

    @pl.when(step == steps - 1)
    def _():
        if last:
            for i in range(4):
                here = slice(i * span, (i + 1) * span)
                y_out[i] = y_acc[here].astype(BF16)
                dx_out[i, :span] = dx_acc[here].astype(BF16)
                rows = [gate_sum[0:1, here], gate_sum[1:2, here]]
                dx_out[i, span:] = pack_rows(rows, full)
        else:
            y_out[...] = y_acc[...]
            dx_out[...] = dx_acc[...]
            gate_out[...] = gate_sum[...]


def run_experts(order, xs, gs, ranks, routes, w0, w1, twos, threes, carried):
    size, wide = w0.shape[1:]
    tokens = ranks.shape[1]
    span = tokens // 4
    full = xs[0].shape[1]
    chunks = tuple(a.shape[0] for a in twos)
    steps = sum(chunks)
    last = carried is not None

    def whole(shape):
        zeros = (0,) * len(shape)
        return pl.BlockSpec(shape, lambda e, s: zeros)

    def chunk(start, count):
        return pl.BlockSpec(
            (1, size, wide), lambda e, s: (jnp.clip(e - start, 0, count - 1), 0, 0)
        )

    mine = pl.BlockSpec((1, size, wide), lambda e, s: (s[e], 0, 0))
    pieces = [chunk(sum(chunks[:i]), count) for i, count in enumerate(chunks)]
    args = (*xs, *gs, ranks, routes, w0, w1, *twos, *threes)
    specs = [whole(a.shape) for a in args[:10]] + [mine, mine] + pieces + pieces
    if last:
        args += tuple(carried)
        specs += [whole(a.shape) for a in carried]
        shapes = [((4, span, full), BF16), ((4, span + EXTRA, full), BF16)]
    else:
        shapes = [((tokens, full), F32), ((tokens, full), F32), ((8, tokens), F32)]
    grad = pl.BlockSpec((2, 1, size, wide), lambda e, s: (0, e, 0, 0))

    def body(*refs):
        experts_kernel(chunks, last, *refs)

    return pl.pallas_call(
        body,
        name="experts",
        cost_estimate=span_of(36),
        grid_spec=pltpu.PrefetchScalarGridSpec(
            num_scalar_prefetch=1,
            grid=(steps,),
            in_specs=specs,
            out_specs=[whole(shape) for shape, _ in shapes] + [grad] * 2,
            scratch_shapes=[
                pltpu.VMEM((full, wide), BF16),
                pltpu.VMEM((tokens, full), F32),
                pltpu.VMEM((tokens, full), F32),
                pltpu.VMEM((8, tokens), F32),
                pltpu.VMEM((8, tokens), F32),
                pltpu.VMEM((full, wide), F32),
            ],
        ),
        out_shape=[jax.ShapeDtypeStruct(shape, dtype) for shape, dtype in shapes]
        + [jax.ShapeDtypeStruct((2, steps, size, wide), BF16)] * 2,
        compiler_params=pltpu.CompilerParams(vmem_limit_bytes=VMEM_LIMIT),
    )(order, *args)


def shards(
    tokens,
    prev_logits,
    routes,
    prefix_len,
    norm1_gain,
    qkv_weight,
    out_weight,
    norm2_gain,
    router_weight,
    const_weight,
    const_values,
    gate_weight,
    up_weight,
    down_weight,
    cotangent,
):
    row = lax.axis_index("row")
    col = lax.axis_index("col")
    rows = lax.axis_size("row")
    cols = lax.axis_size("col")
    groups = lax.axis_size("dp")
    length, size = tokens.shape
    span = length // cols
    kinds = router_weight.shape[1]
    experts = gate_weight.shape[0]
    half = experts // 2
    hidden_width = gate_weight.shape[2]
    first_half = lax.axis_index("dp") if groups == 2 else jnp.int32(0)
    prefix = lax.dynamic_index_in_dim(prefix_len, row, 0, False)
    place = jnp.stack([row, col, prefix, jnp.int32(experts)]).astype(jnp.int32)
    flat = [(i // cols, i % cols) for i in range(rows * cols)]

    def spread(value, turn):
        pairs = [(c * cols + (c ^ r ^ turn), r * cols + c) for r, c in flat]
        return lax.ppermute(value, ("row", "col"), pairs)

    def collect(value, turn):
        pairs = [(r * cols + c, c * cols + (r ^ turn)) for r, c in flat]
        return lax.ppermute(value, ("row", "col"), pairs)

    def across_groups(value):
        return lax.ppermute(value, "dp", [(0, 1), (1, 0)])


    values = [norm1_gain, norm2_gain, const_values[0], const_values[1]]
    lanes = [router_weight, const_weight]
    for value in values:
        lanes += [part[:, None] for part in parts_of(value)]
    lanes.append(jnp.zeros((size, PARAMS - kinds - 4 - 3 * len(values)), BF16))
    piece = jnp.concatenate([qkv_weight[0], qkv_weight[1], qkv_weight[2], out_weight.T], axis=1)
    toks = col_gather(jnp.concatenate([tokens.T] + lanes, axis=1))
    weight = jnp.stack([spread(piece, m) for m in range(rows)])
    halves = HD // 2
    freq = 10000.0 ** (-jnp.arange(halves, dtype=F32) / halves)
    angle = freq[:, None] * jnp.arange(length, dtype=F32)[None, :]
    cosine = jnp.cos(angle)
    sine = jnp.sin(angle)

    flow = after(cotangent.T, toks[2]).reshape(size, cols, span)
    flow_parts = [lax.dynamic_index_in_dim(flow, col ^ k, 1, False) for k in range(cols)]
    flow_quarter = jnp.concatenate(
        [flow_parts[0]] + [col_swap(flow_parts[k], k) for k in range(1, cols)], axis=0
    )
    flow_rows = row_gather(flow_quarter.T)

    own = jnp.concatenate([gate_weight, up_weight, down_weight.transpose(0, 2, 1)], axis=2)
    near_own = lax.dynamic_slice_in_dim(own, first_half * half, half, 0)
    pair = half // 2
    two_a = col_swap(after(near_own[:pair], flow_quarter), 2)
    projs = col_gather(after(weight[:, :, 3 * size :], toks[2]))

    routes_t = routes.T
    share = lax.dynamic_index_in_dim(routes_t.reshape(2, rows, cols, span), col, 2, False)
    turned = (row - jnp.arange(rows)) % rows
    share = jnp.take(share, turned, axis=1).reshape(2, rows * span)
    ids = jnp.arange(experts, dtype=jnp.int32)[:, None]
    hits = (share[0][None] == ids) | (share[1][None] == ids)
    counts = jnp.cumsum(hits.astype(jnp.int32), axis=1)
    ranks = jnp.where(hits, counts - 1, -1)
    order = (first_half * half + jnp.arange(experts, dtype=jnp.int32)) % experts
    tiles = jnp.take(jnp.maximum((counts[:, -1] + TILE - 1) // TILE, 1), order)
    order_near = jnp.concatenate([order[:half], tiles[:half]]).astype(jnp.int32)
    order_far = jnp.concatenate([order[half:], tiles[half:]]).astype(jnp.int32)

    query, keys, values, attn, logsum = attend(place, toks, weight, cosine, sine)
    attn, two_a, flow_rows, projs = join(attn, two_a, flow_rows, projs)
    parts = [attn[0]] + [col_swap(attn[k], k) for k in range(1, cols)]
    two_b = col_swap(after(near_own[pair:], parts[1], parts[2], parts[3]), 2)
    if groups == 2:
        far_two_a = across_groups(two_a)
    else:
        far_two_a = col_swap(own[half : half + pair], 2)
    side = col_swap(after(own, attn), 1)
    parts[1], side = join(parts[1], side)
    mid, in_rows, stats = middle(place, toks, parts, projs, prev_logits.T, routes_t)
    x_rows = row_gather(in_rows)
    three_a = col_swap(after(two_a, parts[1], parts[2], parts[3]), 1)
    two_b, far_two_a = join(after(two_b, *x_rows[1:]), after(far_two_a, *x_rows[1:]))
    if groups == 2:
        far_two_b = across_groups(two_b)
    else:
        far_two_b = col_swap(own[half + pair :], 2)
    three_b = col_swap(two_b, 1)
    far_three_a = col_swap(far_two_a, 1)
    x_rows, far_three_a = join(x_rows, far_three_a)

    near_out = run_experts(
        order_near, x_rows, flow_rows, ranks, share, own, side,
        [two_a, two_b], [three_a, three_b], None,
    )
    near_out, far_two_b = join(near_out, far_two_b)
    *carried, near_mine, near_next = near_out
    far_three_b = col_swap(far_two_b, 1)
    near_next = col_swap(after(near_next, far_three_b), 1)
    y, dx, far_mine, far_next = run_experts(
        order_far, x_rows, flow_rows, ranks, share, own, side,
        [far_two_a, far_two_b], [far_three_a, far_three_b], carried,
    )

    def low_sum(left, right):
        return (left.astype(F32) + right.astype(F32)).astype(BF16)

    def row_scatter(value):
        return [value[0]] + [row_shift(value[s], -s) for s in range(1, rows)]

    def across_sums(sums):
        return [across_groups(s) for s in sums] if groups == 2 else list(sums)

    dx = row_scatter(dx)
    near_mine = after(near_mine, dx[1])
    near_kept, near_sent = low_sum(near_mine[0], near_next[0]), low_sum(near_mine[1], near_next[1])
    near_sent, near_kept, far_next = join(near_sent, near_kept, far_next)
    near_got = [col_swap(near_sent[:pair], 2), col_swap(near_sent[pair:], 2)]
    far_next = col_swap(far_next, 1)
    dx, near_got[0] = join(dx, near_got[0])
    near_sum = [low_sum(near_kept[:pair], near_got[0])]
    near_other = across_sums(near_sum)
    low, grad_mid, grad_logits, small = middle_back(
        place, toks, mid, flow_quarter, stats, routes_t, dx, kinds
    )
    lows = col_gather(low)
    near_sum.append(low_sum(after(near_kept, low)[pair:], near_got[1]))
    lows, near_sum, near_other, far_mine, far_next = join(
        lows, near_sum, near_other, far_mine, far_next
    )
    near_other += across_sums(near_sum[1:])

    y = row_scatter(after(y, dx[1], dx[2], dx[3]))
    far_kept, far_sent = low_sum(far_mine[0], far_next[0]), low_sum(far_mine[1], far_next[1])
    far_got = [col_swap(far_sent[:pair], 2)]
    tokens_parts, weight_parts = attend_back(
        place, toks, weight, cosine, sine,
        query, keys, values, attn, logsum, lows, grad_mid, small,
    )
    tokens_parts, weight_parts, y, near_other, far_got[0], far_sent = join(
        tokens_parts, weight_parts, y, near_other, far_got[0], far_sent
    )
    far_got.append(col_swap(far_sent[pair:], 2))
    far_sum = [low_sum(far_kept[:pair], far_got[0])]
    far_other = across_sums(far_sum)
    out = result(place, toks, mid, stats, routes_t, grad_logits, y)
    weight_parts, out, far_kept = join(weight_parts, out, far_kept)
    totals = [collect(weight_parts[m], m) for m in range(rows)]
    far_sum.append(low_sum(far_kept[pair:], far_got[1]))
    far_other += across_sums(far_sum[1:])
    totals[-1] = after(totals[-1], *far_other)
    out = after(out, far_got[1])

    total = sum(part.astype(F32) for part in totals)
    packed = total[:, 4 * size : 4 * size + 3 * SMALL]
    small = packed[:, :SMALL] + packed[:, SMALL : 2 * SMALL] + packed[:, 2 * SMALL :]
    small = small.T + row_swap(small.T, 1)
    tokens_got = [tokens_parts[0]] + [col_swap(tokens_parts[k], k) for k in range(1, cols)]
    out = [out[0]] + [col_swap(out[k], k) for k in range(1, cols)]
    total, tokens_got, small = join(total, tokens_got, small)
    small = dp_total(row_total(small, 2))
    total = dp_total(total[:, : 4 * size].astype(BF16))
    grad_tokens = sum(part.astype(F32) for part in tokens_got)
    qkv_sum = jnp.stack([total[:, j * size : (j + 1) * size] for j in range(3)])
    proj_sum = total[:, 3 * size :].T
    out = jnp.stack(out)
    out = jnp.take(out, col ^ jnp.arange(cols), axis=0)
    out = jnp.concatenate([out[i] for i in range(cols)], axis=1)
    if groups == 2:
        near_start = first_half * half
        far_start = half - near_start
        grads = []
        for j in range(3):
            wide = slice(j * hidden_width, (j + 1) * hidden_width)
            grad = jnp.zeros((experts, size, hidden_width), F32)
            for i in range(2):
                for start, mine, other in (
                    (near_start, near_sum[i], far_other[i]),
                    (far_start, far_sum[i], near_other[i]),
                ):
                    both = mine[:, :, wide].astype(F32) + other[:, :, wide].astype(F32)
                    grad = lax.dynamic_update_slice_in_dim(grad, both, start + i * pair, 0)
            grads.append(grad)
    else:
        both = lax.psum(jnp.concatenate(near_sum + far_sum).astype(F32), "dp")
        grads = [both[:, :, j * hidden_width : (j + 1) * hidden_width] for j in range(3)]

    return (
        out[:size].T,
        grad_tokens.T,
        out[size : size + kinds].T,
        small[SUM_GAIN1],
        qkv_sum,
        proj_sum,
        small[SUM_GAIN2],
        small[:kinds].T,
        small[kinds : kinds + 4].T,
        small[SUM_VALUE0 : SUM_VALUE1 + 1],
        grads[0],
        grads[1],
        grads[2].transpose(0, 2, 1),
    )


def solution(mesh):
    return jax.shard_map(
        shards,
        mesh=mesh,
        in_specs=(
            P(("dp", "row"), "col"),
            P(("dp", "row"), None),
            P("dp", None),
            P("dp"),
            P("col"),
            P(None, "col", "row"),
            P("row", "col"),
            P("col"),
            P("col", None),
            P("col", None),
            P(None, "col"),
            P(None, "col", "row"),
            P(None, "col", "row"),
            P(None, "row", "col"),
            P(("dp", "row"), "col"),
        ),
        out_specs=(
            P(("dp", "row"), "col"),
            P(("dp", "row"), "col"),
            P(("dp", "row"), None),
            P("col"),
            P(None, "col", "row"),
            P("row", "col"),
            P("col"),
            P("col", None),
            P("col", None),
            P(None, "col"),
            P(None, "col", "row"),
            P(None, "col", "row"),
            P(None, "row", "col"),
        ),
        check_vma=False,
    )
```
